256 devices in a mesh: ens: 8 (over z_lo, core), gy: 4 (over y), gz: 8 (over z_hi, x).
Axes of the slice: x: 4, y: 4, z: 8 (z_hi: 2, z_lo: 4; z = z_hi * 4 + z_lo), core: 2. Of those that a mesh axis runs over, the one named last changes fastest.
Arguments:
- state: float32 [8, 4, 16, 64, 1024], P('ens', None, None, 'gy', 'gz'), parts along dimension 0, may hold values from -32 to 32
- member_set: int32 [8], P('ens'), parts along dimension 0, may hold values from 0 to 15
- courant_table: float32 [16, 3], replicated, may hold values from -0.3 to 0.3
- diffusion_table: float32 [16, 4], replicated, may hold values from 0.05 to 1
- reaction_table: float32 [16, 4, 4], replicated, may hold values from -3 to 3
- quadratic_table: float32 [16, 4], replicated, may hold values from -1 to 1
Outputs:
- state_out: float32 [8, 4, 16, 64, 1024], P('ens', None, None, 'gy', 'gz'), parts along dimension 0
The draws below stay inside these ranges and needn't reach their ends.
There are 8 independent parts, one for each index of `ens`. The reference program is written for one: setup_inputs(seed, part) draws one part's arguments, and reference() takes and returns one part's arrays. A program takes and returns all parts, laid end to end along the dimension named above; an argument that names none is the same for every part. Nothing has to cross between parts.
All inputs are finite; a program needn't handle non-finite values.
Results may differ from the reference program's by a relative error of at most 0.00024.
Values sent between devices are 32-bit elements; how exact they have to be, the bound alone decides.
No kernel may reach another device: no remote copies, remote signals or barrier semaphores. Data moves between devices by JAX's collectives and lax.ppermute only.
A program may use at most 64 MiB of HBM per device.

```python
import math
import jax
import jax.numpy as jnp
from jax import lax

SPECIES = 4
SETS = 16
ITERS = 4
MEMBERS = 1
NX = 16
NY = 64
NZ = 1024


def draw_state(key, part):
    noise_key, y_key, z_key = jax.random.split(key, 3)
    dims_all = (MEMBERS, SPECIES, NX, NY, NZ)
    rising = jnp.arange(NZ, dtype=jnp.float32) / NZ
    jitter_y = jax.random.uniform(y_key, (NY,), minval=0.0, maxval=1.0)
    jitter_z = jax.random.uniform(z_key, (NZ,), minval=0.0, maxval=1.0)
    log_scale = math.log(3.0) * rising[None, :] + 0.5 * math.log(10.0) * (jitter_y[:, None] + jitter_z[None, :] - 1.0)
    magnitude = jnp.exp(log_scale)
    baseline = jax.random.normal(noise_key, dims_all)
    return jnp.clip(baseline * magnitude[None, None, None, :, :], -32.0, 32.0).astype(jnp.float32)


def gaussian(stream_key, dims, width, limit, kind=jnp.bfloat16):
    result = jax.random.normal(stream_key, dims, jnp.float32) * width
    return jnp.minimum(jnp.maximum(result, -limit), limit).astype(kind)


def setup_inputs(seed: int = 0, part: int = 0) -> dict:
    seeds = jax.random.split(jax.random.key(seed), 7)
    part_keys = jax.random.split(jax.random.fold_in(seeds[6], part), 7)
    return {
        "state": draw_state(jax.random.fold_in(jax.random.fold_in(seeds[6], part), 71), part),
        "member_set": jax.random.randint(part_keys[1], (MEMBERS,), 0, SETS).astype(jnp.int32),
        "courant_table": jnp.clip(jax.random.uniform(seeds[2], (SETS, 3), jnp.float32, -0.3, 0.3), -0.3, 0.3),
        "diffusion_table": jnp.clip(jnp.exp(jax.random.uniform(seeds[3], (SETS, SPECIES), jnp.float32, math.log(0.05), math.log(1.0))), 0.05, 1.0),
        "reaction_table": gaussian(seeds[4], (SETS, SPECIES, SPECIES), 0.3, 3.0, jnp.float32),
        "quadratic_table": jnp.clip(jax.random.uniform(seeds[5], (SETS, SPECIES), jnp.float32, -1.0, 1.0), -1.0, 1.0),
    }


def lookup(member_set, coeff_table):
    onehot = (member_set[:, None] == jnp.arange(coeff_table.shape[0], dtype=jnp.int32)[None, :]).astype(coeff_table.dtype)
    flattened = coeff_table.reshape(coeff_table.shape[0], -1)
    picked = lax.optimization_barrier(jnp.sum(onehot[:, :, None] * flattened[None, :, :], axis=1))
    return picked.reshape((member_set.shape[0],) + coeff_table.shape[1:])

def spread_out(values):
    return values[:, None, None, None, None]

def beside_all(padded, spatial, offset):
    slicer = [slice(None), slice(None), slice(1, -1), slice(1, -1), slice(1, -1)]
    slicer[spatial] = slice(offset, padded.shape[spatial] - 2 + offset)
    return padded[tuple(slicer)]

def explicit_section(padded, current, courant, reaction, quadratic):
    running = current
    for spatial in range(3):
        velocity = spread_out(courant[:, spatial])
        behind = beside_all(padded, spatial + 2, 0)
        beyond = beside_all(padded, spatial + 2, 2)
        running = running - jnp.maximum(velocity, 0.0) * (current - behind) - jnp.minimum(velocity, 0.0) * (beyond - current)
    linear = jnp.einsum('mkl,mlxyz->mkxyz', reaction, current, precision=lax.Precision.HIGHEST)
    leading = current[:, 0]
    partner = current[:, 1]
    coupled = leading * partner / (1.0 + leading * leading + partner * partner)
    return running + linear + quadratic[:, :, None, None, None] * coupled[:, None]

def implicit_apply(padded, current, diffuse):
    beside = beside_all(padded, 2, 0) + beside_all(padded, 2, 2)
    beside = beside + beside_all(padded, 3, 0) + beside_all(padded, 3, 2)
    beside = beside + beside_all(padded, 4, 0) + beside_all(padded, 4, 2)
    strength = diffuse[:, :, None, None, None]
    return (1.0 + 6.0 * strength) * current - strength * beside

def inner_product(left_side, right_side):
    return lax.optimization_barrier(jnp.sum(left_side * right_side, axis=(1, 2, 3, 4)))

def least_squares(hessen, beta, iters):
    target = [beta] + [jnp.zeros_like(beta)] * iters
    cosines = []
    sine_list = []
    triangle = []
    for column in range(iters):
        entries = list(hessen[column])
        for earlier in range(column):
            rotated = cosines[earlier] * entries[earlier] + sine_list[earlier] * entries[earlier + 1]
            entries[earlier + 1] = -sine_list[earlier] * entries[earlier] + cosines[earlier] * entries[earlier + 1]
            entries[earlier] = rotated
        radius = jnp.sqrt(entries[column] * entries[column] + entries[column + 1] * entries[column + 1])
        cosine = entries[column] / radius
        sine_val = entries[column + 1] / radius
        entries[column] = radius
        target[column + 1] = -sine_val * target[column]
        target[column] = cosine * target[column]
        cosines.append(cosine)
        sine_list.append(sine_val)
        triangle.append(entries[:column + 1])
    coeffs = [None] * iters
    for column in reversed(range(iters)):
        running = target[column]
        for further in range(column + 1, iters):
            running = running - triangle[further][column] * coeffs[further]
        coeffs[column] = running / triangle[column][column]
    return coeffs

def full_pad(current):
    return jnp.pad(current, ((0, 0), (0, 0), (1, 1), (1, 1), (1, 1)))

def reference(state, member_set, courant_table, diffusion_table, reaction_table, quadratic_table):
    courant = lookup(member_set, courant_table)
    diffuse = lookup(member_set, diffusion_table)
    reaction = lookup(member_set, reaction_table)
    quadratic = lookup(member_set, quadratic_table)
    source = explicit_section(full_pad(state), state, courant, reaction, quadratic)
    beta = jnp.sqrt(inner_product(source, source))
    basis = [source * spread_out(1.0 / beta)]
    hessen = []
    for column in range(ITERS):
        image = implicit_apply(full_pad(basis[column]), basis[column], diffuse)
        projections = [inner_product(basis[earlier], image) for earlier in range(column + 1)]
        remainder = image
        for earlier in range(column + 1):
            remainder = remainder - spread_out(projections[earlier]) * basis[earlier]
        norm_next = jnp.sqrt(inner_product(remainder, remainder))
        hessen.append(projections + [norm_next])
        if column + 1 < ITERS:
            basis.append(remainder * spread_out(1.0 / norm_next))
    coeffs = least_squares(hessen, beta, ITERS)
    state_out = spread_out(coeffs[0]) * basis[0]
    for column in range(1, ITERS):
        state_out = state_out + spread_out(coeffs[column]) * basis[column]
    return state_out
```

```python
import functools

import jax
import jax.numpy as jnp
from jax import lax
from jax.experimental import pallas as pl
from jax.experimental.pallas import tpu as pltpu
from jax.sharding import PartitionSpec as P

SPECIES = 4
X = 16
Y = 16
Z = 128
HALO = 5
GROUP = 6
PACKS = 3
ROWS = Y + 2 * HALO
DOTS = 13
SLOTS = 16

F32 = jnp.float32
VMEM = pltpu.VMEM
SMEM = pltpu.SMEM


def struct(*shape):
    return jax.ShapeDtypeStruct(shape, F32)


def lanes():
    return lax.broadcasted_iota(jnp.int32, (X, Z), 1)


def shift(v, amount):
    amount %= Z
    return pltpu.roll(v, amount, 1) if amount else v


def own(state_ref, s, y):
    return state_ref[pl.ds(s * X * Y + y, X, stride=Y), :]


def over_rows(count, at_once, body, carry=None):
    def step(i, c):
        for k in range(at_once):
            c = body(i * at_once + k, c)
        return c

    whole = count // at_once
    carry = lax.fori_loop(0, whole, step, carry)
    for row in range(whole * at_once, count):
        carry = body(row, carry)
    return carry


def pack_kernel(state_ref, top_ref, bottom_ref, strip_ref, far_ref, near_ref):
    lane = lanes()
    odd = lax.axis_index("gz") % 2 == 1
    place = lane % 32
    for y in range(Y):
        total = jnp.zeros((X, Z), F32)
        for s in range(SPECIES):
            v = own(state_ref, s, y)
            if y < HALO:
                top_ref[y, s] = v
            if y >= Y - HALO:
                bottom_ref[y - (Y - HALO), s] = v
            low = shift(v, 32 * s + HALO)
            high = shift(v, 32 * s + 16 - (Z - 11))
            total = jnp.where((lane >= 32 * s + HALO) & (lane < 32 * s + 16), low, total)
            total = jnp.where((lane >= 32 * s + 16) & (lane < 32 * s + 27), high, total)
        strip_ref[y] = total
    for g in range(PACKS):
        lows = jnp.zeros((X, Z), F32)
        highs = jnp.zeros((X, Z), F32)
        for i in range(GROUP):
            if g * GROUP + i < Y:
                v = strip_ref[g * GROUP + i]
                here = (place >= i * HALO) & (place < (i + 1) * HALO)
                lows = jnp.where(here, shift(v, i * HALO - HALO), lows)
                highs = jnp.where(here, shift(v, i * HALO - 22), highs)
        far_ref[g] = jnp.where(odd, highs, lows)
        near_ref[g] = jnp.where(odd, lows, highs)


def unpack_kernel(strip_ref, far_ref, near_ref, full_ref, top_ref, bottom_ref):
    place = lanes() % 32
    odd = lax.axis_index("gz") % 2 == 1
    for g in range(PACKS):
        far, near = far_ref[g], near_ref[g]
        after = jnp.where(odd, far, near)
        before = jnp.where(odd, near, far)
        for i in range(GROUP):
            y = g * GROUP + i
            if y < Y:
                v = strip_ref[y]
                v = jnp.where(place < HALO, shift(before, -i * HALO), v)
                v = jnp.where(place >= 27, shift(after, 27 - i * HALO), v)
                full_ref[y] = v
                if y < HALO:
                    top_ref[y] = v
                if y >= Y - HALO:
                    bottom_ref[y - (Y - HALO)] = v


def beside_x(v):
    row = lax.broadcasted_iota(jnp.int32, (X, Z), 0)
    below = jnp.where(row == 0, 0.0, pltpu.roll(v, 1, 0))
    above = jnp.where(row == X - 1, 0.0, pltpu.roll(v, X - 1, 0))
    return below, above


def in_grid():
    low = jnp.where(lax.axis_index("gy") > 0, 1.0, 0.0).astype(F32)
    high = jnp.where(lax.axis_index("gy") < lax.axis_size("gy") - 1, 1.0, 0.0).astype(F32)
    return low, high


def row_flag(row, before, low, high):
    flag = jnp.where(row < before, low, 1.0)
    return jnp.where(row >= before + Y, high, flag)


def one_row(value):
    return jnp.full((1, Z), value, F32)


def largest(diffusion_ref, member):
    d = [diffusion_ref[member, s] for s in range(SPECIES)]
    return d, jnp.maximum(jnp.maximum(d[0], d[1]), jnp.maximum(d[2], d[3]))


def dot_terms(b):
    pairs = ((0, 0), (0, 1), (0, 3), (0, 4), (1, 1), (1, 2), (1, 3), (1, 4), (2, 2), (2, 3), (3, 3), (3, 4), (4, 4))
    out = []
    for i, j in pairs:
        p = b[i] * b[j]
        out.append(p[:8] + p[8:])
    return out


def level_value(k, image, v, before):
    if k < 3:
        return image
    if k == 3:
        return image - v
    return 2.0 * (image - v) - before


def main_kernel(
    state_ref, low_ref, high_ref, member_ref, courant_ref, diffusion_ref, reaction_ref, quadratic_ref,
    basis_ref, dots_ref, wide, b0, b1, b2, b3,
):
    member = member_ref[0]
    low, high = in_grid()
    for r in range(HALO):
        for s in range(SPECIES):
            wide[r, s] = low_ref[r, s] * low
            wide[HALO + Y + r, s] = high_ref[r, s] * high
    for y in range(Y):
        for s in range(SPECIES):
            wide[HALO + y, s] = own(state_ref, s, y)

    courant = [courant_ref[member, d] for d in range(3)]
    plus = [jnp.maximum(c, 0.0) for c in courant]
    minus = [jnp.minimum(c, 0.0) for c in courant]
    kept = 1.0 - (plus[0] - minus[0]) - (plus[1] - minus[1]) - (plus[2] - minus[2])
    linear = [[reaction_ref[member, 4 * k + l] for l in range(SPECIES)] for k in range(SPECIES)]
    for k in range(SPECIES):
        linear[k][k] = linear[k][k] + kept
    quad = [quadratic_ref[member, k] for k in range(SPECIES)]

    def source_row(row, _):
        flag = row_flag(row, HALO - 1, low, high)
        v = [wide[row + 1, s] for s in range(SPECIES)]
        a, b = v[0], v[1]
        coupled = a * b / (1.0 + a * a + b * b)
        for k in range(SPECIES):
            below, above = beside_x(v[k])
            out = plus[0] * below - minus[0] * above
            out = out + (plus[1] * wide[row, k] - minus[1] * wide[row + 2, k])
            out = out + (plus[2] * shift(v[k], 1) - minus[2] * shift(v[k], -1))
            for l in range(SPECIES):
                out = out + linear[k][l] * v[l]
            b0[row, k] = (out + quad[k] * coupled) * flag
        return _

    over_rows(Y + 8, 4, source_row)

    d, most = largest(diffusion_ref, member)
    scale = [one_row(d[s]) / one_row(6.0 * most) for s in range(SPECIES)]

    buffers = [b0, b1, b2, b3]

    def image_of(ref, row, s):
        v = ref[row + 1, s]
        below, above = beside_x(v)
        beside = (below + above) + (ref[row, s] + ref[row + 2, s]) + (shift(v, 1) + shift(v, -1))
        return scale[s] * (6.0 * v - beside), v

    for k in (1, 2, 3):
        before = 4 - k

        def level_row(row, _, k=k, before=before):
            flag = row_flag(row, before, low, high)
            for s in range(SPECIES):
                image, v = image_of(buffers[k - 1], row, s)
                buffers[k][row, s] = level_value(k, image, v, None) * flag
            return _

        over_rows(Y + 2 * before, 4, level_row)

    def last_row(row, sums):
        sums = list(sums)
        for s in range(SPECIES):
            image, v = image_of(b3, row, s)
            b = [buffers[k][row + 4 - k, s] for k in range(4)]
            for k in range(4):
                basis_ref[k, row, s] = b[k]
            b.append(level_value(4, image, v, b[2]))
            sums = [t + p for t, p in zip(sums, dot_terms(b))]
        return tuple(sums)

    sums = over_rows(Y, 2, last_row, tuple(jnp.zeros((8, Z), F32) for _ in range(DOTS)))
    lane = lax.broadcasted_iota(jnp.int32, (8, Z), 1)
    inner = (lane >= HALO) & (lane < Z - HALO)
    for k in range(DOTS):
        dots_ref[k] = jnp.where(inner, sums[k], 0.0)


def strip_kernel(
    strip_ref, low_ref, high_ref, dots_in_ref, member_ref, courant_ref, diffusion_ref, reaction_ref, quadratic_ref,
    basis_ref, total_ref, wide, b0, b1, b2, b3,
):
    member = member_ref[0]
    low, high = in_grid()
    for r in range(HALO):
        wide[r] = low_ref[r] * low
        wide[HALO + Y + r] = high_ref[r] * high
    for y in range(Y):
        wide[HALO + y] = strip_ref[y]

    lane = lax.broadcasted_iota(jnp.int32, (1, Z), 1)
    place = lane % 32

    def by_species(values):
        out = one_row(values[3])
        for s in (2, 1, 0):
            out = jnp.where(lane < 32 * (s + 1), values[s], out)
        return out

    first = jnp.where(lax.axis_index("gz") > 0, 1.0, 0.0).astype(F32)
    last = jnp.where(lax.axis_index("gz") < lax.axis_size("gz") - 1, 1.0, 0.0).astype(F32)
    inside = jnp.where(place < HALO, first, jnp.where(place >= 27, last, one_row(1.0)))

    courant = [courant_ref[member, d] for d in range(3)]
    plus = [jnp.maximum(c, 0.0) for c in courant]
    minus = [jnp.minimum(c, 0.0) for c in courant]
    kept = 1.0 - (plus[0] - minus[0]) - (plus[1] - minus[1]) - (plus[2] - minus[2])
    linear = [
        by_species([reaction_ref[member, 4 * k + (k - t) % SPECIES] for k in range(SPECIES)]) for t in range(SPECIES)
    ]
    linear[0] = linear[0] + kept
    quad = by_species([quadratic_ref[member, k] for k in range(SPECIES)])

    def source_row(row, _):
        flag = row_flag(row, HALO - 1, low, high)
        v = wide[row + 1]
        turned = [v] + [shift(v, 32 * t) for t in range(1, SPECIES)]
        b = turned[3]
        coupled = v * b / (1.0 + v * v + b * b)
        coupled = jnp.where(lane < 32, coupled, 0.0)
        coupled = coupled + shift(coupled, 32)
        coupled = coupled + shift(coupled, 64)
        below, above = beside_x(v)
        out = plus[0] * below - minus[0] * above
        out = out + (plus[1] * wide[row] - minus[1] * wide[row + 2])
        out = out + (plus[2] * shift(v, 1) - minus[2] * shift(v, -1))
        for t in range(SPECIES):
            out = out + linear[t] * turned[t]
        b0[row] = (out + quad * coupled) * (flag * inside)
        return _

    over_rows(Y + 8, 12, source_row)

    d, most = largest(diffusion_ref, member)
    scale = by_species(d) / one_row(6.0 * most)
    buffers = [b0, b1, b2, b3]

    def image_of(ref, row):
        v = ref[row + 1]
        below, above = beside_x(v)
        beside = (below + above) + (ref[row] + ref[row + 2]) + (shift(v, 1) + shift(v, -1))
        return scale * (6.0 * v - beside), v

    for k in (1, 2, 3):
        before = 4 - k

        def level_row(row, _, k=k, before=before):
            flag = row_flag(row, before, low, high)
            image, v = image_of(buffers[k - 1], row)
            buffers[k][row] = level_value(k, image, v, None) * (flag * inside)
            return _

        over_rows(Y + 2 * before, 11 if k == 1 else 10 if k == 2 else 9, level_row)

    def last_row(row, sums):
        image, v = image_of(b3, row)
        b = [buffers[k][row + 4 - k] for k in range(4)]
        for k in range(4):
            basis_ref[k, row] = b[k]
        b.append(level_value(4, image, v, b[2]))
        return tuple(t + p for t, p in zip(sums, dot_terms(b)))

    sums = over_rows(Y, 8, last_row, tuple(jnp.zeros((8, Z), F32) for _ in range(DOTS)))
    edge = ((place >= HALO) & (place < 2 * HALO)) | ((place >= 22) & (place < 27))
    slot = lax.broadcasted_iota(jnp.int32, (8, SLOTS), 1)
    total = jnp.zeros((8, SLOTS), F32)
    for k in range(DOTS):
        both = jnp.where(edge, sums[k], 0.0) + dots_in_ref[k]
        one = jnp.sum(jnp.sum(both, axis=0, keepdims=True), axis=1, keepdims=True)
        total = jnp.where(slot == k, one, total)
    for i in range(total_ref.shape[0] // 8):
        total_ref[8 * i : 8 * i + 8, :] = total


def least_squares(h, r):
    n = 5
    root = [[None] * n for _ in range(n)]
    for i in range(n):
        rest = h[i][i]
        for k in range(i):
            rest = rest - root[k][i] * root[k][i]
        rest = jnp.maximum(rest, 3e-7 * h[i][i])
        inverse = 1.0 / jnp.sqrt(rest)
        root[i][i] = rest * inverse
        for j in range(i + 1, n):
            t = h[i][j]
            for k in range(i):
                t = t - root[k][i] * root[k][j]
            root[i][j] = t * inverse
    wide = 1.0 + r
    half = 0.5 * r
    columns = []
    for j, weights in enumerate((((0, 1.0), (1, r)), ((1, 1.0), (2, r)), ((2, wide), (3, r)), ((2, half), (3, wide), (4, half)))):
        column = []
        for i in range(j + 2):
            terms = [w * root[i][m] for m, w in weights if i <= m]
            column.append(sum(terms[1:], terms[0]))
        columns.append(column)
    target = [root[0][0]]
    cosines, sines = [], []
    for j in range(4):
        e = columns[j]
        for i in range(j):
            e[i], e[i + 1] = cosines[i] * e[i] + sines[i] * e[i + 1], cosines[i] * e[i + 1] - sines[i] * e[i]
        inverse = 1.0 / jnp.sqrt(e[j] * e[j] + e[j + 1] * e[j + 1])
        cosines.append(e[j] * inverse)
        sines.append(e[j + 1] * inverse)
        e[j] = cosines[j] * e[j] + sines[j] * e[j + 1]
        target.append(-sines[j] * target[j])
        target[j] = cosines[j] * target[j]
    y = [None] * 4
    for j in (3, 2, 1, 0):
        t = target[j]
        for k in range(j + 1, 4):
            t = t - columns[k][j] * y[k]
        y[j] = t / columns[j][j]
    return y


def combine_kernel(sums_ref, member_ref, diffusion_ref, basis_ref, strip_ref, out_ref):
    total = jnp.sum(sums_ref[...], axis=0, keepdims=True)
    p = [total[:, k : k + 1] for k in range(DOTS)]
    h00, h01, h03, h04, h11, h12, h13, h14, h22, h23, h33, h34, h44 = p
    h = [
        [h00, h01, h11, h03, h04],
        [None, h11, h12, h13, h14],
        [None, None, h22, h23, 2.0 * h33 - h22],
        [None, None, None, h33, h34],
        [None, None, None, None, h44],
    ]
    _, most = largest(diffusion_ref, member_ref[0])
    y = [jnp.broadcast_to(c, (X, Z)) for c in least_squares(h, 6.0 * most)]
    lane = lanes()
    for row in range(Y):
        strip = y[0] * strip_ref[0, row]
        for k in (1, 2, 3):
            strip = strip + y[k] * strip_ref[k, row]
        for s in range(SPECIES):
            v = y[0] * basis_ref[0, row, s]
            for k in (1, 2, 3):
                v = v + y[k] * basis_ref[k, row, s]
            v = jnp.where(lane < HALO, shift(strip, -(32 * s + HALO)), v)
            v = jnp.where(lane >= Z - HALO, shift(strip, Z - HALO - (32 * s + 22)), v)
            out_ref[pl.ds(s * X * Y + row, X, stride=Y), :] = v


def call(kernel, outs, spaces, scratch=(), flops=1000):
    return pl.pallas_call(
        kernel,
        out_shape=outs,
        in_specs=[pl.BlockSpec(memory_space=m) for m in spaces],
        out_specs=jax.tree.map(lambda _: pl.BlockSpec(memory_space=VMEM), outs),
        scratch_shapes=list(scratch),
        cost_estimate=pl.CostEstimate(flops=flops, bytes_accessed=1 << 20, transcendentals=0),
        compiler_params=pltpu.CompilerParams(vmem_limit_bytes=24 << 20),
    )


def shards(state, member_set, courant_table, diffusion_table, reaction_table, quadratic_table):
    gy, gz = lax.axis_size("gy"), lax.axis_size("gz")
    up = [(i, (i + 1) % gy) for i in range(gy)]
    down = [(b, a) for a, b in up]
    far, near = [], []
    for i in range(gz - 1):
        (far if i % 2 else near).extend([(i, i + 1), (i + 1, i)])
    flat = state.reshape(SPECIES * X * Y, Z)
    tables = (courant_table, diffusion_table, reaction_table.reshape(-1, SPECIES * SPECIES), quadratic_table)

    edge = struct(HALO, SPECIES, X, Z)
    strip_edge = struct(HALO, X, Z)
    pack = struct(PACKS, X, Z)
    top, bottom, strip, to_far, to_near = call(
        pack_kernel, (edge, edge, struct(Y, X, Z), pack, pack), [VMEM]
    )(flat)
    from_far = lax.ppermute(to_far, "gz", far)
    from_near = lax.ppermute(to_near, "gz", near)
    low = lax.ppermute(bottom, "gy", up)
    high = lax.ppermute(top, "gy", down)
    strip, strip_top, strip_bottom = call(
        unpack_kernel, (struct(Y, X, Z), strip_edge, strip_edge), [VMEM] * 3
    )(strip, from_far, from_near)
    strip_low = lax.ppermute(strip_bottom, "gy", up)
    strip_high = lax.ppermute(strip_top, "gy", down)

    wide = (SPECIES, X, Z)
    basis, dots = call(
        main_kernel,
        (struct(4, Y, *wide), struct(DOTS, 8, Z)),
        [VMEM] * 3 + [SMEM] * 5,
        [VMEM((n, *wide), F32) for n in (ROWS, Y + 8, Y + 6, Y + 4, Y + 2)],
        flops=10_000_000,
    )(flat, low, high, member_set, *tables)
    strip_basis, total = call(
        strip_kernel,
        (struct(4, Y, X, Z), struct(gy * gz, SLOTS)),
        [VMEM] * 4 + [SMEM] * 5,
        [VMEM((n, X, Z), F32) for n in (ROWS, Y + 8, Y + 6, Y + 4, Y + 2)],
    )(strip, strip_low, strip_high, dots, member_set, *tables)
    sums = lax.all_to_all(total, ("gy", "gz"), split_axis=0, concat_axis=0, tiled=True)
    out = call(
        combine_kernel, struct(SPECIES * X * Y, Z), [VMEM, SMEM, SMEM, VMEM, VMEM]
    )(sums, member_set, diffusion_table, basis, strip_basis)
    return out.reshape(state.shape)


def solution(mesh):
    return jax.shard_map(
        shards,
        mesh=mesh,
        in_specs=(P("ens", None, None, "gy", "gz"), P("ens"), P(), P(), P(), P()),
        out_specs=P("ens", None, None, "gy", "gz"),
        check_vma=False,
    )
```

```python
import jax
import jax.numpy as jnp
from jax import lax
from jax.experimental import pallas as pl
from jax.experimental.pallas import tpu as pltpu
from jax.sharding import PartitionSpec as P


SPECIES = 4
X = 16
Y = 16
Z = 128
HALO = 5
GROUP = 6
PACKS = 3
ROWS = Y + 2 * HALO
DOTS = 13
SLOTS = 16

F32 = jnp.float32
VMEM = pltpu.VMEM


def struct(*shape):
    return jax.ShapeDtypeStruct(shape, F32)


def lanes():
    return lax.broadcasted_iota(jnp.int32, (X, Z), 1)


def shift(v, amount):
    amount %= Z
    return pltpu.roll(v, amount, 1) if amount else v


def over_rows(count, at_once, body, carry=None):
    if at_once >= count:
        for row in range(count):
            carry = body(row, carry)
        return carry

    def step(i, c):
        for k in range(at_once):
            c = body(i * at_once + k, c)
        return c

    whole = count // at_once
    carry = lax.fori_loop(0, whole, step, carry)
    for row in range(whole * at_once, count):
        carry = body(row, carry)
    return carry


def pack_kernel(state_ref, own_ref, top_ref, bottom_ref, strip_ref, far_ref, near_ref, held, sems):
    lane = lanes()
    odd = lax.axis_index("gz") % 2 == 1
    place = lane % 32
    copies = [pltpu.make_async_copy(state_ref.at[s], held.at[s], sems.at[s]) for s in range(SPECIES)]
    for copy in copies:
        copy.start()
    for s in range(SPECIES):
        copies[s].wait()
        for y in range(Y):
            v = held[s, pl.ds(y, X, stride=Y), :]
            own_ref[y, s] = v
            if y < HALO:
                top_ref[y, s] = v
            if y >= Y - HALO:
                bottom_ref[y - (Y - HALO), s] = v
            total = strip_ref[y] if s else jnp.zeros((X, Z), F32)
            low = shift(v, 32 * s + HALO)
            high = shift(v, 32 * s + 16 - (Z - 11))
            total = jnp.where((lane >= 32 * s + HALO) & (lane < 32 * s + 16), low, total)
            total = jnp.where((lane >= 32 * s + 16) & (lane < 32 * s + 27), high, total)
            strip_ref[y] = total
    for g in range(PACKS):
        lows = jnp.zeros((X, Z), F32)
        highs = jnp.zeros((X, Z), F32)
        for i in range(GROUP):
            if g * GROUP + i < Y:
                v = strip_ref[g * GROUP + i]
                here = (place >= i * HALO) & (place < (i + 1) * HALO)
                lows = jnp.where(here, shift(v, i * HALO - HALO), lows)
                highs = jnp.where(here, shift(v, i * HALO - 22), highs)
        far_ref[g] = jnp.where(odd, highs, lows)
        near_ref[g] = jnp.where(odd, lows, highs)


def unpack_kernel(strip_ref, far_ref, near_ref, full_ref, top_ref, bottom_ref):
    place = lanes() % 32
    odd = lax.axis_index("gz") % 2 == 1
    for g in range(PACKS):
        far, near = far_ref[g], near_ref[g]
        after = jnp.where(odd, far, near)
        before = jnp.where(odd, near, far)
        for i in range(GROUP):
            y = g * GROUP + i
            if y < Y:
                v = strip_ref[y]
                v = jnp.where(place < HALO, shift(before, -i * HALO), v)
                v = jnp.where(place >= 27, shift(after, 27 - i * HALO), v)
                full_ref[y] = v
                if y < HALO:
                    top_ref[y] = v
                if y >= Y - HALO:
                    bottom_ref[y - (Y - HALO)] = v


def beside_x(v):
    row = lax.broadcasted_iota(jnp.int32, (X, Z), 0)
    below = jnp.where(row == 0, 0.0, pltpu.roll(v, 1, 0))
    above = jnp.where(row == X - 1, 0.0, pltpu.roll(v, X - 1, 0))
    return below, above


def in_grid():
    low = jnp.where(lax.axis_index("gy") > 0, 1.0, 0.0).astype(F32)
    high = jnp.where(lax.axis_index("gy") < lax.axis_size("gy") - 1, 1.0, 0.0).astype(F32)
    return low, high


def row_flag(row, before, low, high):
    if isinstance(row, int):
        return low if row < before else high if row >= before + Y else 1.0
    flag = jnp.where(row < before, low, 1.0)
    return jnp.where(row >= before + Y, high, flag)


PLUS, MINUS, LINEAR, QUAD, SCALE, TURNED, STRIP_QUAD, STRIP_SCALE, RANGE = 0, 3, 6, 22, 26, 30, 34, 35, 36
COEFFICIENTS = 40


def coefficient_kernel(member_ref, courant_ref, diffusion_ref, reaction_ref, quadratic_ref, out_ref):
    sets = courant_ref.shape[-1]
    hot = lax.broadcasted_iota(jnp.int32, (1, sets), 1) == member_ref[...]

    def picked(table):
        return jnp.sum(jnp.where(hot, table, 0.0), axis=1, keepdims=True)

    def put(row, value):
        out_ref[row : row + 1, :] = jnp.broadcast_to(value, (1, Z))

    lane = lax.broadcasted_iota(jnp.int32, (1, Z), 1)

    def by_species(values):
        out = jnp.broadcast_to(values[3], (1, Z))
        for s in (2, 1, 0):
            out = jnp.where(lane < 32 * (s + 1), values[s], out)
        return out

    courant = picked(courant_ref[...])
    plus, minus = jnp.maximum(courant, 0.0), jnp.minimum(courant, 0.0)
    kept = jnp.ones((1, 1), F32)
    for d in range(3):
        put(PLUS + d, plus[d : d + 1])
        put(MINUS + d, minus[d : d + 1])
        kept = kept - (plus[d : d + 1] - minus[d : d + 1])
    linear = []
    for k in range(SPECIES):
        rates = picked(reaction_ref[k])
        linear.append([rates[l : l + 1] for l in range(SPECIES)])
        linear[k][k] = linear[k][k] + kept
        for l in range(SPECIES):
            put(LINEAR + SPECIES * k + l, linear[k][l])
    for t in range(SPECIES):
        put(TURNED + t, by_species([linear[k][(k - t) % SPECIES] for k in range(SPECIES)]))
    rates = picked(quadratic_ref[...])
    quad = [rates[k : k + 1] for k in range(SPECIES)]
    d = picked(diffusion_ref[...])
    d = [d[k : k + 1] for k in range(SPECIES)]
    reach = 6.0 * jnp.maximum(jnp.maximum(d[0], d[1]), jnp.maximum(d[2], d[3]))
    scale = [v / reach for v in d]
    for k in range(SPECIES):
        put(QUAD + k, quad[k])
        put(SCALE + k, scale[k])
    put(STRIP_QUAD, by_species(quad))
    put(STRIP_SCALE, by_species(scale))
    put(RANGE, reach)


def spread(table_ref, row):
    return jnp.broadcast_to(table_ref[row : row + 1, :], (X, Z))


def dot_terms(b):
    pairs = ((0, 0), (0, 1), (0, 3), (0, 4), (1, 1), (1, 2), (1, 3), (1, 4), (2, 2), (2, 3), (3, 3), (3, 4), (4, 4))
    out = []
    for i, j in pairs:
        p = b[i] * b[j]
        out.append(p[:8] + p[8:])
    return out


def level_value(k, image, v, before):
    if k < 3:
        return image
    if k == 3:
        return image - v
    return 2.0 * (image - v) - before


def main_kernel(own_ref, low_ref, high_ref, table_ref, basis_ref, dots_ref, wide, b0, b1, b2, b3):
    low, high = in_grid()
    for r in range(HALO):
        for s in range(SPECIES):
            wide[r, s] = low_ref[r, s] * low
            wide[HALO + Y + r, s] = high_ref[r, s] * high
    for y in range(Y):
        for s in range(SPECIES):
            wide[HALO + y, s] = own_ref[y, s]

    plus = [spread(table_ref, PLUS + d) for d in range(3)]
    minus = [spread(table_ref, MINUS + d) for d in range(3)]
    linear = [[spread(table_ref, LINEAR + SPECIES * k + l) for l in range(SPECIES)] for k in range(SPECIES)]
    quad = [spread(table_ref, QUAD + k) for k in range(SPECIES)]

    def source_row(row, _):
        flag = row_flag(row, HALO - 1, low, high)
        v = [wide[row + 1, s] for s in range(SPECIES)]
        a, b = v[0], v[1]
        coupled = a * b / (1.0 + a * a + b * b)
        for k in range(SPECIES):
            below, above = beside_x(v[k])
            out = plus[0] * below - minus[0] * above
            out = out + (plus[1] * wide[row, k] - minus[1] * wide[row + 2, k])
            out = out + (plus[2] * shift(v[k], 1) - minus[2] * shift(v[k], -1))
            for l in range(SPECIES):
                out = out + linear[k][l] * v[l]
            b0[row, k] = (out + quad[k] * coupled) * flag
        return _

    over_rows(Y + 8, 4, source_row)

    scale = [spread(table_ref, SCALE + s) for s in range(SPECIES)]
    buffers = [b0, b1, b2, b3]

    def image_of(ref, row, s):
        v = ref[row + 1, s]
        below, above = beside_x(v)
        beside = (below + above) + (ref[row, s] + ref[row + 2, s]) + (shift(v, 1) + shift(v, -1))
        return scale[s] * (6.0 * v - beside), v

    for k in (1, 2, 3):
        before = 4 - k

        def level_row(row, _, k=k, before=before):
            flag = row_flag(row, before, low, high)
            for s in range(SPECIES):
                image, v = image_of(buffers[k - 1], row, s)
                buffers[k][row, s] = level_value(k, image, v, None) * flag
            return _

        over_rows(Y + 2 * before, 4, level_row)

    def last_row(row, sums):
        sums = list(sums)
        for s in range(SPECIES):
            image, v = image_of(b3, row, s)
            b = [buffers[k][row + 4 - k, s] for k in range(4)]
            for k in range(4):
                basis_ref[k, row, s] = b[k]
            b.append(level_value(4, image, v, b[2]))
            sums = [t + p for t, p in zip(sums, dot_terms(b))]
        return tuple(sums)

    sums = over_rows(Y, 2, last_row, tuple(jnp.zeros((8, Z), F32) for _ in range(DOTS)))
    lane = lax.broadcasted_iota(jnp.int32, (8, Z), 1)
    inner = (lane >= HALO) & (lane < Z - HALO)
    for k in range(DOTS):
        dots_ref[k] = jnp.where(inner, sums[k], 0.0)


def strip_kernel(
    strip_ref, low_ref, high_ref, dots_in_ref, table_ref, basis_ref, total_ref, wide, b0, b1, b2, b3
):
    low, high = in_grid()
    for r in range(HALO):
        wide[r] = low_ref[r] * low
        wide[HALO + Y + r] = high_ref[r] * high
    for y in range(Y):
        wide[HALO + y] = strip_ref[y]

    lane = lanes()
    place = lane % 32
    first = jnp.where(lax.axis_index("gz") > 0, 1.0, 0.0).astype(F32)
    last = jnp.where(lax.axis_index("gz") < lax.axis_size("gz") - 1, 1.0, 0.0).astype(F32)
    inside = jnp.where(place < HALO, first, jnp.where(place >= 27, last, 1.0))
    plus = [spread(table_ref, PLUS + d) for d in range(3)]
    minus = [spread(table_ref, MINUS + d) for d in range(3)]
    linear = [spread(table_ref, TURNED + t) for t in range(SPECIES)]
    quad = spread(table_ref, STRIP_QUAD)

    def source_row(row, _):
        flag = row_flag(row, HALO - 1, low, high)
        v = wide[row + 1]
        turned = [v] + [shift(v, 32 * t) for t in range(1, SPECIES)]
        b = turned[3]
        coupled = v * b / (1.0 + v * v + b * b)
        coupled = jnp.where(lane < 32, coupled, 0.0)
        coupled = coupled + shift(coupled, 32)
        coupled = coupled + shift(coupled, 64)
        below, above = beside_x(v)
        out = plus[0] * below - minus[0] * above
        out = out + (plus[1] * wide[row] - minus[1] * wide[row + 2])
        out = out + (plus[2] * shift(v, 1) - minus[2] * shift(v, -1))
        for t in range(SPECIES):
            out = out + linear[t] * turned[t]
        b0[row] = (out + quad * coupled) * (flag * inside)
        return _

    over_rows(Y + 8, Y + 8, source_row)

    scale = spread(table_ref, STRIP_SCALE)
    buffers = [b0, b1, b2, b3]

    def image_of(ref, row):
        v = ref[row + 1]
        below, above = beside_x(v)
        beside = (below + above) + (ref[row] + ref[row + 2]) + (shift(v, 1) + shift(v, -1))
        return scale * (6.0 * v - beside), v

    for k in (1, 2, 3):
        before = 4 - k

        def level_row(row, _, k=k, before=before):
            flag = row_flag(row, before, low, high)
            image, v = image_of(buffers[k - 1], row)
            buffers[k][row] = level_value(k, image, v, None) * (flag * inside)
            return _

        over_rows(Y + 2 * before, Y + 2 * before, level_row)

    def last_row(row, sums):
        image, v = image_of(b3, row)
        b = [buffers[k][row + 4 - k] for k in range(4)]
        for k in range(4):
            basis_ref[k, row] = b[k]
        b.append(level_value(4, image, v, b[2]))
        return tuple(t + p for t, p in zip(sums, dot_terms(b)))

    sums = over_rows(Y, Y, last_row, tuple(jnp.zeros((8, Z), F32) for _ in range(DOTS)))
    place = place[:8]
    edge = ((place >= HALO) & (place < 2 * HALO)) | ((place >= 22) & (place < 27))
    slot = lax.broadcasted_iota(jnp.int32, (8, SLOTS), 1)
    total = jnp.broadcast_to(table_ref[RANGE : RANGE + 1, :SLOTS], (8, SLOTS))
    for k in range(DOTS):
        both = jnp.where(edge, sums[k], 0.0) + dots_in_ref[k]
        one = jnp.sum(jnp.sum(both, axis=0, keepdims=True), axis=1, keepdims=True)
        total = jnp.where(slot == k, one, total)
    for i in range(total_ref.shape[0] // 8):
        total_ref[8 * i : 8 * i + 8, :] = total


def least_squares(h, r):
    n = 5
    root = [[None] * n for _ in range(n)]
    for i in range(n):
        rest = h[i][i]
        for k in range(i):
            rest = rest - root[k][i] * root[k][i]
        rest = jnp.maximum(rest, 3e-7 * h[i][i])
        inverse = 1.0 / jnp.sqrt(rest)
        root[i][i] = rest * inverse
        for j in range(i + 1, n):
            t = h[i][j]
            for k in range(i):
                t = t - root[k][i] * root[k][j]
            root[i][j] = t * inverse
    wide = 1.0 + r
    half = 0.5 * r
    columns = []
    for j, weights in enumerate((((0, 1.0), (1, r)), ((1, 1.0), (2, r)), ((2, wide), (3, r)), ((2, half), (3, wide), (4, half)))):
        column = []
        for i in range(j + 2):
            terms = [w * root[i][m] for m, w in weights if i <= m]
            column.append(sum(terms[1:], terms[0]))
        columns.append(column)
    target = [root[0][0]]
    cosines, sines = [], []
    for j in range(4):
        e = columns[j]
        for i in range(j):
            e[i], e[i + 1] = cosines[i] * e[i] + sines[i] * e[i + 1], cosines[i] * e[i + 1] - sines[i] * e[i]
        inverse = 1.0 / jnp.sqrt(e[j] * e[j] + e[j + 1] * e[j + 1])
        cosines.append(e[j] * inverse)
        sines.append(e[j + 1] * inverse)
        e[j] = cosines[j] * e[j] + sines[j] * e[j + 1]
        target.append(-sines[j] * target[j])
        target[j] = cosines[j] * target[j]
    y = [None] * 4
    for j in (3, 2, 1, 0):
        t = target[j]
        for k in range(j + 1, 4):
            t = t - columns[k][j] * y[k]
        y[j] = t / columns[j][j]
    return y


def combine_kernel(sums_ref, basis_ref, strip_ref, out_ref, held, strips, sems):
    total = jnp.sum(sums_ref[...], axis=0, keepdims=True)
    h00, h01, h03, h04, h11, h12, h13, h14, h22, h23, h33, h34, h44 = (total[:, k : k + 1] for k in range(DOTS))
    h = [
        [h00, h01, h11, h03, h04],
        [None, h11, h12, h13, h14],
        [None, None, h22, h23, 2.0 * h33 - h22],
        [None, None, None, h33, h34],
        [None, None, None, None, h44],
    ]
    y = [jnp.broadcast_to(c, (X, Z)) for c in least_squares(h, sums_ref[0:1, DOTS : DOTS + 1])]
    lane = lanes()
    for row in range(Y):
        strip = y[0] * strip_ref[0, row]
        for k in (1, 2, 3):
            strip = strip + y[k] * strip_ref[k, row]
        strips[row] = strip
    copies = [pltpu.make_async_copy(held.at[s], out_ref.at[s], sems.at[s]) for s in range(SPECIES)]
    for s in range(SPECIES):
        for row in range(Y):
            v = y[0] * basis_ref[0, row, s]
            for k in (1, 2, 3):
                v = v + y[k] * basis_ref[k, row, s]
            strip = strips[row]
            v = jnp.where(lane < HALO, shift(strip, -(32 * s + HALO)), v)
            v = jnp.where(lane >= Z - HALO, shift(strip, Z - HALO - (32 * s + 22)), v)
            held[s, pl.ds(row, X, stride=Y), :] = v
        copies[s].start()
    for copy in copies:
        copy.wait()


def call(kernel, outs, spaces, scratch=(), flops=1000, out_space=VMEM):
    return pl.pallas_call(
        kernel,
        out_shape=outs,
        in_specs=[pl.BlockSpec(memory_space=m) for m in spaces],
        out_specs=jax.tree.map(lambda _: pl.BlockSpec(memory_space=out_space), outs),
        scratch_shapes=list(scratch),
        cost_estimate=pl.CostEstimate(flops=flops, bytes_accessed=1 << 20, transcendentals=0),
        compiler_params=pltpu.CompilerParams(vmem_limit_bytes=24 << 20),
    )


def shards(state, member_set, courant_table, diffusion_table, reaction_table, quadratic_table):
    gy, gz = lax.axis_size("gy"), lax.axis_size("gz")
    up = [(i, (i + 1) % gy) for i in range(gy)]
    down = [(b, a) for a, b in up]
    far, near = [], []
    for i in range(gz - 1):
        (far if i % 2 else near).extend([(i, i + 1), (i + 1, i)])
    flat = state.reshape(SPECIES, X * Y, Z)

    edge = struct(HALO, SPECIES, X, Z)
    strip_edge = struct(HALO, X, Z)
    pack = struct(PACKS, X, Z)
    own, top, bottom, strip, to_far, to_near = call(
        pack_kernel,
        (struct(Y, SPECIES, X, Z), edge, edge, struct(Y, X, Z), pack, pack),
        [pltpu.HBM],
        [VMEM((SPECIES, X * Y, Z), F32), pltpu.SemaphoreType.DMA((SPECIES,))],
    )(flat)
    from_far = lax.ppermute(to_far, "gz", far)
    from_near = lax.ppermute(to_near, "gz", near)
    low = lax.ppermute(bottom, "gy", up)
    high = lax.ppermute(top, "gy", down)
    table = call(coefficient_kernel, struct(COEFFICIENTS, Z), [VMEM] * 5)(
        member_set.reshape(1, 1), courant_table.T, diffusion_table.T, reaction_table.transpose(1, 2, 0), quadratic_table.T
    )
    wide = (SPECIES, X, Z)
    basis, dots = call(
        main_kernel,
        (struct(4, Y, *wide), struct(DOTS, 8, Z)),
        [VMEM] * 4,
        [VMEM((n, *wide), F32) for n in (ROWS, Y + 8, Y + 6, Y + 4, Y + 2)],
        flops=10_000_000,
    )(own, low, high, table)
    strip, strip_top, strip_bottom = call(
        unpack_kernel, (struct(Y, X, Z), strip_edge, strip_edge), [VMEM] * 3
    )(strip, from_far, from_near)
    strip_low = lax.ppermute(strip_bottom, "gy", up)
    strip_high = lax.ppermute(strip_top, "gy", down)
    strip_basis, total = call(
        strip_kernel,
        (struct(4, Y, X, Z), struct(gy * gz, SLOTS)),
        [VMEM] * 5,
        [VMEM((n, X, Z), F32) for n in (ROWS, Y + 8, Y + 6, Y + 4, Y + 2)],
    )(strip, strip_low, strip_high, dots, table)
    sums = lax.all_to_all(total, ("gy", "gz"), split_axis=0, concat_axis=0, tiled=True)
    out = call(
        combine_kernel,
        struct(SPECIES, X * Y, Z),
        [VMEM] * 3,
        [VMEM((SPECIES, X * Y, Z), F32), VMEM((Y, X, Z), F32), pltpu.SemaphoreType.DMA((SPECIES,))],
        out_space=pltpu.HBM,
    )(sums, basis, strip_basis)
    return out.reshape(state.shape)


def solution(mesh):
    return jax.shard_map(
        shards,
        mesh=mesh,
        in_specs=(P("ens", None, None, "gy", "gz"), P("ens"), P(), P(), P(), P()),
        out_specs=P("ens", None, None, "gy", "gz"),
        check_vma=False,
    )
```

```python
import jax
import jax.numpy as jnp
from jax import lax
from jax.experimental import pallas as pl
from jax.experimental.pallas import tpu as pltpu
from jax.sharding import PartitionSpec as P


SPECIES = 4
X = 16
Y = 16
Z = 128
HALO = 5
GROUP = 6
PACKS = 3
ROWS = Y + 2 * HALO
DOTS = 13
SLOTS = 16
MAIN_SOURCE, MAIN_LEVEL, MAIN_DOT = 8, (11, 10, 9, 8), 4
STRIP_SOURCE, STRIP_LEVEL, STRIP_DOT = 12, (11, 10, 9, 8), 4

F32 = jnp.float32
VMEM = pltpu.VMEM
SMEM = pltpu.SMEM


def struct(*shape):
    return jax.ShapeDtypeStruct(shape, F32)


def lanes():
    return lax.broadcasted_iota(jnp.int32, (X, Z), 1)


def shift(v, amount):
    amount %= Z
    return pltpu.roll(v, amount, 1) if amount else v


def over_rows(count, at_once, body, carry=None):
    if at_once >= count:
        for row in range(count):
            carry = body(row, carry)
        return carry

    def step(i, c):
        for k in range(at_once):
            c = body(i * at_once + k, c)
        return c

    whole = count // at_once
    carry = lax.fori_loop(0, whole, step, carry)
    for row in range(whole * at_once, count):
        carry = body(row, carry)
    return carry


def unpack_kernel(strip_ref, far_ref, near_ref, full_ref, top_ref, bottom_ref):
    place = lanes() % 32
    odd = lax.axis_index("gz") % 2 == 1
    for g in range(PACKS):
        far, near = far_ref[g], near_ref[g]
        after = jnp.where(odd, far, near)
        before = jnp.where(odd, near, far)
        for i in range(GROUP):
            y = g * GROUP + i
            if y < Y:
                v = strip_ref[y]
                v = jnp.where(place < HALO, shift(before, -i * HALO), v)
                v = jnp.where(place >= 27, shift(after, 27 - i * HALO), v)
                full_ref[y] = v
                if y < HALO:
                    top_ref[y] = v
                if y >= Y - HALO:
                    bottom_ref[y - (Y - HALO)] = v


def beside_x(v):
    row = lax.broadcasted_iota(jnp.int32, (X, Z), 0)
    below = jnp.where(row == 0, 0.0, pltpu.roll(v, 1, 0))
    above = jnp.where(row == X - 1, 0.0, pltpu.roll(v, X - 1, 0))
    return below, above


def in_grid():
    low = jnp.where(lax.axis_index("gy") > 0, 1.0, 0.0).astype(F32)
    high = jnp.where(lax.axis_index("gy") < lax.axis_size("gy") - 1, 1.0, 0.0).astype(F32)
    return low, high


def row_flag(row, before, low, high):
    if isinstance(row, int):
        return low if row < before else high if row >= before + Y else 1.0
    flag = jnp.where(row < before, low, 1.0)
    return jnp.where(row >= before + Y, high, flag)


PLUS, MINUS, LINEAR, QUAD, SCALE, TURNED, STRIP_QUAD, STRIP_SCALE, RANGE = 0, 3, 6, 22, 26, 30, 34, 35, 36
COEFFICIENTS = 40


def coefficients(hot, courant_ref, diffusion_ref, reaction_ref, quadratic_ref, out_ref):

    def picked(table):
        return jnp.sum(jnp.where(hot, table, 0.0), axis=1, keepdims=True)

    def put(row, value):
        out_ref[row : row + 1, :] = jnp.broadcast_to(value, (1, Z))

    lane = lax.broadcasted_iota(jnp.int32, (1, Z), 1)

    def by_species(values):
        out = jnp.broadcast_to(values[3], (1, Z))
        for s in (2, 1, 0):
            out = jnp.where(lane < 32 * (s + 1), values[s], out)
        return out

    courant = picked(courant_ref[...])
    plus, minus = jnp.maximum(courant, 0.0), jnp.minimum(courant, 0.0)
    kept = jnp.ones((1, 1), F32)
    for d in range(3):
        put(PLUS + d, plus[d : d + 1])
        put(MINUS + d, minus[d : d + 1])
        kept = kept - (plus[d : d + 1] - minus[d : d + 1])
    linear = []
    for k in range(SPECIES):
        rates = picked(reaction_ref[k])
        linear.append([rates[l : l + 1] for l in range(SPECIES)])
        linear[k][k] = linear[k][k] + kept
        for l in range(SPECIES):
            put(LINEAR + SPECIES * k + l, linear[k][l])
    for t in range(SPECIES):
        put(TURNED + t, by_species([linear[k][(k - t) % SPECIES] for k in range(SPECIES)]))
    rates = picked(quadratic_ref[...])
    quad = [rates[k : k + 1] for k in range(SPECIES)]
    d = picked(diffusion_ref[...])
    d = [d[k : k + 1] for k in range(SPECIES)]
    reach = 6.0 * jnp.maximum(jnp.maximum(d[0], d[1]), jnp.maximum(d[2], d[3]))
    scale = [v / reach for v in d]
    for k in range(SPECIES):
        put(QUAD + k, quad[k])
        put(SCALE + k, scale[k])
    put(STRIP_QUAD, by_species(quad))
    put(STRIP_SCALE, by_species(scale))
    put(RANGE, reach)


def pack_kernel(
    state_ref, member_ref, courant_ref, diffusion_ref, reaction_ref, quadratic_ref,
    own_ref, top_ref, bottom_ref, strip_ref, far_ref, near_ref, table_ref,
    state, courant, diffusion, reaction, quadratic, state_sems, sems,
):
    blocks = [pltpu.make_async_copy(state_ref.at[s], state.at[s], state_sems.at[s]) for s in range(SPECIES)]
    tables = (
        (courant_ref, courant), (diffusion_ref, diffusion), (reaction_ref, reaction),
        (quadratic_ref, quadratic),
    )
    copies = [pltpu.make_async_copy(a, b, sems.at[i]) for i, (a, b) in enumerate(tables)]
    for copy in blocks + copies:
        copy.start()
    lane = lanes()
    odd = lax.axis_index("gz") % 2 == 1
    place = lane % 32
    for s in range(SPECIES):
        blocks[s].wait()
        for y in range(Y):
            v = state[s, pl.ds(y, X, stride=Y), :]
            own_ref[y, s] = v
            if y < HALO:
                top_ref[y, s] = v
            if y >= Y - HALO:
                bottom_ref[y - (Y - HALO), s] = v
            total = strip_ref[y] if s else jnp.zeros((X, Z), F32)
            low = shift(v, 32 * s + HALO)
            high = shift(v, 32 * s + 16 - (Z - 11))
            total = jnp.where((lane >= 32 * s + HALO) & (lane < 32 * s + 16), low, total)
            total = jnp.where((lane >= 32 * s + 16) & (lane < 32 * s + 27), high, total)
            strip_ref[y] = total
    for g in range(PACKS):
        lows = jnp.zeros((X, Z), F32)
        highs = jnp.zeros((X, Z), F32)
        for i in range(GROUP):
            if g * GROUP + i < Y:
                v = strip_ref[g * GROUP + i]
                here = (place >= i * HALO) & (place < (i + 1) * HALO)
                lows = jnp.where(here, shift(v, i * HALO - HALO), lows)
                highs = jnp.where(here, shift(v, i * HALO - 22), highs)
        far_ref[g] = jnp.where(odd, highs, lows)
        near_ref[g] = jnp.where(odd, lows, highs)
    for copy in copies:
        copy.wait()
    hot = lax.broadcasted_iota(jnp.int32, (1, courant.shape[-1]), 1) == member_ref[0]
    coefficients(hot, courant, diffusion, reaction, quadratic, table_ref)


def spread(table_ref, row):
    return jnp.broadcast_to(table_ref[row : row + 1, :], (X, Z))


def dot_terms(b):
    pairs = ((0, 0), (0, 1), (0, 3), (0, 4), (1, 1), (1, 2), (1, 3), (1, 4), (2, 2), (2, 3), (3, 3), (3, 4), (4, 4))
    out = []
    for i, j in pairs:
        p = b[i] * b[j]
        out.append(p[:8] + p[8:])
    return out


def level_value(k, image, v, before):
    if k < 3:
        return image
    if k == 3:
        return image - v
    return 2.0 * (image - v) - before


def main_kernel(own_ref, low_ref, high_ref, table_ref, basis_ref, dots_ref, wide, b0, b1, b2, b3, b4):
    low, high = in_grid()
    for r in range(HALO):
        for s in range(SPECIES):
            wide[r, s] = low_ref[r, s] * low
            wide[HALO + Y + r, s] = high_ref[r, s] * high
    for y in range(Y):
        for s in range(SPECIES):
            wide[HALO + y, s] = own_ref[y, s]

    plus = [spread(table_ref, PLUS + d) for d in range(3)]
    minus = [spread(table_ref, MINUS + d) for d in range(3)]
    linear = [[spread(table_ref, LINEAR + SPECIES * k + l) for l in range(SPECIES)] for k in range(SPECIES)]
    quad = [spread(table_ref, QUAD + k) for k in range(SPECIES)]

    def source_row(row, _):
        flag = row_flag(row, HALO - 1, low, high)
        v = [wide[row + 1, s] for s in range(SPECIES)]
        a, b = v[0], v[1]
        coupled = a * b / (1.0 + a * a + b * b)
        for k in range(SPECIES):
            below, above = beside_x(v[k])
            out = plus[0] * below - minus[0] * above
            out = out + (plus[1] * wide[row, k] - minus[1] * wide[row + 2, k])
            out = out + (plus[2] * shift(v[k], 1) - minus[2] * shift(v[k], -1))
            for l in range(SPECIES):
                out = out + linear[k][l] * v[l]
            b0[row, k] = (out + quad[k] * coupled) * flag
        return _

    over_rows(Y + 8, MAIN_SOURCE, source_row)

    scale = [spread(table_ref, SCALE + s) for s in range(SPECIES)]
    buffers = [b0, b1, b2, b3, b4]

    def image_of(ref, row, s):
        v = ref[row + 1, s]
        below, above = beside_x(v)
        beside = (below + above) + (ref[row, s] + ref[row + 2, s]) + (shift(v, 1) + shift(v, -1))
        return scale[s] * (6.0 * v - beside), v

    for k in (1, 2, 3, 4):
        before = 4 - k

        def level_row(row, _, k=k, before=before):
            flag = row_flag(row, before, low, high)
            for s in range(SPECIES):
                image, v = image_of(buffers[k - 1], row, s)
                value = level_value(k, image, v, buffers[2][row + 2, s] if k == 4 else None)
                buffers[k][row, s] = value * flag if before else value
            return _

        over_rows(Y + 2 * before, MAIN_LEVEL[k - 1], level_row)

    def dot_row(row, sums):
        sums = list(sums)
        for s in range(SPECIES):
            b = [buffers[k][row + 4 - k, s] for k in range(5)]
            for k in range(4):
                basis_ref[k, row, s] = b[k]
            sums = [t + p for t, p in zip(sums, dot_terms(b))]
        return tuple(sums)

    sums = over_rows(Y, MAIN_DOT, dot_row, tuple(jnp.zeros((8, Z), F32) for _ in range(DOTS)))
    lane = lax.broadcasted_iota(jnp.int32, (8, Z), 1)
    inner = (lane >= HALO) & (lane < Z - HALO)
    for k in range(DOTS):
        dots_ref[k] = jnp.where(inner, sums[k], 0.0)


def strip_kernel(
    strip_ref, low_ref, high_ref, dots_in_ref, table_ref, basis_ref, total_ref, wide, b0, b1, b2, b3, b4
):
    low, high = in_grid()
    for r in range(HALO):
        wide[r] = low_ref[r] * low
        wide[HALO + Y + r] = high_ref[r] * high
    for y in range(Y):
        wide[HALO + y] = strip_ref[y]

    lane = lanes()
    place = lane % 32
    species = lane // 32
    first = jnp.where(lax.axis_index("gz") > 0, 1.0, 0.0).astype(F32)
    last = jnp.where(lax.axis_index("gz") < lax.axis_size("gz") - 1, 1.0, 0.0).astype(F32)
    inside = jnp.where(place < HALO, first, jnp.where(place >= 27, last, 1.0))
    plus = [spread(table_ref, PLUS + d) for d in range(3)]
    minus = [spread(table_ref, MINUS + d) for d in range(3)]
    linear = [spread(table_ref, TURNED + t) for t in range(SPECIES)]
    quad = spread(table_ref, STRIP_QUAD)

    def source_row(row, _):
        flag = row_flag(row, HALO - 1, low, high)
        v = wide[row + 1]
        turned = [v] + [shift(v, 32 * t) for t in range(1, SPECIES)]
        a, b = turned[3], turned[2]
        for t in (2, 1, 0):
            a = jnp.where(species == t, turned[t], a)
            b = jnp.where(species == (t + 1) % SPECIES, turned[t], b) if t != 2 else jnp.where(species == 0, turned[3], b)
        coupled = a * b / (1.0 + a * a + b * b)
        below, above = beside_x(v)
        out = plus[0] * below - minus[0] * above
        out = out + (plus[1] * wide[row] - minus[1] * wide[row + 2])
        out = out + (plus[2] * shift(v, 1) - minus[2] * shift(v, -1))
        for t in range(SPECIES):
            out = out + linear[t] * turned[t]
        b0[row] = (out + quad * coupled) * (flag * inside)
        return _

    over_rows(Y + 8, STRIP_SOURCE, source_row)

    scale = spread(table_ref, STRIP_SCALE)
    buffers = [b0, b1, b2, b3, b4]

    def image_of(ref, row):
        v = ref[row + 1]
        below, above = beside_x(v)
        beside = (below + above) + (ref[row] + ref[row + 2]) + (shift(v, 1) + shift(v, -1))
        return scale * (6.0 * v - beside), v

    for k in (1, 2, 3, 4):
        before = 4 - k

        def level_row(row, _, k=k, before=before):
            flag = row_flag(row, before, low, high)
            image, v = image_of(buffers[k - 1], row)
            value = level_value(k, image, v, buffers[2][row + 2] if k == 4 else None)
            buffers[k][row] = value * (flag * inside) if before else value
            return _

        over_rows(Y + 2 * before, STRIP_LEVEL[k - 1], level_row)

    def dot_row(row, sums):
        b = [buffers[k][row + 4 - k] for k in range(5)]
        for k in range(4):
            basis_ref[k, row] = b[k]
        return tuple(t + p for t, p in zip(sums, dot_terms(b)))

    sums = over_rows(Y, STRIP_DOT, dot_row, tuple(jnp.zeros((8, Z), F32) for _ in range(DOTS)))
    place = place[:8]
    edge = ((place >= HALO) & (place < 2 * HALO)) | ((place >= 22) & (place < 27))
    slot = lax.broadcasted_iota(jnp.int32, (8, SLOTS), 1)
    total = jnp.broadcast_to(table_ref[RANGE : RANGE + 1, :SLOTS], (8, SLOTS))
    for k in range(DOTS):
        both = jnp.where(edge, sums[k], 0.0) + dots_in_ref[k]
        one = jnp.sum(jnp.sum(both, axis=0, keepdims=True), axis=1, keepdims=True)
        total = jnp.where(slot == k, one, total)
    for i in range(total_ref.shape[0] // 8):
        total_ref[8 * i : 8 * i + 8, :] = total


def least_squares(h, r):
    n = 5
    root = [[None] * n for _ in range(n)]
    for i in range(n):
        rest = h[i][i]
        for k in range(i):
            rest = rest - root[k][i] * root[k][i]
        rest = jnp.maximum(rest, 3e-7 * h[i][i])
        inverse = lax.rsqrt(rest)
        root[i][i] = rest * inverse
        for j in range(i + 1, n):
            t = h[i][j]
            for k in range(i):
                t = t - root[k][i] * root[k][j]
            root[i][j] = t * inverse
    wide = 1.0 + r
    half = 0.5 * r
    columns = []
    for j, weights in enumerate((((0, 1.0), (1, r)), ((1, 1.0), (2, r)), ((2, wide), (3, r)), ((2, half), (3, wide), (4, half)))):
        column = []
        for i in range(j + 2):
            terms = [w * root[i][m] for m, w in weights if i <= m]
            column.append(sum(terms[1:], terms[0]))
        columns.append(column)
    target = [root[0][0]]
    cosines, sines = [], []
    for j in range(4):
        e = columns[j]
        for i in range(j):
            e[i], e[i + 1] = cosines[i] * e[i] + sines[i] * e[i + 1], cosines[i] * e[i + 1] - sines[i] * e[i]
        inverse = lax.rsqrt(e[j] * e[j] + e[j + 1] * e[j + 1])
        cosines.append(e[j] * inverse)
        sines.append(e[j + 1] * inverse)
        e[j] = cosines[j] * e[j] + sines[j] * e[j + 1]
        target.append(-sines[j] * target[j])
        target[j] = cosines[j] * target[j]
    y = [None] * 4
    for j in (3, 2, 1, 0):
        t = target[j]
        for k in range(j + 1, 4):
            t = t - columns[k][j] * y[k]
        y[j] = t / columns[j][j]
    return y


def combine_kernel(sums_ref, basis_ref, strip_ref, out_ref, held, strips, sems):
    total = jnp.sum(sums_ref[...], axis=0, keepdims=True)
    h00, h01, h03, h04, h11, h12, h13, h14, h22, h23, h33, h34, h44 = (total[:, k : k + 1] for k in range(DOTS))
    h = [
        [h00, h01, h11, h03, h04],
        [None, h11, h12, h13, h14],
        [None, None, h22, h23, 2.0 * h33 - h22],
        [None, None, None, h33, h34],
        [None, None, None, None, h44],
    ]
    y = [jnp.broadcast_to(c, (X, Z)) for c in least_squares(h, sums_ref[0:1, DOTS : DOTS + 1])]
    lane = lanes()
    for row in range(Y):
        strip = y[0] * strip_ref[0, row]
        for k in (1, 2, 3):
            strip = strip + y[k] * strip_ref[k, row]
        strips[row] = strip
    copies = [pltpu.make_async_copy(held.at[s], out_ref.at[s], sems.at[s]) for s in range(SPECIES)]
    for s in range(SPECIES):
        for row in range(Y):
            v = y[0] * basis_ref[0, row, s]
            for k in (1, 2, 3):
                v = v + y[k] * basis_ref[k, row, s]
            strip = strips[row]
            v = jnp.where(lane < HALO, shift(strip, -(32 * s + HALO)), v)
            v = jnp.where(lane >= Z - HALO, shift(strip, Z - HALO - (32 * s + 22)), v)
            held[s, pl.ds(row, X, stride=Y), :] = v
        copies[s].start()
    for copy in copies:
        copy.wait()


def call(kernel, outs, spaces, scratch=(), flops=1000, out_space=VMEM):
    return pl.pallas_call(
        kernel,
        out_shape=outs,
        in_specs=[pl.BlockSpec(memory_space=m) for m in spaces],
        out_specs=jax.tree.map(lambda _: pl.BlockSpec(memory_space=out_space), outs),
        scratch_shapes=list(scratch),
        cost_estimate=pl.CostEstimate(flops=flops, bytes_accessed=1 << 20, transcendentals=0),
        compiler_params=pltpu.CompilerParams(vmem_limit_bytes=24 << 20),
    )


def shards(state, member_set, courant_table, diffusion_table, reaction_table, quadratic_table):
    gy, gz = lax.axis_size("gy"), lax.axis_size("gz")
    up = [(i, (i + 1) % gy) for i in range(gy)]
    down = [(b, a) for a, b in up]
    far, near = [], []
    for i in range(gz - 1):
        (far if i % 2 else near).extend([(i, i + 1), (i + 1, i)])
    flat = state.reshape(SPECIES, X * Y, Z)

    edge = struct(HALO, SPECIES, X, Z)
    strip_edge = struct(HALO, X, Z)
    pack = struct(PACKS, X, Z)
    inputs = (
        flat, member_set, courant_table.T, diffusion_table.T, reaction_table.transpose(1, 2, 0), quadratic_table.T,
    )
    own, top, bottom, strip, to_far, to_near, table = call(
        pack_kernel,
        (struct(Y, SPECIES, X, Z), edge, edge, struct(Y, X, Z), pack, pack, struct(COEFFICIENTS, Z)),
        [pltpu.HBM, SMEM] + [pltpu.HBM] * 4,
        [VMEM(flat.shape, F32)]
        + [VMEM(t.shape, F32) for t in inputs[2:]]
        + [pltpu.SemaphoreType.DMA((SPECIES,)), pltpu.SemaphoreType.DMA((len(inputs) - 2,))],
    )(*(t if t is member_set else pltpu.with_memory_space_constraint(t, pltpu.HBM) for t in inputs))
    from_far = lax.ppermute(to_far, "gz", far)
    from_near = lax.ppermute(to_near, "gz", near)
    low = lax.ppermute(bottom, "gy", up)
    high = lax.ppermute(top, "gy", down)
    wide = (SPECIES, X, Z)
    basis, dots = call(
        main_kernel,
        (struct(4, Y, *wide), struct(DOTS, 8, Z)),
        [VMEM] * 4,
        [VMEM((n, *wide), F32) for n in (ROWS, Y + 8, Y + 6, Y + 4, Y + 2, Y)],
        flops=10_000_000,
    )(own, low, high, table)
    strip, strip_top, strip_bottom = call(
        unpack_kernel, (struct(Y, X, Z), strip_edge, strip_edge), [VMEM] * 3
    )(strip, from_far, from_near)
    strip_low = lax.ppermute(strip_bottom, "gy", up)
    strip_high = lax.ppermute(strip_top, "gy", down)
    strip_basis, total = call(
        strip_kernel,
        (struct(4, Y, X, Z), struct(gy * gz, SLOTS)),
        [VMEM] * 5,
        [VMEM((n, X, Z), F32) for n in (ROWS, Y + 8, Y + 6, Y + 4, Y + 2, Y)],
    )(strip, strip_low, strip_high, dots, table)
    sums = lax.all_to_all(total, ("gy", "gz"), split_axis=0, concat_axis=0, tiled=True)
    out = call(
        combine_kernel,
        struct(SPECIES, X * Y, Z),
        [VMEM] * 3,
        [VMEM((SPECIES, X * Y, Z), F32), VMEM((Y, X, Z), F32), pltpu.SemaphoreType.DMA((SPECIES,))],
        out_space=pltpu.HBM,
    )(sums, basis, strip_basis)
    return out.reshape(state.shape)


def solution(mesh):
    return jax.shard_map(
        shards,
        mesh=mesh,
        in_specs=(P("ens", None, None, "gy", "gz"), P("ens"), P(), P(), P(), P()),
        out_specs=P("ens", None, None, "gy", "gz"),
        check_vma=False,
    )
```

```python
import jax
import jax.numpy as jnp
from jax import lax
from jax.experimental import pallas as pl
from jax.experimental.pallas import tpu as pltpu
from jax.sharding import PartitionSpec as P


SPECIES = 4
X = 16
Y = 16
Z = 128
HALO = 5
GROUP = 6
PACKS = 3
ROWS = Y + 2 * HALO
DOTS = 13
SLOTS = 16
MAIN_SOURCE, MAIN_LEVEL, MAIN_DOT = 8, (11, 10, 9, 8), 4
STRIP_SOURCE, STRIP_LEVEL, STRIP_DOT = 12, (11, 10, 9, 8), 4

F32 = jnp.float32
VMEM = pltpu.VMEM
SMEM = pltpu.SMEM


def struct(*shape):
    return jax.ShapeDtypeStruct(shape, F32)


GZ = ("gh", "gx")


def z_index():
    return lax.axis_index("gh") * lax.axis_size("gx") + lax.axis_index("gx")


def z_size():
    return lax.axis_size("gh") * lax.axis_size("gx")


def lanes():
    return lax.broadcasted_iota(jnp.int32, (X, Z), 1)


def shift(v, amount):
    amount %= Z
    return pltpu.roll(v, amount, 1) if amount else v


def over_rows(count, at_once, body, carry=None):
    if at_once >= count:
        for row in range(count):
            carry = body(row, carry)
        return carry

    def step(i, c):
        for k in range(at_once):
            c = body(i * at_once + k, c)
        return c

    whole = count // at_once
    carry = lax.fori_loop(0, whole, step, carry)
    for row in range(whole * at_once, count):
        carry = body(row, carry)
    return carry


def unpack_kernel(strip_ref, far_ref, near_ref, full_ref, top_ref, bottom_ref):
    place = lanes() % 32
    odd = z_index() % 2 == 1
    for g in range(PACKS):
        far, near = far_ref[g], near_ref[g]
        after = jnp.where(odd, far, near)
        before = jnp.where(odd, near, far)
        for i in range(GROUP):
            y = g * GROUP + i
            if y < Y:
                v = strip_ref[y]
                v = jnp.where(place < HALO, shift(before, -i * HALO), v)
                v = jnp.where(place >= 27, shift(after, 27 - i * HALO), v)
                full_ref[y] = v
                if y < HALO:
                    top_ref[y] = v
                if y >= Y - HALO:
                    bottom_ref[y - (Y - HALO)] = v


def beside_x(v):
    row = lax.broadcasted_iota(jnp.int32, (X, Z), 0)
    below = jnp.where(row == 0, 0.0, pltpu.roll(v, 1, 0))
    above = jnp.where(row == X - 1, 0.0, pltpu.roll(v, X - 1, 0))
    return below, above


def in_grid():
    low = jnp.where(lax.axis_index("gy") > 0, 1.0, 0.0).astype(F32)
    high = jnp.where(lax.axis_index("gy") < lax.axis_size("gy") - 1, 1.0, 0.0).astype(F32)
    return low, high


def row_flag(row, before, low, high):
    if isinstance(row, int):
        return low if row < before else high if row >= before + Y else 1.0
    flag = jnp.where(row < before, low, 1.0)
    return jnp.where(row >= before + Y, high, flag)


PLUS, MINUS, LINEAR, QUAD, SCALE, TURNED, STRIP_QUAD, STRIP_SCALE, RANGE = 0, 3, 6, 22, 26, 30, 34, 35, 36
COEFFICIENTS = 40


def coefficient_kernel(member_ref, courant_ref, diffusion_ref, reaction_ref, quadratic_ref, out_ref):
    hot = lax.broadcasted_iota(jnp.int32, (1, courant_ref.shape[-1]), 1) == member_ref[0]

    def picked(table):
        return jnp.sum(jnp.where(hot, table, 0.0), axis=1, keepdims=True)

    def put(row, value):
        out_ref[row : row + 1, :] = jnp.broadcast_to(value, (1, Z))

    lane = lax.broadcasted_iota(jnp.int32, (1, Z), 1)

    def by_species(values):
        out = jnp.broadcast_to(values[3], (1, Z))
        for s in (2, 1, 0):
            out = jnp.where(lane < 32 * (s + 1), values[s], out)
        return out

    courant = picked(courant_ref[...])
    plus, minus = jnp.maximum(courant, 0.0), jnp.minimum(courant, 0.0)
    kept = jnp.ones((1, 1), F32)
    for d in range(3):
        put(PLUS + d, plus[d : d + 1])
        put(MINUS + d, minus[d : d + 1])
        kept = kept - (plus[d : d + 1] - minus[d : d + 1])
    linear = []
    for k in range(SPECIES):
        rates = picked(reaction_ref[k])
        linear.append([rates[l : l + 1] for l in range(SPECIES)])
        linear[k][k] = linear[k][k] + kept
        for l in range(SPECIES):
            put(LINEAR + SPECIES * k + l, linear[k][l])
    for t in range(SPECIES):
        put(TURNED + t, by_species([linear[k][(k - t) % SPECIES] for k in range(SPECIES)]))
    rates = picked(quadratic_ref[...])
    quad = [rates[k : k + 1] for k in range(SPECIES)]
    d = picked(diffusion_ref[...])
    d = [d[k : k + 1] for k in range(SPECIES)]
    reach = 6.0 * jnp.maximum(jnp.maximum(d[0], d[1]), jnp.maximum(d[2], d[3]))
    scale = [v / reach for v in d]
    for k in range(SPECIES):
        put(QUAD + k, quad[k])
        put(SCALE + k, scale[k])
    put(STRIP_QUAD, by_species(quad))
    put(STRIP_SCALE, by_species(scale))
    put(RANGE, reach)


def pack_kernel(
    state_ref, courant_ref, diffusion_ref, reaction_ref, quadratic_ref,
    own_ref, top_ref, bottom_ref, strip_ref, far_ref, near_ref, courant, diffusion, reaction, quadratic,
    state, state_sems, sems,
):
    blocks = [pltpu.make_async_copy(state_ref.at[s], state.at[s], state_sems.at[s]) for s in range(SPECIES)]
    tables = (
        (courant_ref, courant), (diffusion_ref, diffusion), (reaction_ref, reaction),
        (quadratic_ref, quadratic),
    )
    copies = [pltpu.make_async_copy(a, b, sems.at[i]) for i, (a, b) in enumerate(tables)]
    for copy in blocks + copies:
        copy.start()
    lane = lanes()
    odd = z_index() % 2 == 1
    place = lane % 32
    for s in range(SPECIES):
        blocks[s].wait()
        for y in range(Y):
            v = state[s, pl.ds(y, X, stride=Y), :]
            own_ref[y, s] = v
            if y < HALO:
                top_ref[y, s] = v
            if y >= Y - HALO:
                bottom_ref[y - (Y - HALO), s] = v
            total = strip_ref[y] if s else jnp.zeros((X, Z), F32)
            low = shift(v, 32 * s + HALO)
            high = shift(v, 32 * s + 16 - (Z - 11))
            total = jnp.where((lane >= 32 * s + HALO) & (lane < 32 * s + 16), low, total)
            total = jnp.where((lane >= 32 * s + 16) & (lane < 32 * s + 27), high, total)
            strip_ref[y] = total
    for g in range(PACKS):
        lows = jnp.zeros((X, Z), F32)
        highs = jnp.zeros((X, Z), F32)
        for i in range(GROUP):
            if g * GROUP + i < Y:
                v = strip_ref[g * GROUP + i]
                here = (place >= i * HALO) & (place < (i + 1) * HALO)
                lows = jnp.where(here, shift(v, i * HALO - HALO), lows)
                highs = jnp.where(here, shift(v, i * HALO - 22), highs)
        far_ref[g] = jnp.where(odd, highs, lows)
        near_ref[g] = jnp.where(odd, lows, highs)
    for copy in copies:
        copy.wait()


def spread(table_ref, row):
    return jnp.broadcast_to(table_ref[row : row + 1, :], (X, Z))


def dot_terms(b):
    pairs = ((0, 0), (0, 1), (0, 3), (0, 4), (1, 1), (1, 2), (1, 3), (1, 4), (2, 2), (2, 3), (3, 3), (3, 4), (4, 4))
    out = []
    for i, j in pairs:
        p = b[i] * b[j]
        out.append(p[:8] + p[8:])
    return out


def level_value(k, image, v, before):
    if k < 3:
        return image
    if k == 3:
        return image - v
    return 2.0 * (image - v) - before


def main_kernel(own_ref, low_ref, high_ref, table_ref, basis_ref, dots_ref, wide, b0, b1, b2, b3, b4):
    low, high = in_grid()
    for r in range(HALO):
        for s in range(SPECIES):
            wide[r, s] = low_ref[r, s] * low
            wide[HALO + Y + r, s] = high_ref[r, s] * high
    for y in range(Y):
        for s in range(SPECIES):
            wide[HALO + y, s] = own_ref[y, s]

    plus = [spread(table_ref, PLUS + d) for d in range(3)]
    minus = [spread(table_ref, MINUS + d) for d in range(3)]
    linear = [[spread(table_ref, LINEAR + SPECIES * k + l) for l in range(SPECIES)] for k in range(SPECIES)]
    quad = [spread(table_ref, QUAD + k) for k in range(SPECIES)]

    def source_row(row, _):
        flag = row_flag(row, HALO - 1, low, high)
        v = [wide[row + 1, s] for s in range(SPECIES)]
        a, b = v[0], v[1]
        coupled = a * b / (1.0 + a * a + b * b)
        for k in range(SPECIES):
            below, above = beside_x(v[k])
            out = plus[0] * below - minus[0] * above
            out = out + (plus[1] * wide[row, k] - minus[1] * wide[row + 2, k])
            out = out + (plus[2] * shift(v[k], 1) - minus[2] * shift(v[k], -1))
            for l in range(SPECIES):
                out = out + linear[k][l] * v[l]
            b0[row, k] = (out + quad[k] * coupled) * flag
        return _

    over_rows(Y + 8, MAIN_SOURCE, source_row)

    scale = [spread(table_ref, SCALE + s) for s in range(SPECIES)]
    buffers = [b0, b1, b2, b3, b4]

    def image_of(ref, row, s):
        v = ref[row + 1, s]
        below, above = beside_x(v)
        beside = (below + above) + (ref[row, s] + ref[row + 2, s]) + (shift(v, 1) + shift(v, -1))
        return scale[s] * (6.0 * v - beside), v

    for k in (1, 2, 3, 4):
        before = 4 - k

        def level_row(row, _, k=k, before=before):
            flag = row_flag(row, before, low, high)
            for s in range(SPECIES):
                image, v = image_of(buffers[k - 1], row, s)
                value = level_value(k, image, v, buffers[2][row + 2, s] if k == 4 else None)
                buffers[k][row, s] = value * flag if before else value
            return _

        over_rows(Y + 2 * before, MAIN_LEVEL[k - 1], level_row)

    def dot_row(row, sums):
        sums = list(sums)
        for s in range(SPECIES):
            b = [buffers[k][row + 4 - k, s] for k in range(5)]
            for k in range(4):
                basis_ref[k, row, s] = b[k]
            sums = [t + p for t, p in zip(sums, dot_terms(b))]
        return tuple(sums)

    sums = over_rows(Y, MAIN_DOT, dot_row, tuple(jnp.zeros((8, Z), F32) for _ in range(DOTS)))
    lane = lax.broadcasted_iota(jnp.int32, (8, Z), 1)
    inner = (lane >= HALO) & (lane < Z - HALO)
    for k in range(DOTS):
        dots_ref[k] = jnp.where(inner, sums[k], 0.0)


def strip_kernel(
    strip_ref, low_ref, high_ref, dots_in_ref, table_ref, basis_ref, total_ref, wide, b0, b1, b2, b3, b4
):
    low, high = in_grid()
    for r in range(HALO):
        wide[r] = low_ref[r] * low
        wide[HALO + Y + r] = high_ref[r] * high
    for y in range(Y):
        wide[HALO + y] = strip_ref[y]

    lane = lanes()
    place = lane % 32
    species = lane // 32
    first = jnp.where(z_index() > 0, 1.0, 0.0).astype(F32)
    last = jnp.where(z_index() < z_size() - 1, 1.0, 0.0).astype(F32)
    inside = jnp.where(place < HALO, first, jnp.where(place >= 27, last, 1.0))
    plus = [spread(table_ref, PLUS + d) for d in range(3)]
    minus = [spread(table_ref, MINUS + d) for d in range(3)]
    linear = [spread(table_ref, TURNED + t) for t in range(SPECIES)]
    quad = spread(table_ref, STRIP_QUAD)

    def source_row(row, _):
        flag = row_flag(row, HALO - 1, low, high)
        v = wide[row + 1]
        turned = [v] + [shift(v, 32 * t) for t in range(1, SPECIES)]
        a, b = turned[3], turned[2]
        for t in (2, 1, 0):
            a = jnp.where(species == t, turned[t], a)
            b = jnp.where(species == (t + 1) % SPECIES, turned[t], b) if t != 2 else jnp.where(species == 0, turned[3], b)
        coupled = a * b / (1.0 + a * a + b * b)
        below, above = beside_x(v)
        out = plus[0] * below - minus[0] * above
        out = out + (plus[1] * wide[row] - minus[1] * wide[row + 2])
        out = out + (plus[2] * shift(v, 1) - minus[2] * shift(v, -1))
        for t in range(SPECIES):
            out = out + linear[t] * turned[t]
        b0[row] = (out + quad * coupled) * (flag * inside)
        return _

    over_rows(Y + 8, STRIP_SOURCE, source_row)

    scale = spread(table_ref, STRIP_SCALE)
    buffers = [b0, b1, b2, b3, b4]

    def image_of(ref, row):
        v = ref[row + 1]
        below, above = beside_x(v)
        beside = (below + above) + (ref[row] + ref[row + 2]) + (shift(v, 1) + shift(v, -1))
        return scale * (6.0 * v - beside), v

    for k in (1, 2, 3, 4):
        before = 4 - k

        def level_row(row, _, k=k, before=before):
            flag = row_flag(row, before, low, high)
            image, v = image_of(buffers[k - 1], row)
            value = level_value(k, image, v, buffers[2][row + 2] if k == 4 else None)
            buffers[k][row] = value * (flag * inside) if before else value
            return _

        over_rows(Y + 2 * before, STRIP_LEVEL[k - 1], level_row)

    def dot_row(row, sums):
        b = [buffers[k][row + 4 - k] for k in range(5)]
        for k in range(4):
            basis_ref[k, row] = b[k]
        return tuple(t + p for t, p in zip(sums, dot_terms(b)))

    sums = over_rows(Y, STRIP_DOT, dot_row, tuple(jnp.zeros((8, Z), F32) for _ in range(DOTS)))
    place = place[:8]
    edge = ((place >= HALO) & (place < 2 * HALO)) | ((place >= 22) & (place < 27))
    slot = lax.broadcasted_iota(jnp.int32, (8, SLOTS), 1)
    total = jnp.broadcast_to(table_ref[RANGE : RANGE + 1, :SLOTS], (8, SLOTS))
    for k in range(DOTS):
        both = jnp.where(edge, sums[k], 0.0) + dots_in_ref[k]
        one = jnp.sum(jnp.sum(both, axis=0, keepdims=True), axis=1, keepdims=True)
        total = jnp.where(slot == k, one, total)
    total_ref[...] = jnp.broadcast_to(total[:1], total_ref.shape)


def least_squares(h, r):
    n = 5
    root = [[None] * n for _ in range(n)]
    for i in range(n):
        rest = h[i][i]
        for k in range(i):
            rest = rest - root[k][i] * root[k][i]
        rest = jnp.maximum(rest, 3e-7 * h[i][i])
        inverse = lax.rsqrt(rest)
        root[i][i] = rest * inverse
        for j in range(i + 1, n):
            t = h[i][j]
            for k in range(i):
                t = t - root[k][i] * root[k][j]
            root[i][j] = t * inverse
    wide = 1.0 + r
    half = 0.5 * r
    columns = []
    for j, weights in enumerate((((0, 1.0), (1, r)), ((1, 1.0), (2, r)), ((2, wide), (3, r)), ((2, half), (3, wide), (4, half)))):
        column = []
        for i in range(j + 2):
            terms = [w * root[i][m] for m, w in weights if i <= m]
            column.append(sum(terms[1:], terms[0]))
        columns.append(column)
    target = [root[0][0]]
    cosines, sines = [], []
    for j in range(4):
        e = columns[j]
        for i in range(j):
            e[i], e[i + 1] = cosines[i] * e[i] + sines[i] * e[i + 1], cosines[i] * e[i + 1] - sines[i] * e[i]
        inverse = lax.rsqrt(e[j] * e[j] + e[j + 1] * e[j + 1])
        cosines.append(e[j] * inverse)
        sines.append(e[j + 1] * inverse)
        e[j] = cosines[j] * e[j] + sines[j] * e[j + 1]
        target.append(-sines[j] * target[j])
        target[j] = cosines[j] * target[j]
    y = [None] * 4
    for j in (3, 2, 1, 0):
        t = target[j]
        for k in range(j + 1, 4):
            t = t - columns[k][j] * y[k]
        y[j] = t / columns[j][j]
    return y


def combine_kernel(sums_ref, basis_ref, strip_ref, out_ref, held, strips, sems):
    total = jnp.sum(sums_ref[...], axis=0, keepdims=True)
    h00, h01, h03, h04, h11, h12, h13, h14, h22, h23, h33, h34, h44 = (total[:, k : k + 1] for k in range(DOTS))
    h = [
        [h00, h01, h11, h03, h04],
        [None, h11, h12, h13, h14],
        [None, None, h22, h23, 2.0 * h33 - h22],
        [None, None, None, h33, h34],
        [None, None, None, None, h44],
    ]
    y = [jnp.broadcast_to(c, (X, Z)) for c in least_squares(h, 0.5 * sums_ref[0:1, DOTS : DOTS + 1])]
    lane = lanes()
    for row in range(Y):
        strip = y[0] * strip_ref[0, row]
        for k in (1, 2, 3):
            strip = strip + y[k] * strip_ref[k, row]
        strips[row] = strip
    copies = []
    for s in range(SPECIES):
        for row in range(Y):
            v = y[0] * basis_ref[0, row, s]
            for k in (1, 2, 3):
                v = v + y[k] * basis_ref[k, row, s]
            strip = strips[row]
            v = jnp.where(lane < HALO, shift(strip, -(32 * s + HALO)), v)
            v = jnp.where(lane >= Z - HALO, shift(strip, Z - HALO - (32 * s + 22)), v)
            held[s, pl.ds(row, X, stride=Y), :] = v
        for half in range(2):
            part = pl.ds(half * (X * Y // 2), X * Y // 2)
            copy = pltpu.make_async_copy(held.at[s, part], out_ref.at[s, part], sems.at[2 * s + half])
            copy.start()
            copies.append(copy)
    for copy in copies:
        copy.wait()


def call(kernel, outs, spaces, scratch=(), flops=1000, out_space=VMEM):
    return pl.pallas_call(
        kernel,
        out_shape=outs,
        in_specs=[pl.BlockSpec(memory_space=m) for m in spaces],
        out_specs=jax.tree.map(lambda _: pl.BlockSpec(memory_space=out_space), outs),
        scratch_shapes=list(scratch),
        cost_estimate=pl.CostEstimate(flops=flops, bytes_accessed=1 << 20, transcendentals=0),
        compiler_params=pltpu.CompilerParams(vmem_limit_bytes=24 << 20),
    )


def shards(state, member_set, courant_table, diffusion_table, reaction_table, quadratic_table):
    gy, gh, gx = lax.axis_size("gy"), lax.axis_size("gh"), lax.axis_size("gx")
    gz = gh * gx
    up = [(i, (i + 1) % gy) for i in range(gy)]
    down = [(b, a) for a, b in up]
    far, near = [], []
    for i in range(gz - 1):
        (far if i % 2 else near).extend([(i, i + 1), (i + 1, i)])
    flat = state.reshape(SPECIES, X * Y, Z)

    edge = struct(HALO, SPECIES, X, Z)
    strip_edge = struct(HALO, X, Z)
    pack = struct(PACKS, X, Z)
    inputs = (flat, courant_table.T, diffusion_table.T, reaction_table.transpose(1, 2, 0), quadratic_table.T)
    own, top, bottom, strip, to_far, to_near, *tables = call(
        pack_kernel,
        (struct(Y, SPECIES, X, Z), edge, edge, struct(Y, X, Z), pack, pack, *(struct(*t.shape) for t in inputs[1:])),
        [pltpu.HBM] * len(inputs),
        [
            VMEM(flat.shape, F32),
            pltpu.SemaphoreType.DMA((SPECIES,)),
            pltpu.SemaphoreType.DMA((len(inputs) - 1,)),
        ],
    )(*(pltpu.with_memory_space_constraint(t, pltpu.HBM) for t in inputs))
    from_far = lax.ppermute(to_far, GZ, far)
    from_near = lax.ppermute(to_near, GZ, near)
    low = lax.ppermute(bottom, "gy", up)
    high = lax.ppermute(top, "gy", down)
    table = call(coefficient_kernel, struct(COEFFICIENTS, Z), [SMEM] + [VMEM] * 4)(member_set, *tables)
    wide = (SPECIES, X, Z)
    basis, dots = call(
        main_kernel,
        (struct(4, Y, *wide), struct(DOTS, 8, Z)),
        [VMEM] * 4,
        [VMEM((n, *wide), F32) for n in (ROWS, Y + 8, Y + 6, Y + 4, Y + 2, Y)],
        flops=10_000_000,
    )(own, low, high, table)
    strip, strip_top, strip_bottom = call(
        unpack_kernel, (struct(Y, X, Z), strip_edge, strip_edge), [VMEM] * 3
    )(strip, from_far, from_near)
    strip_low = lax.ppermute(strip_bottom, "gy", up)
    strip_high = lax.ppermute(strip_top, "gy", down)
    strip_basis, total = call(
        strip_kernel,
        (struct(4, Y, X, Z), struct(gy * gx, SLOTS)),
        [VMEM] * 5,
        [VMEM((n, X, Z), F32) for n in (ROWS, Y + 8, Y + 6, Y + 4, Y + 2, Y)],
    )(strip, strip_low, strip_high, dots, table)
    other = lax.ppermute(total, "gh", [(i, 1 - i) for i in range(gh)])
    sums = lax.all_to_all(total + other, ("gy", "gx"), split_axis=0, concat_axis=0, tiled=True)
    out = call(
        combine_kernel,
        struct(SPECIES, X * Y, Z),
        [VMEM] * 3,
        [VMEM((SPECIES, X * Y, Z), F32), VMEM((Y, X, Z), F32), pltpu.SemaphoreType.DMA((2 * SPECIES,))],
        out_space=pltpu.HBM,
    )(sums, basis, strip_basis)
    return out.reshape(state.shape)


def solution(mesh):
    ens, gy, gz = (mesh.shape[a] for a in ("ens", "gy", "gz"))
    split = jax.sharding.Mesh(mesh.devices.reshape(ens, gy, 2, gz // 2), ("ens", "gy", *GZ))
    state_spec = P("ens", None, None, "gy", GZ)

    return jax.shard_map(
        shards,
        mesh=split,
        in_specs=(state_spec, P("ens"), P(), P(), P(), P()),
        out_specs=state_spec,
        check_vma=False,
    )
```

```python
import jax
import jax.numpy as jnp
from jax import lax
from jax.experimental import pallas as pl
from jax.experimental.pallas import tpu as pltpu
from jax.sharding import PartitionSpec as P


SPECIES = 4
X = 16
Y = 16
Z = 128
HALO = 5
GROUP = 6
PACKS = 3
ROWS = Y + 2 * HALO
DOTS = 13
SLOTS = 16
MAIN_SOURCE, MAIN_LEVEL, MAIN_DOT = 8, (11, 10, 9, 8), 4
STRIP_SOURCE, STRIP_LEVEL, STRIP_DOT = 12, (11, 10, 9, 8), 4

F32 = jnp.float32
VMEM = pltpu.VMEM
SMEM = pltpu.SMEM


def struct(*shape):
    return jax.ShapeDtypeStruct(shape, F32)


GZ = ("gh", "gx")


def z_index():
    return lax.axis_index("gh") * lax.axis_size("gx") + lax.axis_index("gx")


def z_size():
    return lax.axis_size("gh") * lax.axis_size("gx")


def lanes():
    return lax.broadcasted_iota(jnp.int32, (X, Z), 1)


def shift(v, amount):
    amount %= Z
    return pltpu.roll(v, amount, 1) if amount else v


def over_rows(count, at_once, body, carry=None):
    if at_once >= count:
        for row in range(count):
            carry = body(row, carry)
        return carry

    def step(i, c):
        for k in range(at_once):
            c = body(i * at_once + k, c)
        return c

    whole = count // at_once
    carry = lax.fori_loop(0, whole, step, carry)
    for row in range(whole * at_once, count):
        carry = body(row, carry)
    return carry


def unpack_kernel(strip_ref, far_ref, near_ref, full_ref, top_ref, bottom_ref):
    place = lanes() % 32
    odd = z_index() % 2 == 1
    for g in range(PACKS):
        far, near = far_ref[g], near_ref[g]
        after = jnp.where(odd, far, near)
        before = jnp.where(odd, near, far)
        for i in range(GROUP):
            y = g * GROUP + i
            if y < Y:
                v = strip_ref[y]
                v = jnp.where(place < HALO, shift(before, -i * HALO), v)
                v = jnp.where(place >= 27, shift(after, 27 - i * HALO), v)
                full_ref[y] = v
                if y < HALO:
                    top_ref[y] = v
                if y >= Y - HALO:
                    bottom_ref[y - (Y - HALO)] = v


def beside_x(v):
    row = lax.broadcasted_iota(jnp.int32, (X, Z), 0)
    below = jnp.where(row == 0, 0.0, pltpu.roll(v, 1, 0))
    above = jnp.where(row == X - 1, 0.0, pltpu.roll(v, X - 1, 0))
    return below, above


def in_grid():
    low = jnp.where(lax.axis_index("gy") > 0, 1.0, 0.0).astype(F32)
    high = jnp.where(lax.axis_index("gy") < lax.axis_size("gy") - 1, 1.0, 0.0).astype(F32)
    return low, high


def row_flag(row, before, low, high):
    if isinstance(row, int):
        return low if row < before else high if row >= before + Y else 1.0
    flag = jnp.where(row < before, low, 1.0)
    return jnp.where(row >= before + Y, high, flag)


PLUS, MINUS, LINEAR, QUAD, SCALE, TURNED, STRIP_QUAD, STRIP_SCALE, RANGE = 0, 3, 6, 22, 26, 30, 34, 35, 36
COEFFICIENTS = 40


def coefficient_kernel(member_ref, courant_ref, diffusion_ref, reaction_ref, quadratic_ref, out_ref):
    hot = lax.broadcasted_iota(jnp.int32, (1, courant_ref.shape[-1]), 1) == member_ref[0]

    def picked(table):
        return jnp.sum(jnp.where(hot, table, 0.0), axis=1, keepdims=True)

    def put(row, value):
        out_ref[row : row + 1, :] = jnp.broadcast_to(value, (1, Z))

    lane = lax.broadcasted_iota(jnp.int32, (1, Z), 1)

    def by_species(values):
        out = jnp.broadcast_to(values[3], (1, Z))
        for s in (2, 1, 0):
            out = jnp.where(lane < 32 * (s + 1), values[s], out)
        return out

    courant = picked(courant_ref[...])
    plus, minus = jnp.maximum(courant, 0.0), jnp.minimum(courant, 0.0)
    kept = jnp.ones((1, 1), F32)
    for d in range(3):
        put(PLUS + d, plus[d : d + 1])
        put(MINUS + d, minus[d : d + 1])
        kept = kept - (plus[d : d + 1] - minus[d : d + 1])
    linear = []
    for k in range(SPECIES):
        rates = picked(reaction_ref[k])
        linear.append([rates[l : l + 1] for l in range(SPECIES)])
        linear[k][k] = linear[k][k] + kept
        for l in range(SPECIES):
            put(LINEAR + SPECIES * k + l, linear[k][l])
    for t in range(SPECIES):
        put(TURNED + t, by_species([linear[k][(k - t) % SPECIES] for k in range(SPECIES)]))
    rates = picked(quadratic_ref[...])
    quad = [rates[k : k + 1] for k in range(SPECIES)]
    d = picked(diffusion_ref[...])
    d = [d[k : k + 1] for k in range(SPECIES)]
    reach = 6.0 * jnp.maximum(jnp.maximum(d[0], d[1]), jnp.maximum(d[2], d[3]))
    scale = [v / reach for v in d]
    for k in range(SPECIES):
        put(QUAD + k, quad[k])
        put(SCALE + k, scale[k])
    put(STRIP_QUAD, by_species(quad))
    put(STRIP_SCALE, by_species(scale))
    put(RANGE, reach)


def pack_kernel(
    state_ref, courant_ref, diffusion_ref, reaction_ref, quadratic_ref,
    own_ref, top_ref, bottom_ref, strip_ref, far_ref, near_ref, courant, diffusion, reaction, quadratic,
    state, state_sems, sems,
):
    blocks = [pltpu.make_async_copy(state_ref.at[s], state.at[s], state_sems.at[s]) for s in range(SPECIES)]
    tables = (
        (courant_ref, courant), (diffusion_ref, diffusion), (reaction_ref, reaction),
        (quadratic_ref, quadratic),
    )
    copies = [pltpu.make_async_copy(a, b, sems.at[i]) for i, (a, b) in enumerate(tables)]
    for copy in blocks + copies:
        copy.start()
    lane = lanes()
    odd = z_index() % 2 == 1
    place = lane % 32
    for s in range(SPECIES):
        blocks[s].wait()
        for y in range(Y):
            v = state[s, pl.ds(y, X, stride=Y), :]
            own_ref[y, s] = v
            if y < HALO:
                top_ref[y, s] = v
            if y >= Y - HALO:
                bottom_ref[y - (Y - HALO), s] = v
            total = strip_ref[y] if s else jnp.zeros((X, Z), F32)
            low = shift(v, 32 * s + HALO)
            high = shift(v, 32 * s + 16 - (Z - 11))
            total = jnp.where((lane >= 32 * s + HALO) & (lane < 32 * s + 16), low, total)
            total = jnp.where((lane >= 32 * s + 16) & (lane < 32 * s + 27), high, total)
            strip_ref[y] = total
    for g in range(PACKS):
        lows = jnp.zeros((X, Z), F32)
        highs = jnp.zeros((X, Z), F32)
        for i in range(GROUP):
            if g * GROUP + i < Y:
                v = strip_ref[g * GROUP + i]
                here = (place >= i * HALO) & (place < (i + 1) * HALO)
                lows = jnp.where(here, shift(v, i * HALO - HALO), lows)
                highs = jnp.where(here, shift(v, i * HALO - 22), highs)
        far_ref[g] = jnp.where(odd, highs, lows)
        near_ref[g] = jnp.where(odd, lows, highs)
    for copy in copies:
        copy.wait()


def spread(table_ref, row):
    return jnp.broadcast_to(table_ref[row : row + 1, :], (X, Z))


def dot_terms(b):
    pairs = ((0, 0), (0, 1), (0, 3), (0, 4), (1, 1), (1, 2), (1, 3), (1, 4), (2, 2), (2, 3), (3, 3), (3, 4), (4, 4))
    out = []
    for i, j in pairs:
        p = b[i] * b[j]
        out.append(p[:8] + p[8:])
    return out


def level_value(k, image, v, before):
    if k < 3:
        return image
    if k == 3:
        return image - v
    return 2.0 * (image - v) - before


def main_kernel(own_ref, low_ref, high_ref, table_ref, basis_ref, dots_ref, wide, b0, b1, b2, b3, b4):
    low, high = in_grid()
    for r in range(HALO):
        for s in range(SPECIES):
            wide[r, s] = low_ref[r, s] * low
            wide[HALO + Y + r, s] = high_ref[r, s] * high
    for y in range(Y):
        for s in range(SPECIES):
            wide[HALO + y, s] = own_ref[y, s]

    plus = [spread(table_ref, PLUS + d) for d in range(3)]
    minus = [spread(table_ref, MINUS + d) for d in range(3)]
    linear = [[spread(table_ref, LINEAR + SPECIES * k + l) for l in range(SPECIES)] for k in range(SPECIES)]
    quad = [spread(table_ref, QUAD + k) for k in range(SPECIES)]

    def source_row(row, _):
        flag = row_flag(row, HALO - 1, low, high)
        v = [wide[row + 1, s] for s in range(SPECIES)]
        a, b = v[0], v[1]
        coupled = a * b / (1.0 + a * a + b * b)
        for k in range(SPECIES):
            below, above = beside_x(v[k])
            out = plus[0] * below - minus[0] * above
            out = out + (plus[1] * wide[row, k] - minus[1] * wide[row + 2, k])
            out = out + (plus[2] * shift(v[k], 1) - minus[2] * shift(v[k], -1))
            for l in range(SPECIES):
                out = out + linear[k][l] * v[l]
            b0[row, k] = (out + quad[k] * coupled) * flag
        return _

    over_rows(Y + 8, MAIN_SOURCE, source_row)

    scale = [spread(table_ref, SCALE + s) for s in range(SPECIES)]
    buffers = [b0, b1, b2, b3, b4]

    def image_of(ref, row, s):
        v = ref[row + 1, s]
        below, above = beside_x(v)
        beside = (below + above) + (ref[row, s] + ref[row + 2, s]) + (shift(v, 1) + shift(v, -1))
        return scale[s] * (6.0 * v - beside), v

    for k in (1, 2, 3, 4):
        before = 4 - k

        def level_row(row, _, k=k, before=before):
            flag = row_flag(row, before, low, high)
            for s in range(SPECIES):
                image, v = image_of(buffers[k - 1], row, s)
                value = level_value(k, image, v, buffers[2][row + 2, s] if k == 4 else None)
                buffers[k][row, s] = value * flag if before else value
            return _

        over_rows(Y + 2 * before, MAIN_LEVEL[k - 1], level_row)

    def dot_row(row, sums):
        sums = list(sums)
        for s in range(SPECIES):
            b = [buffers[k][row + 4 - k, s] for k in range(5)]
            for k in range(4):
                basis_ref[k, row, s] = b[k]
            sums = [t + p for t, p in zip(sums, dot_terms(b))]
        return tuple(sums)

    sums = over_rows(Y, MAIN_DOT, dot_row, tuple(jnp.zeros((8, Z), F32) for _ in range(DOTS)))
    lane = lax.broadcasted_iota(jnp.int32, (8, Z), 1)
    inner = (lane >= HALO) & (lane < Z - HALO)
    for k in range(DOTS):
        dots_ref[k] = jnp.where(inner, sums[k], 0.0)


def strip_kernel(
    strip_ref, low_ref, high_ref, dots_in_ref, table_ref, basis_ref, total_ref, wide, b0, b1, b2, b3, b4
):
    low, high = in_grid()
    for r in range(HALO):
        wide[r] = low_ref[r] * low
        wide[HALO + Y + r] = high_ref[r] * high
    for y in range(Y):
        wide[HALO + y] = strip_ref[y]

    lane = lanes()
    place = lane % 32
    species = lane // 32
    first = jnp.where(z_index() > 0, 1.0, 0.0).astype(F32)
    last = jnp.where(z_index() < z_size() - 1, 1.0, 0.0).astype(F32)
    inside = jnp.where(place < HALO, first, jnp.where(place >= 27, last, 1.0))
    plus = [spread(table_ref, PLUS + d) for d in range(3)]
    minus = [spread(table_ref, MINUS + d) for d in range(3)]
    linear = [spread(table_ref, TURNED + t) for t in range(SPECIES)]
    quad = spread(table_ref, STRIP_QUAD)

    def source_row(row, _):
        flag = row_flag(row, HALO - 1, low, high)
        v = wide[row + 1]
        turned = [v] + [shift(v, 32 * t) for t in range(1, SPECIES)]
        a, b = turned[3], turned[2]
        for t in (2, 1, 0):
            a = jnp.where(species == t, turned[t], a)
            b = jnp.where(species == (t + 1) % SPECIES, turned[t], b) if t != 2 else jnp.where(species == 0, turned[3], b)
        coupled = a * b / (1.0 + a * a + b * b)
        below, above = beside_x(v)
        out = plus[0] * below - minus[0] * above
        out = out + (plus[1] * wide[row] - minus[1] * wide[row + 2])
        out = out + (plus[2] * shift(v, 1) - minus[2] * shift(v, -1))
        for t in range(SPECIES):
            out = out + linear[t] * turned[t]
        b0[row] = (out + quad * coupled) * (flag * inside)
        return _

    over_rows(Y + 8, STRIP_SOURCE, source_row)

    scale = spread(table_ref, STRIP_SCALE)
    buffers = [b0, b1, b2, b3, b4]

    def image_of(ref, row):
        v = ref[row + 1]
        below, above = beside_x(v)
        beside = (below + above) + (ref[row] + ref[row + 2]) + (shift(v, 1) + shift(v, -1))
        return scale * (6.0 * v - beside), v

    for k in (1, 2, 3, 4):
        before = 4 - k

        def level_row(row, _, k=k, before=before):
            flag = row_flag(row, before, low, high)
            image, v = image_of(buffers[k - 1], row)
            value = level_value(k, image, v, buffers[2][row + 2] if k == 4 else None)
            buffers[k][row] = value * (flag * inside) if before else value
            return _

        over_rows(Y + 2 * before, STRIP_LEVEL[k - 1], level_row)

    def dot_row(row, sums):
        b = [buffers[k][row + 4 - k] for k in range(5)]
        for k in range(4):
            basis_ref[k, row] = b[k]
        return tuple(t + p for t, p in zip(sums, dot_terms(b)))

    sums = over_rows(Y, STRIP_DOT, dot_row, tuple(jnp.zeros((8, Z), F32) for _ in range(DOTS)))
    place = place[:8]
    edge = ((place >= HALO) & (place < 2 * HALO)) | ((place >= 22) & (place < 27))
    slot = lax.broadcasted_iota(jnp.int32, (8, SLOTS), 1)
    total = jnp.broadcast_to(table_ref[RANGE : RANGE + 1, :SLOTS], (8, SLOTS))
    for k in range(DOTS):
        both = jnp.where(edge, sums[k], 0.0) + dots_in_ref[k]
        one = jnp.sum(jnp.sum(both, axis=0, keepdims=True), axis=1, keepdims=True)
        total = jnp.where(slot == k, one, total)
    total_ref[...] = jnp.broadcast_to(total[:1], total_ref.shape)


def least_squares(h, r):
    n = 5
    root = [[None] * n for _ in range(n)]
    for i in range(n):
        rest = h[i][i]
        for k in range(i):
            rest = rest - root[k][i] * root[k][i]
        rest = jnp.maximum(rest, 3e-7 * h[i][i])
        inverse = lax.rsqrt(rest)
        root[i][i] = rest * inverse
        for j in range(i + 1, n):
            t = h[i][j]
            for k in range(i):
                t = t - root[k][i] * root[k][j]
            root[i][j] = t * inverse
    wide = 1.0 + r
    half = 0.5 * r
    columns = []
    for j, weights in enumerate((((0, 1.0), (1, r)), ((1, 1.0), (2, r)), ((2, wide), (3, r)), ((2, half), (3, wide), (4, half)))):
        column = []
        for i in range(j + 2):
            terms = [w * root[i][m] for m, w in weights if i <= m]
            column.append(sum(terms[1:], terms[0]))
        columns.append(column)
    target = [root[0][0]]
    cosines, sines, inverses = [], [], []
    for j in range(4):
        e = columns[j]
        for i in range(j):
            e[i], e[i + 1] = cosines[i] * e[i] + sines[i] * e[i + 1], cosines[i] * e[i + 1] - sines[i] * e[i]
        inverse = lax.rsqrt(e[j] * e[j] + e[j + 1] * e[j + 1])
        inverses.append(inverse)
        cosines.append(e[j] * inverse)
        sines.append(e[j + 1] * inverse)
        target.append(-sines[j] * target[j])
        target[j] = cosines[j] * target[j]
    y = [None] * 4
    for j in (3, 2, 1, 0):
        t = target[j]
        for k in range(j + 1, 4):
            t = t - columns[k][j] * y[k]
        y[j] = t * inverses[j]
    return y


def combine_kernel(sums_ref, others_ref, basis_ref, strip_ref, out_ref, held, strips, sems):
    total = jnp.sum(sums_ref[...] + others_ref[...], axis=0, keepdims=True)
    h00, h01, h03, h04, h11, h12, h13, h14, h22, h23, h33, h34, h44 = (total[:, k : k + 1] for k in range(DOTS))
    h = [
        [h00, h01, h11, h03, h04],
        [None, h11, h12, h13, h14],
        [None, None, h22, h23, 2.0 * h33 - h22],
        [None, None, None, h33, h34],
        [None, None, None, None, h44],
    ]
    y = [jnp.broadcast_to(c, (X, Z)) for c in least_squares(h, sums_ref[0:1, DOTS : DOTS + 1])]
    lane = lanes()
    for row in range(Y):
        strip = y[0] * strip_ref[0, row]
        for k in (1, 2, 3):
            strip = strip + y[k] * strip_ref[k, row]
        strips[row] = strip
    copies = []
    for s in range(SPECIES):
        for row in range(Y):
            v = y[0] * basis_ref[0, row, s]
            for k in (1, 2, 3):
                v = v + y[k] * basis_ref[k, row, s]
            strip = strips[row]
            v = jnp.where(lane < HALO, shift(strip, -(32 * s + HALO)), v)
            v = jnp.where(lane >= Z - HALO, shift(strip, Z - HALO - (32 * s + 22)), v)
            held[s, pl.ds(row, X, stride=Y), :] = v
        for half in range(2):
            part = pl.ds(half * (X * Y // 2), X * Y // 2)
            copy = pltpu.make_async_copy(held.at[s, part], out_ref.at[s, part], sems.at[2 * s + half])
            copy.start()
            copies.append(copy)
    for copy in copies:
        copy.wait()


def call(kernel, outs, spaces, scratch=(), flops=1000, out_space=VMEM):
    return pl.pallas_call(
        kernel,
        out_shape=outs,
        in_specs=[pl.BlockSpec(memory_space=m) for m in spaces],
        out_specs=jax.tree.map(lambda _: pl.BlockSpec(memory_space=out_space), outs),
        scratch_shapes=list(scratch),
        cost_estimate=pl.CostEstimate(flops=flops, bytes_accessed=1 << 20, transcendentals=0),
        compiler_params=pltpu.CompilerParams(vmem_limit_bytes=24 << 20),
    )


def shards(state, member_set, courant_table, diffusion_table, reaction_table, quadratic_table):
    gy, gh, gx = lax.axis_size("gy"), lax.axis_size("gh"), lax.axis_size("gx")
    gz = gh * gx
    up = [(i, (i + 1) % gy) for i in range(gy)]
    down = [(b, a) for a, b in up]
    far, near = [], []
    for i in range(gz - 1):
        (far if i % 2 else near).extend([(i, i + 1), (i + 1, i)])
    flat = state.reshape(SPECIES, X * Y, Z)

    edge = struct(HALO, SPECIES, X, Z)
    strip_edge = struct(HALO, X, Z)
    pack = struct(PACKS, X, Z)
    inputs = (flat, courant_table.T, diffusion_table.T, reaction_table.transpose(1, 2, 0), quadratic_table.T)
    own, top, bottom, strip, to_far, to_near, *tables = call(
        pack_kernel,
        (struct(Y, SPECIES, X, Z), edge, edge, struct(Y, X, Z), pack, pack, *(struct(*t.shape) for t in inputs[1:])),
        [pltpu.HBM] * len(inputs),
        [
            VMEM(flat.shape, F32),
            pltpu.SemaphoreType.DMA((SPECIES,)),
            pltpu.SemaphoreType.DMA((len(inputs) - 1,)),
        ],
    )(*(pltpu.with_memory_space_constraint(t, pltpu.HBM) for t in inputs))
    from_far = lax.ppermute(to_far, GZ, far)
    from_near = lax.ppermute(to_near, GZ, near)
    low = lax.ppermute(bottom, "gy", up)
    high = lax.ppermute(top, "gy", down)
    table = call(coefficient_kernel, struct(COEFFICIENTS, Z), [SMEM] + [VMEM] * 4)(member_set, *tables)
    wide = (SPECIES, X, Z)
    basis, dots = call(
        main_kernel,
        (struct(4, Y, *wide), struct(DOTS, 8, Z)),
        [VMEM] * 4,
        [VMEM((n, *wide), F32) for n in (ROWS, Y + 8, Y + 6, Y + 4, Y + 2, Y)],
        flops=10_000_000,
    )(own, low, high, table)
    strip, strip_top, strip_bottom = call(
        unpack_kernel, (struct(Y, X, Z), strip_edge, strip_edge), [VMEM] * 3
    )(strip, from_far, from_near)
    strip_low = lax.ppermute(strip_bottom, "gy", up)
    strip_high = lax.ppermute(strip_top, "gy", down)
    strip_basis, total = call(
        strip_kernel,
        (struct(4, Y, X, Z), struct(gy * gx, SLOTS)),
        [VMEM] * 5,
        [VMEM((n, X, Z), F32) for n in (ROWS, Y + 8, Y + 6, Y + 4, Y + 2, Y)],
    )(strip, strip_low, strip_high, dots, table)
    sums = lax.all_to_all(total, ("gy", "gx"), split_axis=0, concat_axis=0, tiled=True)
    others = lax.ppermute(sums, "gh", [(i, 1 - i) for i in range(gh)])
    out = call(
        combine_kernel,
        struct(SPECIES, X * Y, Z),
        [VMEM] * 4,
        [VMEM((SPECIES, X * Y, Z), F32), VMEM((Y, X, Z), F32), pltpu.SemaphoreType.DMA((2 * SPECIES,))],
        out_space=pltpu.HBM,
    )(sums, others, basis, strip_basis)
    return out.reshape(state.shape)


def solution(mesh):
    ens, gy, gz = (mesh.shape[a] for a in ("ens", "gy", "gz"))
    split = jax.sharding.Mesh(mesh.devices.reshape(ens, gy, 2, gz // 2), ("ens", "gy", *GZ))
    state_spec = P("ens", None, None, "gy", GZ)

    return jax.shard_map(
        shards,
        mesh=split,
        in_specs=(state_spec, P("ens"), P(), P(), P(), P()),
        out_specs=state_spec,
        check_vma=False,
    )
```

```python
import jax
import jax.numpy as jnp
from jax import lax
from jax.experimental import pallas as pl
from jax.experimental.pallas import tpu as pltpu
from jax.sharding import PartitionSpec as P


SPECIES = 4
X = 16
Y = 16
Z = 128
HALO = 5
GROUP = 6
PACKS = 3
ROWS = Y + 2 * HALO
DOTS = 13
SLOTS = 16
MAIN_SOURCE, MAIN_LEVEL, MAIN_DOT = 8, (11, 10, 9, 8), 4
STRIP_SOURCE, STRIP_LEVEL, STRIP_DOT = 12, (11, 10, 9, 8), 4

F32 = jnp.float32
VMEM = pltpu.VMEM
SMEM = pltpu.SMEM


def struct(*shape):
    return jax.ShapeDtypeStruct(shape, F32)


GZ = ("gh", "gx")


def z_index():
    return lax.axis_index("gh") * lax.axis_size("gx") + lax.axis_index("gx")


def z_size():
    return lax.axis_size("gh") * lax.axis_size("gx")


def lanes():
    return lax.broadcasted_iota(jnp.int32, (X, Z), 1)


def shift(v, amount):
    amount %= Z
    return pltpu.roll(v, amount, 1) if amount else v


def over_rows(count, at_once, body, carry=None):
    if at_once >= count:
        for row in range(count):
            carry = body(row, carry)
        return carry

    def step(i, c):
        for k in range(at_once):
            c = body(i * at_once + k, c)
        return c

    whole = count // at_once
    carry = lax.fori_loop(0, whole, step, carry)
    for row in range(whole * at_once, count):
        carry = body(row, carry)
    return carry


def unpack_kernel(strip_ref, far_ref, near_ref, full_ref, top_ref, bottom_ref):
    place = lanes() % 32
    odd = z_index() % 2 == 1
    for g in range(PACKS):
        far, near = far_ref[g], near_ref[g]
        after = jnp.where(odd, far, near)
        before = jnp.where(odd, near, far)
        for i in range(GROUP):
            y = g * GROUP + i
            if y < Y:
                v = strip_ref[y]
                v = jnp.where(place < HALO, shift(before, -i * HALO), v)
                v = jnp.where(place >= 27, shift(after, 27 - i * HALO), v)
                full_ref[y] = v
                if y < HALO:
                    top_ref[y] = v
                if y >= Y - HALO:
                    bottom_ref[y - (Y - HALO)] = v


def beside_x(v):
    row = lax.broadcasted_iota(jnp.int32, (X, Z), 0)
    below = jnp.where(row == 0, 0.0, pltpu.roll(v, 1, 0))
    above = jnp.where(row == X - 1, 0.0, pltpu.roll(v, X - 1, 0))
    return below, above


def in_grid():
    low = jnp.where(lax.axis_index("gy") > 0, 1.0, 0.0).astype(F32)
    high = jnp.where(lax.axis_index("gy") < lax.axis_size("gy") - 1, 1.0, 0.0).astype(F32)
    return low, high


def row_flag(row, before, low, high):
    if isinstance(row, int):
        return low if row < before else high if row >= before + Y else 1.0
    flag = jnp.where(row < before, low, 1.0)
    return jnp.where(row >= before + Y, high, flag)


PLUS, MINUS, LINEAR, QUAD, SCALE, TURNED, STRIP_QUAD, STRIP_SCALE, RANGE = 0, 3, 6, 22, 26, 30, 34, 35, 36
COEFFICIENTS = 40


def coefficient_kernel(member_ref, courant_ref, diffusion_ref, reaction_ref, quadratic_ref, out_ref):
    hot = lax.broadcasted_iota(jnp.int32, (1, courant_ref.shape[-1]), 1) == member_ref[0]

    def picked(table):
        return jnp.sum(jnp.where(hot, table, 0.0), axis=1, keepdims=True)

    def put(row, value):
        out_ref[row : row + 1, :] = jnp.broadcast_to(value, (1, Z))

    lane = lax.broadcasted_iota(jnp.int32, (1, Z), 1)

    def by_species(values):
        out = jnp.broadcast_to(values[3], (1, Z))
        for s in (2, 1, 0):
            out = jnp.where(lane < 32 * (s + 1), values[s], out)
        return out

    courant = picked(courant_ref[...])
    plus, minus = jnp.maximum(courant, 0.0), jnp.minimum(courant, 0.0)
    kept = jnp.ones((1, 1), F32)
    for d in range(3):
        put(PLUS + d, plus[d : d + 1])
        put(MINUS + d, minus[d : d + 1])
        kept = kept - (plus[d : d + 1] - minus[d : d + 1])
    linear = []
    for k in range(SPECIES):
        rates = picked(reaction_ref[k])
        linear.append([rates[l : l + 1] for l in range(SPECIES)])
        linear[k][k] = linear[k][k] + kept
        for l in range(SPECIES):
            put(LINEAR + SPECIES * k + l, linear[k][l])
    for t in range(SPECIES):
        put(TURNED + t, by_species([linear[k][(k - t) % SPECIES] for k in range(SPECIES)]))
    rates = picked(quadratic_ref[...])
    quad = [rates[k : k + 1] for k in range(SPECIES)]
    d = picked(diffusion_ref[...])
    d = [d[k : k + 1] for k in range(SPECIES)]
    reach = 6.0 * jnp.maximum(jnp.maximum(d[0], d[1]), jnp.maximum(d[2], d[3]))
    scale = [v / reach for v in d]
    for k in range(SPECIES):
        put(QUAD + k, quad[k])
        put(SCALE + k, scale[k])
    put(STRIP_QUAD, by_species(quad))
    put(STRIP_SCALE, by_species(scale))
    put(RANGE, reach)


def pack_kernel(
    state_ref, courant_ref, diffusion_ref, reaction_ref, quadratic_ref,
    own_ref, top_ref, bottom_ref, strip_ref, far_ref, near_ref, courant, diffusion, reaction, quadratic,
    state, state_sems, sems,
):
    blocks = [pltpu.make_async_copy(state_ref.at[s], state.at[s], state_sems.at[s]) for s in range(SPECIES)]
    tables = (
        (courant_ref, courant), (diffusion_ref, diffusion), (reaction_ref, reaction),
        (quadratic_ref, quadratic),
    )
    copies = [pltpu.make_async_copy(a, b, sems.at[i]) for i, (a, b) in enumerate(tables)]
    for copy in blocks + copies:
        copy.start()
    lane = lanes()
    odd = z_index() % 2 == 1
    place = lane % 32
    for s in range(SPECIES):
        blocks[s].wait()
        for y in range(Y):
            v = state[s, pl.ds(y, X, stride=Y), :]
            own_ref[y, s] = v
            if y < HALO:
                top_ref[y, s] = v
            if y >= Y - HALO:
                bottom_ref[y - (Y - HALO), s] = v
            total = strip_ref[y] if s else jnp.zeros((X, Z), F32)
            low = shift(v, 32 * s + HALO)
            high = shift(v, 32 * s + 16 - (Z - 11))
            total = jnp.where((lane >= 32 * s + HALO) & (lane < 32 * s + 16), low, total)
            total = jnp.where((lane >= 32 * s + 16) & (lane < 32 * s + 27), high, total)
            strip_ref[y] = total
    for g in range(PACKS):
        lows = jnp.zeros((X, Z), F32)
        highs = jnp.zeros((X, Z), F32)
        for i in range(GROUP):
            if g * GROUP + i < Y:
                v = strip_ref[g * GROUP + i]
                here = (place >= i * HALO) & (place < (i + 1) * HALO)
                lows = jnp.where(here, shift(v, i * HALO - HALO), lows)
                highs = jnp.where(here, shift(v, i * HALO - 22), highs)
        far_ref[g] = jnp.where(odd, highs, lows)
        near_ref[g] = jnp.where(odd, lows, highs)
    for copy in copies:
        copy.wait()


def spread(table_ref, row):
    return jnp.broadcast_to(table_ref[row : row + 1, :], (X, Z))


def dot_terms(b):
    pairs = ((0, 0), (0, 1), (0, 3), (0, 4), (1, 1), (1, 2), (1, 3), (1, 4), (2, 2), (2, 3), (3, 3), (3, 4), (4, 4))
    out = []
    for i, j in pairs:
        p = b[i] * b[j]
        out.append(p[:8] + p[8:])
    return out


def level_value(k, image, v, before):
    if k < 3:
        return image
    if k == 3:
        return image - v
    return 2.0 * (image - v) - before


def main_kernel(own_ref, low_ref, high_ref, table_ref, basis_ref, dots_ref, wide, b0, b1, b2, b3, b4):
    low, high = in_grid()
    for r in range(HALO):
        for s in range(SPECIES):
            wide[r, s] = low_ref[r, s] * low
            wide[HALO + Y + r, s] = high_ref[r, s] * high
    for y in range(Y):
        for s in range(SPECIES):
            wide[HALO + y, s] = own_ref[y, s]

    plus = [spread(table_ref, PLUS + d) for d in range(3)]
    minus = [spread(table_ref, MINUS + d) for d in range(3)]
    linear = [[spread(table_ref, LINEAR + SPECIES * k + l) for l in range(SPECIES)] for k in range(SPECIES)]
    quad = [spread(table_ref, QUAD + k) for k in range(SPECIES)]

    def source_row(row, _):
        flag = row_flag(row, HALO - 1, low, high)
        v = [wide[row + 1, s] for s in range(SPECIES)]
        a, b = v[0], v[1]
        coupled = a * b / (1.0 + a * a + b * b)
        for k in range(SPECIES):
            below, above = beside_x(v[k])
            out = plus[0] * below - minus[0] * above
            out = out + (plus[1] * wide[row, k] - minus[1] * wide[row + 2, k])
            out = out + (plus[2] * shift(v[k], 1) - minus[2] * shift(v[k], -1))
            for l in range(SPECIES):
                out = out + linear[k][l] * v[l]
            b0[row, k] = (out + quad[k] * coupled) * flag
        return _

    over_rows(Y + 8, MAIN_SOURCE, source_row)

    scale = [spread(table_ref, SCALE + s) for s in range(SPECIES)]
    buffers = [b0, b1, b2, b3, b4]

    def image_of(ref, row, s):
        v = ref[row + 1, s]
        below, above = beside_x(v)
        beside = (below + above) + (ref[row, s] + ref[row + 2, s]) + (shift(v, 1) + shift(v, -1))
        return scale[s] * (6.0 * v - beside), v

    for k in (1, 2, 3, 4):
        before = 4 - k

        def level_row(row, _, k=k, before=before):
            flag = row_flag(row, before, low, high)
            for s in range(SPECIES):
                image, v = image_of(buffers[k - 1], row, s)
                value = level_value(k, image, v, buffers[2][row + 2, s] if k == 4 else None)
                buffers[k][row, s] = value * flag if before else value
            return _

        over_rows(Y + 2 * before, MAIN_LEVEL[k - 1], level_row)

    def dot_row(row, sums):
        sums = list(sums)
        for s in range(SPECIES):
            b = [buffers[k][row + 4 - k, s] for k in range(5)]
            for k in range(4):
                basis_ref[k, row, s] = b[k]
            sums = [t + p for t, p in zip(sums, dot_terms(b))]
        return tuple(sums)

    sums = over_rows(Y, MAIN_DOT, dot_row, tuple(jnp.zeros((8, Z), F32) for _ in range(DOTS)))
    lane = lax.broadcasted_iota(jnp.int32, (8, Z), 1)
    inner = (lane >= HALO) & (lane < Z - HALO)
    for k in range(DOTS):
        dots_ref[k] = jnp.where(inner, sums[k], 0.0)


def strip_kernel(
    strip_ref, low_ref, high_ref, dots_in_ref, table_ref, basis_ref, total_ref, wide, b0, b1, b2, b3, b4
):
    low, high = in_grid()
    for r in range(HALO):
        wide[r] = low_ref[r] * low
        wide[HALO + Y + r] = high_ref[r] * high
    for y in range(Y):
        wide[HALO + y] = strip_ref[y]

    lane = lanes()
    place = lane % 32
    species = lane // 32
    first = jnp.where(z_index() > 0, 1.0, 0.0).astype(F32)
    last = jnp.where(z_index() < z_size() - 1, 1.0, 0.0).astype(F32)
    inside = jnp.where(place < HALO, first, jnp.where(place >= 27, last, 1.0))
    plus = [spread(table_ref, PLUS + d) for d in range(3)]
    minus = [spread(table_ref, MINUS + d) for d in range(3)]
    linear = [spread(table_ref, TURNED + t) for t in range(SPECIES)]
    quad = spread(table_ref, STRIP_QUAD)

    def source_row(row, _):
        flag = row_flag(row, HALO - 1, low, high)
        v = wide[row + 1]
        turned = [v] + [shift(v, 32 * t) for t in range(1, SPECIES)]
        a, b = turned[3], turned[2]
        for t in (2, 1, 0):
            a = jnp.where(species == t, turned[t], a)
            b = jnp.where(species == (t + 1) % SPECIES, turned[t], b) if t != 2 else jnp.where(species == 0, turned[3], b)
        coupled = a * b / (1.0 + a * a + b * b)
        below, above = beside_x(v)
        out = plus[0] * below - minus[0] * above
        out = out + (plus[1] * wide[row] - minus[1] * wide[row + 2])
        out = out + (plus[2] * shift(v, 1) - minus[2] * shift(v, -1))
        for t in range(SPECIES):
            out = out + linear[t] * turned[t]
        b0[row] = (out + quad * coupled) * (flag * inside)
        return _

    over_rows(Y + 8, STRIP_SOURCE, source_row)

    scale = spread(table_ref, STRIP_SCALE)
    buffers = [b0, b1, b2, b3, b4]

    def image_of(ref, row):
        v = ref[row + 1]
        below, above = beside_x(v)
        beside = (below + above) + (ref[row] + ref[row + 2]) + (shift(v, 1) + shift(v, -1))
        return scale * (6.0 * v - beside), v

    for k in (1, 2, 3, 4):
        before = 4 - k

        def level_row(row, _, k=k, before=before):
            flag = row_flag(row, before, low, high)
            image, v = image_of(buffers[k - 1], row)
            value = level_value(k, image, v, buffers[2][row + 2] if k == 4 else None)
            buffers[k][row] = value * (flag * inside) if before else value
            return _

        over_rows(Y + 2 * before, STRIP_LEVEL[k - 1], level_row)

    def dot_row(row, sums):
        b = [buffers[k][row + 4 - k] for k in range(5)]
        for k in range(4):
            basis_ref[k, row] = b[k]
        return tuple(t + p for t, p in zip(sums, dot_terms(b)))

    sums = over_rows(Y, STRIP_DOT, dot_row, tuple(jnp.zeros((8, Z), F32) for _ in range(DOTS)))
    place = place[:8]
    edge = ((place >= HALO) & (place < 2 * HALO)) | ((place >= 22) & (place < 27))
    slot = lax.broadcasted_iota(jnp.int32, (8, SLOTS), 1)
    total = jnp.broadcast_to(table_ref[RANGE : RANGE + 1, :SLOTS], (8, SLOTS))
    for k in range(DOTS):
        both = jnp.where(edge, sums[k], 0.0) + dots_in_ref[k]
        one = jnp.sum(jnp.sum(both, axis=0, keepdims=True), axis=1, keepdims=True)
        total = jnp.where(slot == k, one, total)
    total_ref[...] = jnp.broadcast_to(total[:1], total_ref.shape)


def least_squares(h, r):
    n = 5
    root = [[None] * n for _ in range(n)]
    for i in range(n):
        rest = h[i][i]
        for k in range(i):
            rest = rest - root[k][i] * root[k][i]
        rest = jnp.maximum(rest, 3e-7 * h[i][i])
        inverse = lax.rsqrt(rest)
        root[i][i] = rest * inverse
        for j in range(i + 1, n):
            t = h[i][j]
            for k in range(i):
                t = t - root[k][i] * root[k][j]
            root[i][j] = t * inverse
    wide = 1.0 + r
    half = 0.5 * r
    columns = []
    for j, weights in enumerate((((0, 1.0), (1, r)), ((1, 1.0), (2, r)), ((2, wide), (3, r)), ((2, half), (3, wide), (4, half)))):
        column = []
        for i in range(j + 2):
            terms = [w * root[i][m] for m, w in weights if i <= m]
            column.append(sum(terms[1:], terms[0]))
        columns.append(column)
    target = [root[0][0]]
    cosines, sines, inverses = [], [], []
    for j in range(4):
        e = columns[j]
        for i in range(j):
            e[i], e[i + 1] = cosines[i] * e[i] + sines[i] * e[i + 1], cosines[i] * e[i + 1] - sines[i] * e[i]
        inverse = lax.rsqrt(e[j] * e[j] + e[j + 1] * e[j + 1])
        inverses.append(inverse)
        cosines.append(e[j] * inverse)
        sines.append(e[j + 1] * inverse)
        target.append(-sines[j] * target[j])
        target[j] = cosines[j] * target[j]
    y = [None] * 4
    for j in (3, 2, 1, 0):
        t = target[j]
        for k in range(j + 1, 4):
            t = t - columns[k][j] * y[k]
        y[j] = t * inverses[j]
    return y


def combine_kernel(sums_ref, basis_ref, strip_ref, out_ref, held, strips, sems):
    total = jnp.sum(sums_ref[...], axis=0, keepdims=True)
    h00, h01, h03, h04, h11, h12, h13, h14, h22, h23, h33, h34, h44 = (total[:, k : k + 1] for k in range(DOTS))
    h = [
        [h00, h01, h11, h03, h04],
        [None, h11, h12, h13, h14],
        [None, None, h22, h23, 2.0 * h33 - h22],
        [None, None, None, h33, h34],
        [None, None, None, None, h44],
    ]
    y = [jnp.broadcast_to(c, (X, Z)) for c in least_squares(h, sums_ref[0:1, DOTS : DOTS + 1])]
    lane = lanes()
    for row in range(Y):
        strip = y[0] * strip_ref[0, row]
        for k in (1, 2, 3):
            strip = strip + y[k] * strip_ref[k, row]
        strips[row] = strip
    copies = []
    for s in range(SPECIES):
        for row in range(Y):
            v = y[0] * basis_ref[0, row, s]
            for k in (1, 2, 3):
                v = v + y[k] * basis_ref[k, row, s]
            strip = strips[row]
            v = jnp.where(lane < HALO, shift(strip, -(32 * s + HALO)), v)
            v = jnp.where(lane >= Z - HALO, shift(strip, Z - HALO - (32 * s + 22)), v)
            held[s, pl.ds(row, X, stride=Y), :] = v
        for half in range(2):
            part = pl.ds(half * (X * Y // 2), X * Y // 2)
            copy = pltpu.make_async_copy(held.at[s, part], out_ref.at[s, part], sems.at[2 * s + half])
            copy.start()
            copies.append(copy)
    for copy in copies:
        copy.wait()


def call(kernel, outs, spaces, scratch=(), flops=1000, out_space=VMEM):
    return pl.pallas_call(
        kernel,
        out_shape=outs,
        in_specs=[pl.BlockSpec(memory_space=m) for m in spaces],
        out_specs=jax.tree.map(lambda _: pl.BlockSpec(memory_space=out_space), outs),
        scratch_shapes=list(scratch),
        cost_estimate=pl.CostEstimate(flops=flops, bytes_accessed=1 << 20, transcendentals=0),
        compiler_params=pltpu.CompilerParams(vmem_limit_bytes=24 << 20),
    )


def shards(state, member_set, courant_table, diffusion_table, reaction_table, quadratic_table):
    gy, gh, gx = lax.axis_size("gy"), lax.axis_size("gh"), lax.axis_size("gx")
    gz = gh * gx
    up = [(i, (i + 1) % gy) for i in range(gy)]
    down = [(b, a) for a, b in up]
    far, near = [], []
    for i in range(gz - 1):
        (far if i % 2 else near).extend([(i, i + 1), (i + 1, i)])
    flat = state.reshape(SPECIES, X * Y, Z)

    edge = struct(HALO, SPECIES, X, Z)
    strip_edge = struct(HALO, X, Z)
    pack = struct(PACKS, X, Z)
    inputs = (flat, courant_table.T, diffusion_table.T, reaction_table.transpose(1, 2, 0), quadratic_table.T)
    own, top, bottom, strip, to_far, to_near, *tables = call(
        pack_kernel,
        (struct(Y, SPECIES, X, Z), edge, edge, struct(Y, X, Z), pack, pack, *(struct(*t.shape) for t in inputs[1:])),
        [pltpu.HBM] * len(inputs),
        [
            VMEM(flat.shape, F32),
            pltpu.SemaphoreType.DMA((SPECIES,)),
            pltpu.SemaphoreType.DMA((len(inputs) - 1,)),
        ],
    )(*(pltpu.with_memory_space_constraint(t, pltpu.HBM) for t in inputs))
    from_far = lax.ppermute(to_far, GZ, far)
    from_near = lax.ppermute(to_near, GZ, near)
    low = lax.ppermute(bottom, "gy", up)
    high = lax.ppermute(top, "gy", down)
    table = call(coefficient_kernel, struct(COEFFICIENTS, Z), [SMEM] + [VMEM] * 4)(member_set, *tables)
    wide = (SPECIES, X, Z)
    basis, dots = call(
        main_kernel,
        (struct(4, Y, *wide), struct(DOTS, 8, Z)),
        [VMEM] * 4,
        [VMEM((n, *wide), F32) for n in (ROWS, Y + 8, Y + 6, Y + 4, Y + 2, Y)],
        flops=10_000_000,
    )(own, low, high, table)
    strip, strip_top, strip_bottom = call(
        unpack_kernel, (struct(Y, X, Z), strip_edge, strip_edge), [VMEM] * 3
    )(strip, from_far, from_near)
    strip_low = lax.ppermute(strip_bottom, "gy", up)
    strip_high = lax.ppermute(strip_top, "gy", down)
    strip_basis, total = call(
        strip_kernel,
        (struct(4, Y, X, Z), struct(gy * gz, SLOTS)),
        [VMEM] * 5,
        [VMEM((n, X, Z), F32) for n in (ROWS, Y + 8, Y + 6, Y + 4, Y + 2, Y)],
    )(strip, strip_low, strip_high, dots, table)
    sums = lax.all_to_all(total, ("gy", *GZ), split_axis=0, concat_axis=0, tiled=True)
    out = call(
        combine_kernel,
        struct(SPECIES, X * Y, Z),
        [VMEM] * 3,
        [VMEM((SPECIES, X * Y, Z), F32), VMEM((Y, X, Z), F32), pltpu.SemaphoreType.DMA((2 * SPECIES,))],
        out_space=pltpu.HBM,
    )(sums, basis, strip_basis)
    return out.reshape(state.shape)


def solution(mesh):
    ens, gy, gz = (mesh.shape[a] for a in ("ens", "gy", "gz"))
    split = jax.sharding.Mesh(mesh.devices.reshape(ens, gy, 2, gz // 2), ("ens", "gy", *GZ))
    state_spec = P("ens", None, None, "gy", GZ)

    return jax.shard_map(
        shards,
        mesh=split,
        in_specs=(state_spec, P("ens"), P(), P(), P(), P()),
        out_specs=state_spec,
        check_vma=False,
    )
```

```python
import jax
import jax.numpy as jnp
from jax import lax
from jax.experimental import pallas as pl
from jax.experimental.pallas import tpu as pltpu
from jax.sharding import PartitionSpec as P


SPECIES = 4
X = 16
Y = 16
Z = 128
HALO = 5
GROUP = 6
PACKS = 3
ROWS = Y + 2 * HALO
DOTS = 13
SLOTS = 16
MAIN_SOURCE, MAIN_LEVEL, MAIN_DOT = 24, (22, 20, 18, 16), 16
STRIP_SOURCE, STRIP_LEVEL, STRIP_DOT = 24, (22, 20, 18, 16), 4

F32 = jnp.float32
VMEM = pltpu.VMEM
SMEM = pltpu.SMEM


def struct(*shape):
    return jax.ShapeDtypeStruct(shape, F32)


GZ = ("gh", "gx")


def z_index():
    return lax.axis_index("gh") * lax.axis_size("gx") + lax.axis_index("gx")


def z_size():
    return lax.axis_size("gh") * lax.axis_size("gx")


def lanes():
    return lax.broadcasted_iota(jnp.int32, (X, Z), 1)


def shift(v, amount):
    amount %= Z
    return pltpu.roll(v, amount, 1) if amount else v


def over_rows(count, at_once, body, carry=None):
    if at_once >= count:
        for row in range(count):
            carry = body(row, carry)
        return carry

    def step(i, c):
        for k in range(at_once):
            c = body(i * at_once + k, c)
        return c

    whole = count // at_once
    carry = lax.fori_loop(0, whole, step, carry)
    for row in range(whole * at_once, count):
        carry = body(row, carry)
    return carry


def unpack_kernel(strip_ref, far_ref, near_ref, full_ref, top_ref, bottom_ref):
    place = lanes() % 32
    odd = z_index() % 2 == 1
    for g in range(PACKS):
        far, near = far_ref[g], near_ref[g]
        after = jnp.where(odd, far, near)
        before = jnp.where(odd, near, far)
        for i in range(GROUP):
            y = g * GROUP + i
            if y < Y:
                v = strip_ref[y]
                v = jnp.where(place < HALO, shift(before, -i * HALO), v)
                v = jnp.where(place >= 27, shift(after, 27 - i * HALO), v)
                full_ref[y] = v
                if y < HALO:
                    top_ref[y] = v
                if y >= Y - HALO:
                    bottom_ref[y - (Y - HALO)] = v


def beside_x(v):
    row = lax.broadcasted_iota(jnp.int32, (X, Z), 0)
    below = jnp.where(row == 0, 0.0, pltpu.roll(v, 1, 0))
    above = jnp.where(row == X - 1, 0.0, pltpu.roll(v, X - 1, 0))
    return below, above


def in_grid():
    low = jnp.where(lax.axis_index("gy") > 0, 1.0, 0.0).astype(F32)
    high = jnp.where(lax.axis_index("gy") < lax.axis_size("gy") - 1, 1.0, 0.0).astype(F32)
    return low, high


def row_flag(row, before, low, high):
    if isinstance(row, int):
        return low if row < before else high if row >= before + Y else 1.0
    flag = jnp.where(row < before, low, 1.0)
    return jnp.where(row >= before + Y, high, flag)


PLUS, MINUS, LINEAR, QUAD, SCALE, TURNED, STRIP_QUAD, STRIP_SCALE, RANGE = 0, 3, 6, 22, 26, 30, 34, 35, 36
COEFFICIENTS = 40


def coefficient_kernel(member_ref, courant_ref, diffusion_ref, reaction_ref, quadratic_ref, out_ref):
    hot = lax.broadcasted_iota(jnp.int32, (1, courant_ref.shape[-1]), 1) == member_ref[0]

    def picked(table):
        return jnp.sum(jnp.where(hot, table, 0.0), axis=1, keepdims=True)

    def put(row, value):
        out_ref[row : row + 1, :] = jnp.broadcast_to(value, (1, Z))

    lane = lax.broadcasted_iota(jnp.int32, (1, Z), 1)

    def by_species(values):
        out = jnp.broadcast_to(values[3], (1, Z))
        for s in (2, 1, 0):
            out = jnp.where(lane < 32 * (s + 1), values[s], out)
        return out

    courant = picked(courant_ref[...])
    plus, minus = jnp.maximum(courant, 0.0), jnp.minimum(courant, 0.0)
    kept = jnp.ones((1, 1), F32)
    for d in range(3):
        put(PLUS + d, plus[d : d + 1])
        put(MINUS + d, minus[d : d + 1])
        kept = kept - (plus[d : d + 1] - minus[d : d + 1])
    linear = []
    for k in range(SPECIES):
        rates = picked(reaction_ref[k])
        linear.append([rates[l : l + 1] for l in range(SPECIES)])
        linear[k][k] = linear[k][k] + kept
        for l in range(SPECIES):
            put(LINEAR + SPECIES * k + l, linear[k][l])
    for t in range(SPECIES):
        put(TURNED + t, by_species([linear[k][(k - t) % SPECIES] for k in range(SPECIES)]))
    rates = picked(quadratic_ref[...])
    quad = [rates[k : k + 1] for k in range(SPECIES)]
    d = picked(diffusion_ref[...])
    d = [d[k : k + 1] for k in range(SPECIES)]
    reach = 6.0 * jnp.maximum(jnp.maximum(d[0], d[1]), jnp.maximum(d[2], d[3]))
    scale = [v / reach for v in d]
    for k in range(SPECIES):
        put(QUAD + k, quad[k])
        put(SCALE + k, scale[k])
    put(STRIP_QUAD, by_species(quad))
    put(STRIP_SCALE, by_species(scale))
    put(RANGE, reach)


def pack_kernel(
    state_ref, courant_ref, diffusion_ref, reaction_ref, quadratic_ref,
    own_ref, top_ref, bottom_ref, strip_ref, far_ref, near_ref, courant, diffusion, reaction, quadratic,
    state, state_sems, sems,
):
    blocks = [pltpu.make_async_copy(state_ref.at[s], state.at[s], state_sems.at[s]) for s in range(SPECIES)]
    tables = (
        (courant_ref, courant), (diffusion_ref, diffusion), (reaction_ref, reaction),
        (quadratic_ref, quadratic),
    )
    copies = [pltpu.make_async_copy(a, b, sems.at[i]) for i, (a, b) in enumerate(tables)]
    for copy in blocks + copies:
        copy.start()
    lane = lanes()
    odd = z_index() % 2 == 1
    place = lane % 32
    for s in range(SPECIES):
        blocks[s].wait()
        for y in range(Y):
            v = state[s, pl.ds(y, X, stride=Y), :]
            own_ref[y, s] = v
            if y < HALO:
                top_ref[y, s] = v
            if y >= Y - HALO:
                bottom_ref[y - (Y - HALO), s] = v
            total = strip_ref[y] if s else jnp.zeros((X, Z), F32)
            low = shift(v, 32 * s + HALO)
            high = shift(v, 32 * s + 16 - (Z - 11))
            total = jnp.where((lane >= 32 * s + HALO) & (lane < 32 * s + 16), low, total)
            total = jnp.where((lane >= 32 * s + 16) & (lane < 32 * s + 27), high, total)
            strip_ref[y] = total
    for g in range(PACKS):
        lows = jnp.zeros((X, Z), F32)
        highs = jnp.zeros((X, Z), F32)
        for i in range(GROUP):
            if g * GROUP + i < Y:
                v = strip_ref[g * GROUP + i]
                here = (place >= i * HALO) & (place < (i + 1) * HALO)
                lows = jnp.where(here, shift(v, i * HALO - HALO), lows)
                highs = jnp.where(here, shift(v, i * HALO - 22), highs)
        far_ref[g] = jnp.where(odd, highs, lows)
        near_ref[g] = jnp.where(odd, lows, highs)
    for copy in copies:
        copy.wait()


def spread(table_ref, row):
    return jnp.broadcast_to(table_ref[row : row + 1, :], (X, Z))


def dot_terms(b):
    pairs = ((0, 0), (0, 1), (0, 3), (0, 4), (1, 1), (1, 2), (1, 3), (1, 4), (2, 2), (2, 3), (3, 3), (3, 4), (4, 4))
    out = []
    for i, j in pairs:
        p = b[i] * b[j]
        out.append(p[:8] + p[8:])
    return out


def level_value(k, image, v, before):
    if k < 3:
        return image
    if k == 3:
        return image - v
    return 2.0 * (image - v) - before


def main_kernel(own_ref, low_ref, high_ref, table_ref, basis_ref, dots_ref, wide, b0, b1, b2, b3, b4):
    low, high = in_grid()
    for r in range(HALO):
        for s in range(SPECIES):
            wide[r, s] = low_ref[r, s] * low
            wide[HALO + Y + r, s] = high_ref[r, s] * high
    for y in range(Y):
        for s in range(SPECIES):
            wide[HALO + y, s] = own_ref[y, s]

    plus = [spread(table_ref, PLUS + d) for d in range(3)]
    minus = [spread(table_ref, MINUS + d) for d in range(3)]
    linear = [[spread(table_ref, LINEAR + SPECIES * k + l) for l in range(SPECIES)] for k in range(SPECIES)]
    quad = [spread(table_ref, QUAD + k) for k in range(SPECIES)]

    def source_row(row, _):
        flag = row_flag(row, HALO - 1, low, high)
        v = [wide[row + 1, s] for s in range(SPECIES)]
        a, b = v[0], v[1]
        coupled = a * b / (1.0 + a * a + b * b)
        for k in range(SPECIES):
            below, above = beside_x(v[k])
            out = plus[0] * below - minus[0] * above
            out = out + (plus[1] * wide[row, k] - minus[1] * wide[row + 2, k])
            out = out + (plus[2] * shift(v[k], 1) - minus[2] * shift(v[k], -1))
            for l in range(SPECIES):
                out = out + linear[k][l] * v[l]
            b0[row, k] = (out + quad[k] * coupled) * flag
        return _

    over_rows(Y + 8, MAIN_SOURCE, source_row)

    scale = [spread(table_ref, SCALE + s) for s in range(SPECIES)]
    buffers = [b0, b1, b2, b3, b4]

    def image_of(ref, row, s):
        v = ref[row + 1, s]
        below, above = beside_x(v)
        beside = (below + above) + (ref[row, s] + ref[row + 2, s]) + (shift(v, 1) + shift(v, -1))
        return scale[s] * (6.0 * v - beside), v

    for k in (1, 2, 3, 4):
        before = 4 - k

        def level_row(row, _, k=k, before=before):
            flag = row_flag(row, before, low, high)
            for s in range(SPECIES):
                image, v = image_of(buffers[k - 1], row, s)
                value = level_value(k, image, v, buffers[2][row + 2, s] if k == 4 else None)
                buffers[k][row, s] = value * flag if before else value
            return _

        over_rows(Y + 2 * before, MAIN_LEVEL[k - 1], level_row)

    def dot_row(row, sums):
        sums = list(sums)
        for s in range(SPECIES):
            b = [buffers[k][row + 4 - k, s] for k in range(5)]
            for k in range(4):
                basis_ref[k, row, s] = b[k]
            sums = [t + p for t, p in zip(sums, dot_terms(b))]
        return tuple(sums)

    sums = over_rows(Y, MAIN_DOT, dot_row, tuple(jnp.zeros((8, Z), F32) for _ in range(DOTS)))
    lane = lax.broadcasted_iota(jnp.int32, (8, Z), 1)
    inner = (lane >= HALO) & (lane < Z - HALO)
    for k in range(DOTS):
        dots_ref[k] = jnp.where(inner, sums[k], 0.0)


def strip_kernel(
    strip_ref, low_ref, high_ref, dots_in_ref, table_ref, basis_ref, total_ref, wide, b0, b1, b2, b3, b4
):
    low, high = in_grid()
    for r in range(HALO):
        wide[r] = low_ref[r] * low
        wide[HALO + Y + r] = high_ref[r] * high
    for y in range(Y):
        wide[HALO + y] = strip_ref[y]

    lane = lanes()
    place = lane % 32
    species = lane // 32
    first = jnp.where(z_index() > 0, 1.0, 0.0).astype(F32)
    last = jnp.where(z_index() < z_size() - 1, 1.0, 0.0).astype(F32)
    inside = jnp.where(place < HALO, first, jnp.where(place >= 27, last, 1.0))
    plus = [spread(table_ref, PLUS + d) for d in range(3)]
    minus = [spread(table_ref, MINUS + d) for d in range(3)]
    linear = [spread(table_ref, TURNED + t) for t in range(SPECIES)]
    quad = spread(table_ref, STRIP_QUAD)

    def source_row(row, _):
        flag = row_flag(row, HALO - 1, low, high)
        v = wide[row + 1]
        turned = [v] + [shift(v, 32 * t) for t in range(1, SPECIES)]
        a, b = turned[3], turned[2]
        for t in (2, 1, 0):
            a = jnp.where(species == t, turned[t], a)
            b = jnp.where(species == (t + 1) % SPECIES, turned[t], b) if t != 2 else jnp.where(species == 0, turned[3], b)
        coupled = a * b / (1.0 + a * a + b * b)
        below, above = beside_x(v)
        out = plus[0] * below - minus[0] * above
        out = out + (plus[1] * wide[row] - minus[1] * wide[row + 2])
        out = out + (plus[2] * shift(v, 1) - minus[2] * shift(v, -1))
        for t in range(SPECIES):
            out = out + linear[t] * turned[t]
        b0[row] = (out + quad * coupled) * (flag * inside)
        return _

    over_rows(Y + 8, STRIP_SOURCE, source_row)

    scale = spread(table_ref, STRIP_SCALE)
    buffers = [b0, b1, b2, b3, b4]

    def image_of(ref, row):
        v = ref[row + 1]
        below, above = beside_x(v)
        beside = (below + above) + (ref[row] + ref[row + 2]) + (shift(v, 1) + shift(v, -1))
        return scale * (6.0 * v - beside), v

    for k in (1, 2, 3, 4):
        before = 4 - k

        def level_row(row, _, k=k, before=before):
            flag = row_flag(row, before, low, high)
            image, v = image_of(buffers[k - 1], row)
            value = level_value(k, image, v, buffers[2][row + 2] if k == 4 else None)
            buffers[k][row] = value * (flag * inside) if before else value
            return _

        over_rows(Y + 2 * before, STRIP_LEVEL[k - 1], level_row)

    def dot_row(row, sums):
        b = [buffers[k][row + 4 - k] for k in range(5)]
        for k in range(4):
            basis_ref[k, row] = b[k]
        return tuple(t + p for t, p in zip(sums, dot_terms(b)))

    sums = over_rows(Y, STRIP_DOT, dot_row, tuple(jnp.zeros((8, Z), F32) for _ in range(DOTS)))
    place = place[:8]
    edge = ((place >= HALO) & (place < 2 * HALO)) | ((place >= 22) & (place < 27))
    slot = lax.broadcasted_iota(jnp.int32, (8, SLOTS), 1)
    total = jnp.broadcast_to(table_ref[RANGE : RANGE + 1, :SLOTS], (8, SLOTS))
    for k in range(DOTS):
        both = jnp.where(edge, sums[k], 0.0) + dots_in_ref[k]
        one = jnp.sum(jnp.sum(both, axis=0, keepdims=True), axis=1, keepdims=True)
        total = jnp.where(slot == k, one, total)
    total_ref[...] = jnp.broadcast_to(total[:1], total_ref.shape)


def least_squares(h, r):
    n = 5
    root = [[None] * n for _ in range(n)]
    for i in range(n):
        rest = h[i][i]
        for k in range(i):
            rest = rest - root[k][i] * root[k][i]
        rest = jnp.maximum(rest, 3e-7 * h[i][i])
        inverse = lax.rsqrt(rest)
        root[i][i] = rest * inverse
        for j in range(i + 1, n):
            t = h[i][j]
            for k in range(i):
                t = t - root[k][i] * root[k][j]
            root[i][j] = t * inverse
    wide = 1.0 + r
    half = 0.5 * r
    columns = []
    for j, weights in enumerate((((0, 1.0), (1, r)), ((1, 1.0), (2, r)), ((2, wide), (3, r)), ((2, half), (3, wide), (4, half)))):
        column = []
        for i in range(j + 2):
            terms = [w * root[i][m] for m, w in weights if i <= m]
            column.append(sum(terms[1:], terms[0]))
        columns.append(column)
    target = [root[0][0]]
    cosines, sines, inverses = [], [], []
    for j in range(4):
        e = columns[j]
        for i in range(j):
            e[i], e[i + 1] = cosines[i] * e[i] + sines[i] * e[i + 1], cosines[i] * e[i + 1] - sines[i] * e[i]
        inverse = lax.rsqrt(e[j] * e[j] + e[j + 1] * e[j + 1])
        inverses.append(inverse)
        cosines.append(e[j] * inverse)
        sines.append(e[j + 1] * inverse)
        target.append(-sines[j] * target[j])
        target[j] = cosines[j] * target[j]
    y = [None] * 4
    for j in (3, 2, 1, 0):
        t = target[j]
        for k in range(j + 1, 4):
            t = t - columns[k][j] * y[k]
        y[j] = t * inverses[j]
    return y


def combine_kernel(sums_ref, basis_ref, strip_ref, out_ref, held, strips, sems):
    total = jnp.sum(sums_ref[...], axis=0, keepdims=True)
    slot = lax.broadcasted_iota(jnp.int32, (1, SLOTS), 1)
    total = jnp.where(slot == DOTS, sums_ref[0:1, :], total)
    h00, h01, h03, h04, h11, h12, h13, h14, h22, h23, h33, h34, h44, reach = (
        jnp.broadcast_to(total[:, k : k + 1], (8, Z)) for k in range(DOTS + 1)
    )
    h = [
        [h00, h01, h11, h03, h04],
        [None, h11, h12, h13, h14],
        [None, None, h22, h23, 2.0 * h33 - h22],
        [None, None, None, h33, h34],
        [None, None, None, None, h44],
    ]
    y = [jnp.concatenate([c, c]) for c in least_squares(h, reach)]
    lane = lanes()
    for row in range(Y):
        strip = y[0] * strip_ref[0, row]
        for k in (1, 2, 3):
            strip = strip + y[k] * strip_ref[k, row]
        strips[row] = strip
    copies = []
    for s in range(SPECIES):
        for row in range(Y):
            v = y[0] * basis_ref[0, row, s]
            for k in (1, 2, 3):
                v = v + y[k] * basis_ref[k, row, s]
            strip = strips[row]
            v = jnp.where(lane < HALO, shift(strip, -(32 * s + HALO)), v)
            v = jnp.where(lane >= Z - HALO, shift(strip, Z - HALO - (32 * s + 22)), v)
            held[s, pl.ds(row, X, stride=Y), :] = v
        for half in range(2):
            part = pl.ds(half * (X * Y // 2), X * Y // 2)
            copy = pltpu.make_async_copy(held.at[s, part], out_ref.at[s, part], sems.at[2 * s + half])
            copy.start()
            copies.append(copy)
    for copy in copies:
        copy.wait()


def call(kernel, outs, spaces, scratch=(), flops=1000, out_space=VMEM):
    return pl.pallas_call(
        kernel,
        out_shape=outs,
        in_specs=[pl.BlockSpec(memory_space=m) for m in spaces],
        out_specs=jax.tree.map(lambda _: pl.BlockSpec(memory_space=out_space), outs),
        scratch_shapes=list(scratch),
        cost_estimate=pl.CostEstimate(flops=flops, bytes_accessed=1 << 20, transcendentals=0),
        compiler_params=pltpu.CompilerParams(vmem_limit_bytes=24 << 20),
    )


def shards(state, member_set, courant_table, diffusion_table, reaction_table, quadratic_table):
    gy, gh, gx = lax.axis_size("gy"), lax.axis_size("gh"), lax.axis_size("gx")
    gz = gh * gx
    up = [(i, (i + 1) % gy) for i in range(gy)]
    down = [(b, a) for a, b in up]
    far, near = [], []
    for i in range(gz - 1):
        (far if i % 2 else near).extend([(i, i + 1), (i + 1, i)])
    flat = state.reshape(SPECIES, X * Y, Z)

    edge = struct(HALO, SPECIES, X, Z)
    strip_edge = struct(HALO, X, Z)
    pack = struct(PACKS, X, Z)
    inputs = (flat, courant_table.T, diffusion_table.T, reaction_table.transpose(1, 2, 0), quadratic_table.T)
    own, top, bottom, strip, to_far, to_near, *tables = call(
        pack_kernel,
        (struct(Y, SPECIES, X, Z), edge, edge, struct(Y, X, Z), pack, pack, *(struct(*t.shape) for t in inputs[1:])),
        [pltpu.HBM] * len(inputs),
        [
            VMEM(flat.shape, F32),
            pltpu.SemaphoreType.DMA((SPECIES,)),
            pltpu.SemaphoreType.DMA((len(inputs) - 1,)),
        ],
    )(*(pltpu.with_memory_space_constraint(t, pltpu.HBM) for t in inputs))
    from_far = lax.ppermute(to_far, GZ, far)
    from_near = lax.ppermute(to_near, GZ, near)
    low = lax.ppermute(bottom, "gy", up)
    high = lax.ppermute(top, "gy", down)
    table = call(coefficient_kernel, struct(COEFFICIENTS, Z), [SMEM] + [VMEM] * 4)(member_set, *tables)
    wide = (SPECIES, X, Z)
    basis, dots = call(
        main_kernel,
        (struct(4, Y, *wide), struct(DOTS, 8, Z)),
        [VMEM] * 4,
        [VMEM((n, *wide), F32) for n in (ROWS, Y + 8, Y + 6, Y + 4, Y + 2, Y)],
        flops=10_000_000,
    )(own, low, high, table)
    strip, strip_top, strip_bottom = call(
        unpack_kernel, (struct(Y, X, Z), strip_edge, strip_edge), [VMEM] * 3
    )(strip, from_far, from_near)
    strip_low = lax.ppermute(strip_bottom, "gy", up)
    strip_high = lax.ppermute(strip_top, "gy", down)
    strip_basis, total = call(
        strip_kernel,
        (struct(4, Y, X, Z), struct(gy * gz, SLOTS)),
        [VMEM] * 5,
        [VMEM((n, X, Z), F32) for n in (ROWS, Y + 8, Y + 6, Y + 4, Y + 2, Y)],
    )(strip, strip_low, strip_high, dots, table)
    sums = lax.all_to_all(total, ("gy", *GZ), split_axis=0, concat_axis=0, tiled=True)
    out = call(
        combine_kernel,
        struct(SPECIES, X * Y, Z),
        [VMEM] * 3,
        [VMEM((SPECIES, X * Y, Z), F32), VMEM((Y, X, Z), F32), pltpu.SemaphoreType.DMA((2 * SPECIES,))],
        out_space=pltpu.HBM,
    )(sums, basis, strip_basis)
    return out.reshape(state.shape)


def solution(mesh):
    ens, gy, gz = (mesh.shape[a] for a in ("ens", "gy", "gz"))
    split = jax.sharding.Mesh(mesh.devices.reshape(ens, gy, 2, gz // 2), ("ens", "gy", *GZ))
    state_spec = P("ens", None, None, "gy", GZ)

    return jax.shard_map(
        shards,
        mesh=split,
        in_specs=(state_spec, P("ens"), P(), P(), P(), P()),
        out_specs=state_spec,
        check_vma=False,
    )
```

```python
import jax
import jax.numpy as jnp
from jax import lax
from jax.experimental import pallas as pl
from jax.experimental.pallas import tpu as pltpu
from jax.sharding import PartitionSpec as P


SPECIES = 4
X = 16
Y = 16
Z = 128
HALO = 5
GROUP = 6
PACKS = 3
ROWS = Y + 2 * HALO
DOTS = 13
SLOTS = 16
MAIN_SOURCE, MAIN_LEVEL, MAIN_DOT = 24, (22, 20, 18, 16), 16
STRIP_SOURCE, STRIP_LEVEL, STRIP_DOT = 24, (22, 20, 18, 16), 4

F32 = jnp.float32
VMEM = pltpu.VMEM
SMEM = pltpu.SMEM


def struct(*shape):
    return jax.ShapeDtypeStruct(shape, F32)


GZ = ("gh", "gx")


def z_index():
    return lax.axis_index("gh") * lax.axis_size("gx") + lax.axis_index("gx")


def z_size():
    return lax.axis_size("gh") * lax.axis_size("gx")


def lanes():
    return lax.broadcasted_iota(jnp.int32, (X, Z), 1)


def shift(v, amount):
    amount %= Z
    return pltpu.roll(v, amount, 1) if amount else v


def over_rows(count, at_once, body, carry=None):
    if at_once >= count:
        for row in range(count):
            carry = body(row, carry)
        return carry

    def step(i, c):
        for k in range(at_once):
            c = body(i * at_once + k, c)
        return c

    whole = count // at_once
    carry = lax.fori_loop(0, whole, step, carry)
    for row in range(whole * at_once, count):
        carry = body(row, carry)
    return carry


def unpack_kernel(strip_ref, far_ref, near_ref, full_ref, top_ref, bottom_ref):
    place = lanes() % 32
    odd = z_index() % 2 == 1
    for g in range(PACKS):
        far, near = far_ref[g], near_ref[g]
        after = jnp.where(odd, far, near)
        before = jnp.where(odd, near, far)
        for i in range(GROUP):
            y = g * GROUP + i
            if y < Y:
                v = strip_ref[y]
                v = jnp.where(place < HALO, shift(before, -i * HALO), v)
                v = jnp.where(place >= 27, shift(after, 27 - i * HALO), v)
                full_ref[y] = v
                if y < HALO:
                    top_ref[y] = v
                if y >= Y - HALO:
                    bottom_ref[y - (Y - HALO)] = v


def beside_x(v):
    row = lax.broadcasted_iota(jnp.int32, (X, Z), 0)
    below = jnp.where(row == 0, 0.0, pltpu.roll(v, 1, 0))
    above = jnp.where(row == X - 1, 0.0, pltpu.roll(v, X - 1, 0))
    return below, above


def in_grid():
    low = jnp.where(lax.axis_index("gy") > 0, 1.0, 0.0).astype(F32)
    high = jnp.where(lax.axis_index("gy") < lax.axis_size("gy") - 1, 1.0, 0.0).astype(F32)
    return low, high


def row_flag(row, before, low, high):
    if isinstance(row, int):
        return low if row < before else high if row >= before + Y else 1.0
    flag = jnp.where(row < before, low, 1.0)
    return jnp.where(row >= before + Y, high, flag)


def times(value, flag):
    return value if isinstance(flag, float) else value * flag


PLUS, MINUS, LINEAR, QUAD, SCALE, TURNED, STRIP_QUAD, STRIP_SCALE, RANGE = 0, 3, 6, 22, 26, 30, 34, 35, 36
COEFFICIENTS = 40


def coefficient_kernel(member_ref, courant_ref, diffusion_ref, reaction_ref, quadratic_ref, out_ref):
    hot = lax.broadcasted_iota(jnp.int32, (1, courant_ref.shape[-1]), 1) == member_ref[0]

    def picked(table):
        return jnp.sum(jnp.where(hot, table, 0.0), axis=1, keepdims=True)

    def put(row, value):
        out_ref[row : row + 1, :] = jnp.broadcast_to(value, (1, Z))

    lane = lax.broadcasted_iota(jnp.int32, (1, Z), 1)

    def by_species(values):
        out = jnp.broadcast_to(values[3], (1, Z))
        for s in (2, 1, 0):
            out = jnp.where(lane < 32 * (s + 1), values[s], out)
        return out

    courant = picked(courant_ref[...])
    plus, minus = jnp.maximum(courant, 0.0), jnp.minimum(courant, 0.0)
    kept = jnp.ones((1, 1), F32)
    for d in range(3):
        put(PLUS + d, plus[d : d + 1])
        put(MINUS + d, minus[d : d + 1])
        kept = kept - (plus[d : d + 1] - minus[d : d + 1])
    linear = []
    for k in range(SPECIES):
        rates = picked(reaction_ref[k])
        linear.append([rates[l : l + 1] for l in range(SPECIES)])
        linear[k][k] = linear[k][k] + kept
        for l in range(SPECIES):
            put(LINEAR + SPECIES * k + l, linear[k][l])
    for t in range(SPECIES):
        put(TURNED + t, by_species([linear[k][(k - t) % SPECIES] for k in range(SPECIES)]))
    rates = picked(quadratic_ref[...])
    quad = [rates[k : k + 1] for k in range(SPECIES)]
    d = picked(diffusion_ref[...])
    d = [d[k : k + 1] for k in range(SPECIES)]
    reach = 6.0 * jnp.maximum(jnp.maximum(d[0], d[1]), jnp.maximum(d[2], d[3]))
    scale = [v / reach for v in d]
    for k in range(SPECIES):
        put(QUAD + k, quad[k])
        put(SCALE + k, scale[k])
    put(STRIP_QUAD, by_species(quad))
    put(STRIP_SCALE, by_species(scale))
    put(RANGE, reach)


def edge_kernel(state_ref, strip_ref, far_ref, near_ref):
    lane = lanes()
    odd = z_index() % 2 == 1
    place = lane % 32
    lows = [jnp.zeros((X, Z), F32)] * PACKS
    highs = [jnp.zeros((X, Z), F32)] * PACKS
    for y in range(Y):
        total = jnp.zeros((X, Z), F32)
        for s in range(SPECIES):
            v = state_ref[s, pl.ds(y, X, stride=Y), :]
            low = shift(v, 32 * s + HALO)
            high = shift(v, 32 * s + 16 - (Z - 11))
            total = jnp.where((lane >= 32 * s + HALO) & (lane < 32 * s + 16), low, total)
            total = jnp.where((lane >= 32 * s + 16) & (lane < 32 * s + 27), high, total)
        strip_ref[y] = total
    for g in range(PACKS):
        for i in range(GROUP):
            if g * GROUP + i < Y:
                v = strip_ref[g * GROUP + i]
                here = (place >= i * HALO) & (place < (i + 1) * HALO)
                lows[g] = jnp.where(here, shift(v, i * HALO - HALO), lows[g])
                highs[g] = jnp.where(here, shift(v, i * HALO - 22), highs[g])
        far_ref[g] = jnp.where(odd, highs[g], lows[g])
        near_ref[g] = jnp.where(odd, lows[g], highs[g])


def row_kernel(
    state_ref, courant_ref, diffusion_ref, reaction_ref, quadratic_ref,
    own_ref, top_ref, bottom_ref, courant, diffusion, reaction, quadratic, sems,
):
    tables = ((courant_ref, courant), (diffusion_ref, diffusion), (reaction_ref, reaction), (quadratic_ref, quadratic))
    copies = [pltpu.make_async_copy(a, b, sems.at[i]) for i, (a, b) in enumerate(tables)]
    for copy in copies:
        copy.start()
    for y in range(Y):
        for s in range(SPECIES):
            v = state_ref[s, pl.ds(y, X, stride=Y), :]
            own_ref[y, s] = v
            if y < HALO:
                top_ref[y, s] = v
            if y >= Y - HALO:
                bottom_ref[y - (Y - HALO), s] = v
    for copy in copies:
        copy.wait()


def spread(table_ref, row):
    return jnp.broadcast_to(table_ref[row : row + 1, :], (X, Z))


def dot_terms(b):
    pairs = ((0, 0), (0, 1), (0, 3), (0, 4), (1, 1), (1, 2), (1, 3), (1, 4), (2, 2), (2, 3), (3, 3), (3, 4), (4, 4))
    out = []
    for i, j in pairs:
        p = b[i] * b[j]
        out.append(p[:8] + p[8:])
    return out


def level_value(k, image, v, before):
    if k < 3:
        return image
    if k == 3:
        return image - v
    return 2.0 * (image - v) - before


def main_kernel(own_ref, low_ref, high_ref, table_ref, basis_ref, dots_ref, wide, b0, b1, b2, b3, b4):
    low, high = in_grid()
    for r in range(HALO):
        for s in range(SPECIES):
            wide[r, s] = low_ref[r, s] * low
            wide[HALO + Y + r, s] = high_ref[r, s] * high
    for y in range(Y):
        for s in range(SPECIES):
            wide[HALO + y, s] = own_ref[y, s]

    plus = [spread(table_ref, PLUS + d) for d in range(3)]
    minus = [spread(table_ref, MINUS + d) for d in range(3)]
    linear = [[spread(table_ref, LINEAR + SPECIES * k + l) for l in range(SPECIES)] for k in range(SPECIES)]
    quad = [spread(table_ref, QUAD + k) for k in range(SPECIES)]

    def source_row(row, _):
        flag = row_flag(row, HALO - 1, low, high)
        v = [wide[row + 1, s] for s in range(SPECIES)]
        a, b = v[0], v[1]
        coupled = a * b / (1.0 + a * a + b * b)
        for k in range(SPECIES):
            below, above = beside_x(v[k])
            out = plus[0] * below - minus[0] * above
            out = out + (plus[1] * wide[row, k] - minus[1] * wide[row + 2, k])
            out = out + (plus[2] * shift(v[k], 1) - minus[2] * shift(v[k], -1))
            for l in range(SPECIES):
                out = out + linear[k][l] * v[l]
            b0[row, k] = times(out + quad[k] * coupled, flag)
        return _

    over_rows(Y + 8, MAIN_SOURCE, source_row)

    scale = [spread(table_ref, SCALE + s) for s in range(SPECIES)]
    buffers = [b0, b1, b2, b3, b4]

    def image_of(ref, row, s):
        v = ref[row + 1, s]
        below, above = beside_x(v)
        beside = (below + above) + (ref[row, s] + ref[row + 2, s]) + (shift(v, 1) + shift(v, -1))
        return scale[s] * (6.0 * v - beside), v

    for k in (1, 2, 3, 4):
        before = 4 - k

        def level_row(row, _, k=k, before=before):
            flag = row_flag(row, before, low, high)
            for s in range(SPECIES):
                image, v = image_of(buffers[k - 1], row, s)
                value = level_value(k, image, v, buffers[2][row + 2, s] if k == 4 else None)
                buffers[k][row, s] = times(value, flag)
            return _

        over_rows(Y + 2 * before, MAIN_LEVEL[k - 1], level_row)

    def dot_row(row, sums):
        sums = list(sums)
        for s in range(SPECIES):
            b = [buffers[k][row + 4 - k, s] for k in range(5)]
            for k in range(4):
                basis_ref[k, row, s] = b[k]
            sums = [t + p for t, p in zip(sums, dot_terms(b))]
        return tuple(sums)

    sums = over_rows(Y, MAIN_DOT, dot_row, tuple(jnp.zeros((8, Z), F32) for _ in range(DOTS)))
    lane = lax.broadcasted_iota(jnp.int32, (8, Z), 1)
    inner = (lane >= HALO) & (lane < Z - HALO)
    for k in range(DOTS):
        dots_ref[k] = jnp.where(inner, sums[k], 0.0)


def strip_kernel(
    strip_ref, low_ref, high_ref, dots_in_ref, table_ref, basis_ref, total_ref, wide, b0, b1, b2, b3, b4
):
    low, high = in_grid()
    for r in range(HALO):
        wide[r] = low_ref[r] * low
        wide[HALO + Y + r] = high_ref[r] * high
    for y in range(Y):
        wide[HALO + y] = strip_ref[y]

    lane = lanes()
    place = lane % 32
    species = lane // 32
    first = jnp.where(z_index() > 0, 1.0, 0.0).astype(F32)
    last = jnp.where(z_index() < z_size() - 1, 1.0, 0.0).astype(F32)
    inside = jnp.where(place < HALO, first, jnp.where(place >= 27, last, 1.0))
    plus = [spread(table_ref, PLUS + d) for d in range(3)]
    minus = [spread(table_ref, MINUS + d) for d in range(3)]
    linear = [spread(table_ref, TURNED + t) for t in range(SPECIES)]
    quad = spread(table_ref, STRIP_QUAD)

    def source_row(row, _):
        flag = row_flag(row, HALO - 1, low, high)
        v = wide[row + 1]
        turned = [v] + [shift(v, 32 * t) for t in range(1, SPECIES)]
        a, b = turned[3], turned[2]
        for t in (2, 1, 0):
            a = jnp.where(species == t, turned[t], a)
            b = jnp.where(species == (t + 1) % SPECIES, turned[t], b) if t != 2 else jnp.where(species == 0, turned[3], b)
        coupled = a * b / (1.0 + a * a + b * b)
        below, above = beside_x(v)
        out = plus[0] * below - minus[0] * above
        out = out + (plus[1] * wide[row] - minus[1] * wide[row + 2])
        out = out + (plus[2] * shift(v, 1) - minus[2] * shift(v, -1))
        for t in range(SPECIES):
            out = out + linear[t] * turned[t]
        b0[row] = times(out + quad * coupled, flag) * inside
        return _

    over_rows(Y + 8, STRIP_SOURCE, source_row)

    scale = spread(table_ref, STRIP_SCALE)
    buffers = [b0, b1, b2, b3, b4]

    def image_of(ref, row):
        v = ref[row + 1]
        below, above = beside_x(v)
        beside = (below + above) + (ref[row] + ref[row + 2]) + (shift(v, 1) + shift(v, -1))
        return scale * (6.0 * v - beside), v

    for k in (1, 2, 3, 4):
        before = 4 - k

        def level_row(row, _, k=k, before=before):
            flag = row_flag(row, before, low, high)
            image, v = image_of(buffers[k - 1], row)
            value = level_value(k, image, v, buffers[2][row + 2] if k == 4 else None)
            buffers[k][row] = times(value, flag) * inside if before else value
            return _

        over_rows(Y + 2 * before, STRIP_LEVEL[k - 1], level_row)

    def dot_row(row, sums):
        b = [buffers[k][row + 4 - k] for k in range(5)]
        for k in range(4):
            basis_ref[k, row] = b[k]
        return tuple(t + p for t, p in zip(sums, dot_terms(b)))

    sums = over_rows(Y, STRIP_DOT, dot_row, tuple(jnp.zeros((8, Z), F32) for _ in range(DOTS)))
    place = place[:8]
    edge = ((place >= HALO) & (place < 2 * HALO)) | ((place >= 22) & (place < 27))
    slot = lax.broadcasted_iota(jnp.int32, (8, SLOTS), 1)
    total = jnp.broadcast_to(table_ref[RANGE : RANGE + 1, :SLOTS], (8, SLOTS))
    for k in range(DOTS):
        both = jnp.where(edge, sums[k], 0.0) + dots_in_ref[k]
        one = jnp.sum(jnp.sum(both, axis=0, keepdims=True), axis=1, keepdims=True)
        total = jnp.where(slot == k, one, total)
    total_ref[...] = jnp.broadcast_to(total[:1], total_ref.shape)


def least_squares(h, r):
    n = 5
    root = [[None] * n for _ in range(n)]
    for i in range(n):
        rest = h[i][i]
        for k in range(i):
            rest = rest - root[k][i] * root[k][i]
        rest = jnp.maximum(rest, 3e-7 * h[i][i])
        inverse = lax.rsqrt(rest)
        root[i][i] = rest * inverse
        for j in range(i + 1, n):
            t = h[i][j]
            for k in range(i):
                t = t - root[k][i] * root[k][j]
            root[i][j] = t * inverse
    wide = 1.0 + r
    half = 0.5 * r
    columns = []
    for j, weights in enumerate((((0, 1.0), (1, r)), ((1, 1.0), (2, r)), ((2, wide), (3, r)), ((2, half), (3, wide), (4, half)))):
        column = []
        for i in range(j + 2):
            terms = [w * root[i][m] for m, w in weights if i <= m]
            column.append(sum(terms[1:], terms[0]))
        columns.append(column)
    target = [root[0][0]]
    cosines, sines, inverses = [], [], []
    for j in range(4):
        e = columns[j]
        for i in range(j):
            e[i], e[i + 1] = cosines[i] * e[i] + sines[i] * e[i + 1], cosines[i] * e[i + 1] - sines[i] * e[i]
        inverse = lax.rsqrt(e[j] * e[j] + e[j + 1] * e[j + 1])
        inverses.append(inverse)
        cosines.append(e[j] * inverse)
        sines.append(e[j + 1] * inverse)
        target.append(-sines[j] * target[j])
        target[j] = cosines[j] * target[j]
    y = [None] * 4
    for j in (3, 2, 1, 0):
        t = target[j]
        for k in range(j + 1, 4):
            t = t - columns[k][j] * y[k]
        y[j] = t * inverses[j]
    return y


def combine_kernel(sums_ref, basis_ref, strip_ref, out_ref, held, strips, sems):
    total = jnp.sum(sums_ref[...], axis=0, keepdims=True)
    slot = lax.broadcasted_iota(jnp.int32, (1, SLOTS), 1)
    total = jnp.where(slot == DOTS, sums_ref[0:1, :], total)
    h00, h01, h03, h04, h11, h12, h13, h14, h22, h23, h33, h34, h44, reach = (
        jnp.broadcast_to(total[:, k : k + 1], (8, Z)) for k in range(DOTS + 1)
    )
    h = [
        [h00, h01, h11, h03, h04],
        [None, h11, h12, h13, h14],
        [None, None, h22, h23, 2.0 * h33 - h22],
        [None, None, None, h33, h34],
        [None, None, None, None, h44],
    ]
    y = [jnp.concatenate([c, c]) for c in least_squares(h, reach)]
    lane = lanes()
    for row in range(Y):
        strip = y[0] * strip_ref[0, row]
        for k in (1, 2, 3):
            strip = strip + y[k] * strip_ref[k, row]
        strips[row] = strip
    copies = []
    for s in range(SPECIES):
        for row in range(Y):
            v = y[0] * basis_ref[0, row, s]
            for k in (1, 2, 3):
                v = v + y[k] * basis_ref[k, row, s]
            strip = strips[row]
            v = jnp.where(lane < HALO, shift(strip, -(32 * s + HALO)), v)
            v = jnp.where(lane >= Z - HALO, shift(strip, Z - HALO - (32 * s + 22)), v)
            held[s, pl.ds(row, X, stride=Y), :] = v
        for half in range(2):
            part = pl.ds(half * (X * Y // 2), X * Y // 2)
            copy = pltpu.make_async_copy(held.at[s, part], out_ref.at[s, part], sems.at[2 * s + half])
            copy.start()
            copies.append(copy)
    for copy in copies:
        copy.wait()


def call(kernel, outs, spaces, scratch=(), flops=1000, out_space=VMEM):
    return pl.pallas_call(
        kernel,
        out_shape=outs,
        in_specs=[pl.BlockSpec(memory_space=m) for m in spaces],
        out_specs=jax.tree.map(lambda _: pl.BlockSpec(memory_space=out_space), outs),
        scratch_shapes=list(scratch),
        cost_estimate=pl.CostEstimate(flops=flops, bytes_accessed=1 << 20, transcendentals=0),
        compiler_params=pltpu.CompilerParams(vmem_limit_bytes=24 << 20),
    )


def shards(state, member_set, courant_table, diffusion_table, reaction_table, quadratic_table):
    gy, gh, gx = lax.axis_size("gy"), lax.axis_size("gh"), lax.axis_size("gx")
    gz = gh * gx
    up = [(i, (i + 1) % gy) for i in range(gy)]
    down = [(b, a) for a, b in up]
    far, near = [], []
    for i in range(gz - 1):
        (far if i % 2 else near).extend([(i, i + 1), (i + 1, i)])
    flat = state.reshape(SPECIES, X * Y, Z)

    edge = struct(HALO, SPECIES, X, Z)
    strip_edge = struct(HALO, X, Z)
    pack = struct(PACKS, X, Z)
    inputs = (courant_table.T, diffusion_table.T, reaction_table.transpose(1, 2, 0), quadratic_table.T)
    strip, to_far, to_near = call(edge_kernel, (struct(Y, X, Z), pack, pack), [VMEM])(flat)
    own, top, bottom, *tables = call(
        row_kernel,
        (struct(Y, SPECIES, X, Z), edge, edge, *(struct(*t.shape) for t in inputs)),
        [VMEM] + [pltpu.HBM] * len(inputs),
        [pltpu.SemaphoreType.DMA((len(inputs),))],
    )(flat, *(pltpu.with_memory_space_constraint(t, pltpu.HBM) for t in inputs))
    from_far = lax.ppermute(to_far, GZ, far)
    from_near = lax.ppermute(to_near, GZ, near)
    low = lax.ppermute(bottom, "gy", up)
    high = lax.ppermute(top, "gy", down)
    table = call(coefficient_kernel, struct(COEFFICIENTS, Z), [SMEM] + [VMEM] * 4)(member_set, *tables)
    wide = (SPECIES, X, Z)
    basis, dots = call(
        main_kernel,
        (struct(4, Y, *wide), struct(DOTS, 8, Z)),
        [VMEM] * 4,
        [VMEM((n, *wide), F32) for n in (ROWS, Y + 8, Y + 6, Y + 4, Y + 2, Y)],
        flops=10_000_000,
    )(own, low, high, table)
    strip, strip_top, strip_bottom = call(
        unpack_kernel, (struct(Y, X, Z), strip_edge, strip_edge), [VMEM] * 3
    )(strip, from_far, from_near)
    strip_low = lax.ppermute(strip_bottom, "gy", up)
    strip_high = lax.ppermute(strip_top, "gy", down)
    strip_basis, total = call(
        strip_kernel,
        (struct(4, Y, X, Z), struct(gy * gz, SLOTS)),
        [VMEM] * 5,
        [VMEM((n, X, Z), F32) for n in (ROWS, Y + 8, Y + 6, Y + 4, Y + 2, Y)],
    )(strip, strip_low, strip_high, dots, table)
    sums = lax.all_to_all(total, ("gy", *GZ), split_axis=0, concat_axis=0, tiled=True)
    out = call(
        combine_kernel,
        struct(SPECIES, X * Y, Z),
        [VMEM] * 3,
        [VMEM((SPECIES, X * Y, Z), F32), VMEM((Y, X, Z), F32), pltpu.SemaphoreType.DMA((2 * SPECIES,))],
        out_space=pltpu.HBM,
    )(sums, basis, strip_basis)
    return out.reshape(state.shape)


def solution(mesh):
    ens, gy, gz = (mesh.shape[a] for a in ("ens", "gy", "gz"))
    split = jax.sharding.Mesh(mesh.devices.reshape(ens, gy, 2, gz // 2), ("ens", "gy", *GZ))
    state_spec = P("ens", None, None, "gy", GZ)

    return jax.shard_map(
        shards,
        mesh=split,
        in_specs=(state_spec, P("ens"), P(), P(), P(), P()),
        out_specs=state_spec,
        check_vma=False,
    )
```

```python
import jax
import jax.numpy as jnp
from jax import lax
from jax.experimental import pallas as pl
from jax.experimental.pallas import tpu as pltpu
from jax.sharding import PartitionSpec as P


SPECIES = 4
X = 16
Y = 16
Z = 128
HALO = 5
GROUP = 6
PACKS = 3
ROWS = Y + 2 * HALO
DOTS = 13
SLOTS = 16
MAIN_SOURCE, MAIN_LEVEL, MAIN_DOT = 24, (22, 20, 18, 16), 16
STRIP_SOURCE, STRIP_LEVEL, STRIP_DOT = 24, (22, 20, 18, 16), 4

F32 = jnp.float32
VMEM = pltpu.VMEM
SMEM = pltpu.SMEM


def struct(*shape):
    return jax.ShapeDtypeStruct(shape, F32)


GZ = ("gh", "gx")


def z_index():
    return lax.axis_index("gh") * lax.axis_size("gx") + lax.axis_index("gx")


def z_size():
    return lax.axis_size("gh") * lax.axis_size("gx")


def lanes():
    return lax.broadcasted_iota(jnp.int32, (X, Z), 1)


def shift(v, amount):
    amount %= Z
    return pltpu.roll(v, amount, 1) if amount else v


def over_rows(count, at_once, body, carry=None):
    if at_once >= count:
        for row in range(count):
            carry = body(row, carry)
        return carry

    def step(i, c):
        for k in range(at_once):
            c = body(i * at_once + k, c)
        return c

    whole = count // at_once
    carry = lax.fori_loop(0, whole, step, carry)
    for row in range(whole * at_once, count):
        carry = body(row, carry)
    return carry


def unpack_kernel(strip_ref, far_ref, near_ref, full_ref, top_ref, bottom_ref):
    place = lanes() % 32
    odd = z_index() % 2 == 1
    for g in range(PACKS):
        far, near = far_ref[g], near_ref[g]
        after = jnp.where(odd, far, near)
        before = jnp.where(odd, near, far)
        for i in range(GROUP):
            y = g * GROUP + i
            if y < Y:
                v = strip_ref[y]
                v = jnp.where(place < HALO, shift(before, -i * HALO), v)
                v = jnp.where(place >= 27, shift(after, 27 - i * HALO), v)
                full_ref[y] = v
                if y < HALO:
                    top_ref[y] = v
                if y >= Y - HALO:
                    bottom_ref[y - (Y - HALO)] = v


def beside_x(v):
    edge = jnp.zeros((1, Z), F32)
    below = jnp.concatenate([edge, v[: X - 1]])
    above = jnp.concatenate([v[1:], edge])
    return below, above


def in_grid():
    low = jnp.where(lax.axis_index("gy") > 0, 1.0, 0.0).astype(F32)
    high = jnp.where(lax.axis_index("gy") < lax.axis_size("gy") - 1, 1.0, 0.0).astype(F32)
    return low, high


def row_flag(row, before, low, high):
    if isinstance(row, int):
        return low if row < before else high if row >= before + Y else 1.0
    flag = jnp.where(row < before, low, 1.0)
    return jnp.where(row >= before + Y, high, flag)


def times(value, flag):
    return value if isinstance(flag, float) else value * flag


PLUS, MINUS, LINEAR, QUAD, SCALE, TURNED, STRIP_QUAD, STRIP_SCALE, RANGE = 0, 3, 6, 22, 26, 30, 34, 35, 36
COEFFICIENTS = 40


def coefficient_kernel(member_ref, courant_ref, diffusion_ref, reaction_ref, quadratic_ref, out_ref):
    hot = lax.broadcasted_iota(jnp.int32, (1, courant_ref.shape[-1]), 1) == member_ref[0]

    def picked(table):
        return jnp.sum(jnp.where(hot, table, 0.0), axis=1, keepdims=True)

    def put(row, value):
        out_ref[row : row + 1, :] = jnp.broadcast_to(value, (1, Z))

    lane = lax.broadcasted_iota(jnp.int32, (1, Z), 1)

    def by_species(values):
        out = jnp.broadcast_to(values[3], (1, Z))
        for s in (2, 1, 0):
            out = jnp.where(lane < 32 * (s + 1), values[s], out)
        return out

    courant = picked(courant_ref[...])
    plus, minus = jnp.maximum(courant, 0.0), jnp.minimum(courant, 0.0)
    kept = jnp.ones((1, 1), F32)
    for d in range(3):
        put(PLUS + d, plus[d : d + 1])
        put(MINUS + d, minus[d : d + 1])
        kept = kept - (plus[d : d + 1] - minus[d : d + 1])
    linear = []
    for k in range(SPECIES):
        rates = picked(reaction_ref[k])
        linear.append([rates[l : l + 1] for l in range(SPECIES)])
        linear[k][k] = linear[k][k] + kept
        for l in range(SPECIES):
            put(LINEAR + SPECIES * k + l, linear[k][l])
    for t in range(SPECIES):
        put(TURNED + t, by_species([linear[k][(k - t) % SPECIES] for k in range(SPECIES)]))
    rates = picked(quadratic_ref[...])
    quad = [rates[k : k + 1] for k in range(SPECIES)]
    d = picked(diffusion_ref[...])
    d = [d[k : k + 1] for k in range(SPECIES)]
    reach = 6.0 * jnp.maximum(jnp.maximum(d[0], d[1]), jnp.maximum(d[2], d[3]))
    scale = [v / reach for v in d]
    for k in range(SPECIES):
        put(QUAD + k, quad[k])
        put(SCALE + k, scale[k])
    put(STRIP_QUAD, by_species(quad))
    put(STRIP_SCALE, by_species(scale))
    put(RANGE, reach)


def edge_kernel(state_ref, strip_ref, far_ref, near_ref):
    lane = lanes()
    odd = z_index() % 2 == 1
    place = lane % 32
    lows = [jnp.zeros((X, Z), F32)] * PACKS
    highs = [jnp.zeros((X, Z), F32)] * PACKS
    for y in range(Y):
        total = jnp.zeros((X, Z), F32)
        for s in range(SPECIES):
            v = state_ref[s, pl.ds(y, X, stride=Y), :]
            low = shift(v, 32 * s + HALO)
            high = shift(v, 32 * s + 16 - (Z - 11))
            total = jnp.where((lane >= 32 * s + HALO) & (lane < 32 * s + 16), low, total)
            total = jnp.where((lane >= 32 * s + 16) & (lane < 32 * s + 27), high, total)
        strip_ref[y] = total
    for g in range(PACKS):
        for i in range(GROUP):
            if g * GROUP + i < Y:
                v = strip_ref[g * GROUP + i]
                here = (place >= i * HALO) & (place < (i + 1) * HALO)
                lows[g] = jnp.where(here, shift(v, i * HALO - HALO), lows[g])
                highs[g] = jnp.where(here, shift(v, i * HALO - 22), highs[g])
        far_ref[g] = jnp.where(odd, highs[g], lows[g])
        near_ref[g] = jnp.where(odd, lows[g], highs[g])


def row_kernel(
    state_ref, courant_ref, diffusion_ref, reaction_ref, quadratic_ref,
    own_ref, top_ref, bottom_ref, courant, diffusion, reaction, quadratic, sems,
):
    tables = ((courant_ref, courant), (diffusion_ref, diffusion), (reaction_ref, reaction), (quadratic_ref, quadratic))
    copies = [pltpu.make_async_copy(a, b, sems.at[i]) for i, (a, b) in enumerate(tables)]
    for copy in copies:
        copy.start()
    for y in range(Y):
        for s in range(SPECIES):
            v = state_ref[s, pl.ds(y, X, stride=Y), :]
            own_ref[y, s] = v
            if y < HALO:
                top_ref[y, s] = v
            if y >= Y - HALO:
                bottom_ref[y - (Y - HALO), s] = v
    for copy in copies:
        copy.wait()


def spread(table_ref, row):
    return jnp.broadcast_to(table_ref[row : row + 1, :], (X, Z))


def dot_terms(b):
    pairs = ((0, 0), (0, 1), (0, 3), (0, 4), (1, 1), (1, 2), (1, 3), (1, 4), (2, 2), (2, 3), (3, 3), (3, 4), (4, 4))
    out = []
    for i, j in pairs:
        p = b[i] * b[j]
        out.append(p[:8] + p[8:])
    return out


def level_value(k, image, v, before):
    if k < 3:
        return image
    if k == 3:
        return image - v
    return 2.0 * (image - v) - before


def main_kernel(own_ref, low_ref, high_ref, table_ref, basis_ref, dots_ref, wide, b0, b1, b2, b3, b4):
    low, high = in_grid()
    for r in range(HALO):
        for s in range(SPECIES):
            wide[r, s] = low_ref[r, s] * low
            wide[HALO + Y + r, s] = high_ref[r, s] * high
    for y in range(Y):
        for s in range(SPECIES):
            wide[HALO + y, s] = own_ref[y, s]

    plus = [spread(table_ref, PLUS + d) for d in range(3)]
    minus = [spread(table_ref, MINUS + d) for d in range(3)]
    linear = [[spread(table_ref, LINEAR + SPECIES * k + l) for l in range(SPECIES)] for k in range(SPECIES)]
    quad = [spread(table_ref, QUAD + k) for k in range(SPECIES)]

    def source_row(row, _):
        flag = row_flag(row, HALO - 1, low, high)
        v = [wide[row + 1, s] for s in range(SPECIES)]
        a, b = v[0], v[1]
        coupled = a * b / (1.0 + a * a + b * b)
        for k in range(SPECIES):
            below, above = beside_x(v[k])
            out = plus[0] * below - minus[0] * above
            out = out + (plus[1] * wide[row, k] - minus[1] * wide[row + 2, k])
            out = out + (plus[2] * shift(v[k], 1) - minus[2] * shift(v[k], -1))
            for l in range(SPECIES):
                out = out + linear[k][l] * v[l]
            b0[row, k] = times(out + quad[k] * coupled, flag)
        return _

    over_rows(Y + 8, MAIN_SOURCE, source_row)

    scale = [spread(table_ref, SCALE + s) for s in range(SPECIES)]
    buffers = [b0, b1, b2, b3, b4]

    def image_of(ref, row, s):
        v = ref[row + 1, s]
        below, above = beside_x(v)
        beside = (below + above) + (ref[row, s] + ref[row + 2, s]) + (shift(v, 1) + shift(v, -1))
        return scale[s] * (6.0 * v - beside), v

    for k in (1, 2, 3, 4):
        before = 4 - k

        def level_row(row, _, k=k, before=before):
            flag = row_flag(row, before, low, high)
            for s in range(SPECIES):
                image, v = image_of(buffers[k - 1], row, s)
                value = level_value(k, image, v, buffers[2][row + 2, s] if k == 4 else None)
                buffers[k][row, s] = times(value, flag)
            return _

        over_rows(Y + 2 * before, MAIN_LEVEL[k - 1], level_row)

    def dot_row(row, sums):
        sums = list(sums)
        for s in range(SPECIES):
            b = [buffers[k][row + 4 - k, s] for k in range(5)]
            for k in range(4):
                basis_ref[k, row, s] = b[k]
            sums = [t + p for t, p in zip(sums, dot_terms(b))]
        return tuple(sums)

    sums = over_rows(Y, MAIN_DOT, dot_row, tuple(jnp.zeros((8, Z), F32) for _ in range(DOTS)))
    lane = lax.broadcasted_iota(jnp.int32, (8, Z), 1)
    inner = (lane >= HALO) & (lane < Z - HALO)
    for k in range(DOTS):
        dots_ref[k] = jnp.where(inner, sums[k], 0.0)


def strip_kernel(
    strip_ref, low_ref, high_ref, dots_in_ref, table_ref, basis_ref, total_ref, wide, b0, b1, b2, b3, b4
):
    low, high = in_grid()
    for r in range(HALO):
        wide[r] = low_ref[r] * low
        wide[HALO + Y + r] = high_ref[r] * high
    for y in range(Y):
        wide[HALO + y] = strip_ref[y]

    lane = lanes()
    place = lane % 32
    species = lane // 32
    first = jnp.where(z_index() > 0, 1.0, 0.0).astype(F32)
    last = jnp.where(z_index() < z_size() - 1, 1.0, 0.0).astype(F32)
    inside = jnp.where(place < HALO, first, jnp.where(place >= 27, last, 1.0))
    plus = [spread(table_ref, PLUS + d) for d in range(3)]
    minus = [spread(table_ref, MINUS + d) for d in range(3)]
    linear = [spread(table_ref, TURNED + t) for t in range(SPECIES)]
    quad = spread(table_ref, STRIP_QUAD)

    def source_row(row, _):
        flag = row_flag(row, HALO - 1, low, high)
        v = wide[row + 1]
        turned = [v] + [shift(v, 32 * t) for t in range(1, SPECIES)]
        a, b = turned[3], turned[2]
        for t in (2, 1, 0):
            a = jnp.where(species == t, turned[t], a)
            b = jnp.where(species == (t + 1) % SPECIES, turned[t], b) if t != 2 else jnp.where(species == 0, turned[3], b)
        coupled = a * b / (1.0 + a * a + b * b)
        below, above = beside_x(v)
        out = plus[0] * below - minus[0] * above
        out = out + (plus[1] * wide[row] - minus[1] * wide[row + 2])
        out = out + (plus[2] * shift(v, 1) - minus[2] * shift(v, -1))
        for t in range(SPECIES):
            out = out + linear[t] * turned[t]
        b0[row] = times(out + quad * coupled, flag) * inside
        return _

    over_rows(Y + 8, STRIP_SOURCE, source_row)

    scale = spread(table_ref, STRIP_SCALE)
    buffers = [b0, b1, b2, b3, b4]

    def image_of(ref, row):
        v = ref[row + 1]
        below, above = beside_x(v)
        beside = (below + above) + (ref[row] + ref[row + 2]) + (shift(v, 1) + shift(v, -1))
        return scale * (6.0 * v - beside), v

    for k in (1, 2, 3, 4):
        before = 4 - k

        def level_row(row, _, k=k, before=before):
            flag = row_flag(row, before, low, high)
            image, v = image_of(buffers[k - 1], row)
            value = level_value(k, image, v, buffers[2][row + 2] if k == 4 else None)
            buffers[k][row] = times(value, flag) * inside if before else value
            return _

        over_rows(Y + 2 * before, STRIP_LEVEL[k - 1], level_row)

    def dot_row(row, sums):
        b = [buffers[k][row + 4 - k] for k in range(5)]
        for k in range(4):
            basis_ref[k, row] = b[k]
        return tuple(t + p for t, p in zip(sums, dot_terms(b)))

    sums = over_rows(Y, STRIP_DOT, dot_row, tuple(jnp.zeros((8, Z), F32) for _ in range(DOTS)))
    place = place[:8]
    edge = ((place >= HALO) & (place < 2 * HALO)) | ((place >= 22) & (place < 27))
    slot = lax.broadcasted_iota(jnp.int32, (8, SLOTS), 1)
    total = jnp.broadcast_to(table_ref[RANGE : RANGE + 1, :SLOTS], (8, SLOTS))
    for k in range(DOTS):
        both = jnp.where(edge, sums[k], 0.0) + dots_in_ref[k]
        one = jnp.sum(jnp.sum(both, axis=0, keepdims=True), axis=1, keepdims=True)
        total = jnp.where(slot == k, one, total)
    total_ref[...] = jnp.broadcast_to(total[:1], total_ref.shape)


def least_squares(h, r):
    n = 5
    root = [[None] * n for _ in range(n)]
    for i in range(n):
        rest = h[i][i]
        for k in range(i):
            rest = rest - root[k][i] * root[k][i]
        rest = jnp.maximum(rest, 3e-7 * h[i][i])
        inverse = lax.rsqrt(rest)
        root[i][i] = rest * inverse
        for j in range(i + 1, n):
            t = h[i][j]
            for k in range(i):
                t = t - root[k][i] * root[k][j]
            root[i][j] = t * inverse
    wide = 1.0 + r
    half = 0.5 * r
    columns = []
    for j, weights in enumerate((((0, 1.0), (1, r)), ((1, 1.0), (2, r)), ((2, wide), (3, r)), ((2, half), (3, wide), (4, half)))):
        column = []
        for i in range(j + 2):
            terms = [w * root[i][m] for m, w in weights if i <= m]
            column.append(sum(terms[1:], terms[0]))
        columns.append(column)
    target = [root[0][0]]
    cosines, sines, inverses = [], [], []
    for j in range(4):
        e = columns[j]
        for i in range(j):
            e[i], e[i + 1] = cosines[i] * e[i] + sines[i] * e[i + 1], cosines[i] * e[i + 1] - sines[i] * e[i]
        inverse = lax.rsqrt(e[j] * e[j] + e[j + 1] * e[j + 1])
        inverses.append(inverse)
        cosines.append(e[j] * inverse)
        sines.append(e[j + 1] * inverse)
        target.append(-sines[j] * target[j])
        target[j] = cosines[j] * target[j]
    y = [None] * 4
    for j in (3, 2, 1, 0):
        t = target[j]
        for k in range(j + 1, 4):
            t = t - columns[k][j] * y[k]
        y[j] = t * inverses[j]
    return y


def combine_kernel(sums_ref, basis_ref, strip_ref, out_ref, held, strips, sems):
    total = jnp.sum(sums_ref[...], axis=0, keepdims=True)
    slot = lax.broadcasted_iota(jnp.int32, (1, SLOTS), 1)
    total = jnp.where(slot == DOTS, sums_ref[0:1, :], total)
    h00, h01, h03, h04, h11, h12, h13, h14, h22, h23, h33, h34, h44, reach = (
        jnp.broadcast_to(total[:, k : k + 1], (8, Z)) for k in range(DOTS + 1)
    )
    h = [
        [h00, h01, h11, h03, h04],
        [None, h11, h12, h13, h14],
        [None, None, h22, h23, 2.0 * h33 - h22],
        [None, None, None, h33, h34],
        [None, None, None, None, h44],
    ]
    y = [jnp.concatenate([c, c]) for c in least_squares(h, reach)]
    lane = lanes()
    for row in range(Y):
        strip = y[0] * strip_ref[0, row]
        for k in (1, 2, 3):
            strip = strip + y[k] * strip_ref[k, row]
        strips[row] = strip
    copies = []
    for s in range(SPECIES):
        for row in range(Y):
            v = y[0] * basis_ref[0, row, s]
            for k in (1, 2, 3):
                v = v + y[k] * basis_ref[k, row, s]
            strip = strips[row]
            v = jnp.where(lane < HALO, shift(strip, -(32 * s + HALO)), v)
            v = jnp.where(lane >= Z - HALO, shift(strip, Z - HALO - (32 * s + 22)), v)
            held[s, pl.ds(row, X, stride=Y), :] = v
        for half in range(2):
            part = pl.ds(half * (X * Y // 2), X * Y // 2)
            copy = pltpu.make_async_copy(held.at[s, part], out_ref.at[s, part], sems.at[2 * s + half])
            copy.start()
            copies.append(copy)
    for copy in copies:
        copy.wait()


def call(kernel, outs, spaces, scratch=(), flops=1000, out_space=VMEM):
    return pl.pallas_call(
        kernel,
        out_shape=outs,
        in_specs=[pl.BlockSpec(memory_space=m) for m in spaces],
        out_specs=jax.tree.map(lambda _: pl.BlockSpec(memory_space=out_space), outs),
        scratch_shapes=list(scratch),
        cost_estimate=pl.CostEstimate(flops=flops, bytes_accessed=1 << 20, transcendentals=0),
        compiler_params=pltpu.CompilerParams(vmem_limit_bytes=24 << 20),
    )


def shards(state, member_set, courant_table, diffusion_table, reaction_table, quadratic_table):
    gy, gh, gx = lax.axis_size("gy"), lax.axis_size("gh"), lax.axis_size("gx")
    gz = gh * gx
    up = [(i, (i + 1) % gy) for i in range(gy)]
    down = [(b, a) for a, b in up]
    far, near = [], []
    for i in range(gz - 1):
        (far if i % 2 else near).extend([(i, i + 1), (i + 1, i)])
    flat = state.reshape(SPECIES, X * Y, Z)

    edge = struct(HALO, SPECIES, X, Z)
    strip_edge = struct(HALO, X, Z)
    pack = struct(PACKS, X, Z)
    inputs = (courant_table.T, diffusion_table.T, reaction_table.transpose(1, 2, 0), quadratic_table.T)
    strip, to_far, to_near = call(edge_kernel, (struct(Y, X, Z), pack, pack), [VMEM])(flat)
    own, top, bottom, *tables = call(
        row_kernel,
        (struct(Y, SPECIES, X, Z), edge, edge, *(struct(*t.shape) for t in inputs)),
        [VMEM] + [pltpu.HBM] * len(inputs),
        [pltpu.SemaphoreType.DMA((len(inputs),))],
    )(flat, *(pltpu.with_memory_space_constraint(t, pltpu.HBM) for t in inputs))
    from_far = lax.ppermute(to_far, GZ, far)
    from_near = lax.ppermute(to_near, GZ, near)
    low = lax.ppermute(bottom, "gy", up)
    high = lax.ppermute(top, "gy", down)
    table = call(coefficient_kernel, struct(COEFFICIENTS, Z), [SMEM] + [VMEM] * 4)(member_set, *tables)
    wide = (SPECIES, X, Z)
    basis, dots = call(
        main_kernel,
        (struct(4, Y, *wide), struct(DOTS, 8, Z)),
        [VMEM] * 4,
        [VMEM((n, *wide), F32) for n in (ROWS, Y + 8, Y + 6, Y + 4, Y + 2, Y)],
        flops=10_000_000,
    )(own, low, high, table)
    strip, strip_top, strip_bottom = call(
        unpack_kernel, (struct(Y, X, Z), strip_edge, strip_edge), [VMEM] * 3
    )(strip, from_far, from_near)
    strip_low = lax.ppermute(strip_bottom, "gy", up)
    strip_high = lax.ppermute(strip_top, "gy", down)
    strip_basis, total = call(
        strip_kernel,
        (struct(4, Y, X, Z), struct(gy * gz, SLOTS)),
        [VMEM] * 5,
        [VMEM((n, X, Z), F32) for n in (ROWS, Y + 8, Y + 6, Y + 4, Y + 2, Y)],
    )(strip, strip_low, strip_high, dots, table)
    sums = lax.all_to_all(total, ("gy", *GZ), split_axis=0, concat_axis=0, tiled=True)
    out = call(
        combine_kernel,
        struct(SPECIES, X * Y, Z),
        [VMEM] * 3,
        [VMEM((SPECIES, X * Y, Z), F32), VMEM((Y, X, Z), F32), pltpu.SemaphoreType.DMA((2 * SPECIES,))],
        out_space=pltpu.HBM,
    )(sums, basis, strip_basis)
    return out.reshape(state.shape)


def solution(mesh):
    ens, gy, gz = (mesh.shape[a] for a in ("ens", "gy", "gz"))
    split = jax.sharding.Mesh(mesh.devices.reshape(ens, gy, 2, gz // 2), ("ens", "gy", *GZ))
    state_spec = P("ens", None, None, "gy", GZ)

    return jax.shard_map(
        shards,
        mesh=split,
        in_specs=(state_spec, P("ens"), P(), P(), P(), P()),
        out_specs=state_spec,
        check_vma=False,
    )
```
